32 devices in a mesh: dp: 4 (over y, z), tp: 8 (over x, core).
Axes of the slice: x: 4, y: 2, z: 2, core: 2. Of those that a mesh axis runs over, the one named last changes fastest.
The devices are a block of a 4x4x8 slice.
Arguments:
- x: bfloat16 [16384, 3072], P('dp'), parts along dimension 0
- pos: int32 [16384], P('dp'), parts along dimension 0
- g1: bfloat16 [3072], replicated
- g2: bfloat16 [3072], replicated
- wq: bfloat16 [3072, 3072], P(None, 'tp')
- wk: bfloat16 [3072, 1024], replicated
- wv: bfloat16 [3072, 1024], replicated
- wo: bfloat16 [3072, 3072], P('tp')
- wg: bfloat16 [3072, 8192], P(None, 'tp')
- wu: bfloat16 [3072, 8192], P(None, 'tp')
- wd: bfloat16 [8192, 3072], P('tp')
Outputs:
- output 1: bfloat16 [16384, 3072], P('dp'), parts along dimension 0
- output 2: bfloat16 [16384, 8, 128], P('dp', 'tp'), parts along dimension 0
- output 3: bfloat16 [16384, 8, 128], P('dp', 'tp'), parts along dimension 0
There are 4 independent parts. The reference program is written for one: setup_inputs(seed, part) draws one part's arguments, and reference() takes and returns one part's arrays. A program takes and returns all parts, laid end to end along the dimension named above; an argument that names none is the same for every part.
All inputs are finite; a program needn't handle non-finite values.
Results may differ from the reference program's by a relative error of at most 0.0168319.
Values are sent between devices in bfloat16 or wider.
A program may use at most 768 MiB of HBM per device.

```python
import jax
import jax.numpy as jnp
from jax import lax
import numpy as np

D = 3072
HEADS = 24
KV_HEADS = 8
HEAD = 128
FF = 8192
T = 4096
SLOTS = 8

EPS = 1e-5
ROPE_BASE = 500000.0
R = HEADS // KV_HEADS
QB = min(T, 256)


def setup_inputs(seed: int = 0, part: int = 0) -> dict:
    base = jax.random.PRNGKey(seed)
    kw = jax.random.split(jax.random.fold_in(base, 0), 9)
    kx, kp = jax.random.split(jax.random.fold_in(jax.random.fold_in(base, 1), part))

    def w(k, shape, scale):
        return (jax.random.normal(k, shape, jnp.float32) * scale).astype(jnp.bfloat16)

    def gain(k):
        return (1.0 + 0.2 * jax.random.normal(k, (D,), jnp.float32)).astype(jnp.bfloat16)

    x = jax.random.normal(kx, (T, D), jnp.float32).astype(jnp.bfloat16)
    pos = jax.random.randint(kp, (), 0, 4096, dtype=jnp.int32) + jnp.arange(T, dtype=jnp.int32)
    return {
        "x": x,
        "pos": pos,
        "g1": gain(kw[0]),
        "g2": gain(kw[1]),
        "wq": w(kw[2], (D, HEADS * HEAD), 1.5 * D ** -0.5),
        "wk": w(kw[3], (D, KV_HEADS * HEAD), 1.5 * D ** -0.5),
        "wv": w(kw[4], (D, KV_HEADS * HEAD), D ** -0.5),
        "wo": w(kw[5], (HEADS * HEAD, D), 2.0 * (HEADS * HEAD) ** -0.5),
        "wg": w(kw[6], (D, FF), D ** -0.5),
        "wu": w(kw[7], (D, FF), D ** -0.5),
        "wd": w(kw[8], (FF, D), 2.0 * FF ** -0.5),
    }


def _rms(x, g):
    x32 = x.astype(jnp.float32)
    inv = lax.rsqrt(jnp.mean(x32 * x32, axis=-1, keepdims=True) + EPS)
    return (x32 * inv * g.astype(jnp.float32)).astype(jnp.bfloat16)


def _rope(t, pos):
    half = HEAD // 2
    inv = ROPE_BASE ** (-2.0 * jnp.arange(half, dtype=jnp.float32) / HEAD)
    ang = pos.astype(jnp.float32)[:, None] * inv[None, :]
    c = jnp.cos(ang)[:, None, :]
    s = jnp.sin(ang)[:, None, :]
    t1, t2 = t[..., :half], t[..., half:]
    return jnp.concatenate([t1 * c - t2 * s, t2 * c + t1 * s], axis=-1)


def reference(x, pos, g1, g2, wq, wk, wv, wo, wg, wu, wd):
    a = _rms(x, g1)
    q = _rope(jnp.dot(a, wq, preferred_element_type=jnp.float32).reshape(T, HEADS, HEAD), pos).astype(jnp.bfloat16)
    k = _rope(jnp.dot(a, wk, preferred_element_type=jnp.float32).reshape(T, KV_HEADS, HEAD), pos).astype(jnp.bfloat16)
    v = jnp.dot(a, wv, preferred_element_type=jnp.float32).astype(jnp.bfloat16).reshape(T, KV_HEADS, HEAD)
    qg = q.reshape(T // QB, QB, KV_HEADS, R, HEAD)
    pq = pos.reshape(T // QB, QB)
    scale = HEAD ** -0.5

    def one_head(g):
        kg = k[:, g].astype(jnp.float32)
        vg = v[:, g].astype(jnp.float32)

        def one_block(blk):
            qq, pb = blk
            sc = jnp.einsum("qrd,kd->rqk", qq.astype(jnp.float32), kg) * scale
            sc = jnp.where((pos[None, :] <= pb[:, None])[None], sc, -jnp.inf)
            e = jnp.exp(sc - jnp.max(sc, axis=-1, keepdims=True))
            pr = (e / jnp.sum(e, axis=-1, keepdims=True)).astype(jnp.bfloat16)
            return jnp.einsum("rqk,kd->qrd", pr.astype(jnp.float32), vg).astype(jnp.bfloat16)

        return lax.map(one_block, (qg[:, :, g], pq))

    o = lax.map(one_head, jnp.arange(KV_HEADS))
    o = o.transpose(1, 2, 0, 3, 4).reshape(T, HEADS * HEAD)
    h = (x.astype(jnp.float32) + jnp.dot(o, wo, preferred_element_type=jnp.float32)).astype(jnp.bfloat16)
    b = _rms(h, g2)
    gt = jnp.dot(b, wg, preferred_element_type=jnp.float32)
    up = jnp.dot(b, wu, preferred_element_type=jnp.float32)
    u = (jax.nn.silu(gt) * up).astype(jnp.bfloat16)
    y = (h.astype(jnp.float32) + jnp.dot(u, wd, preferred_element_type=jnp.float32)).astype(jnp.bfloat16)
    sl = np.arange(SLOTS) * KV_HEADS // SLOTS
    return (y, k[:, sl], v[:, sl])
```

```python
import functools

import jax
import jax.numpy as jnp
from jax import lax
from jax.experimental import pallas as pl
from jax.experimental.pallas import tpu as pltpu
from jax.sharding import PartitionSpec as P

HEAD = 128
EPS = 1e-5
ROPE_BASE = 500000.0
MESH = pl.DeviceIdType.MESH
BLOCK = 256
BF = jnp.bfloat16
F32 = jnp.float32


def _sincos(ang):
    n = jnp.floor(ang * 0.6366197723675814 + 0.5)
    r = ((ang - n * 1.5703125) - n * 4.837512969970703125e-4) - n * 7.54978995489188216e-8
    z = r * r
    s = ((-1.9515295891e-4 * z + 8.3321608736e-3) * z - 1.6666654611e-1) * z * r + r
    c = ((2.443315711809948e-5 * z - 1.388731625493765e-3) * z + 4.166664568298827e-2) * z * z - 0.5 * z + 1.0
    m = n.astype(jnp.int32)
    odd = (m & 1) == 1
    cs = jnp.where(odd, s, c)
    sn = jnp.where(odd, c, s)
    cs = jnp.where(((m + 1) & 2) == 2, -cs, cs)
    sn = jnp.where((m & 2) == 2, -sn, sn)
    return cs, sn


def _kernel(tp, dp, l1, l2, w2, w3,
            x_ref, posf_ref, inv_ref, g1_ref, g2_ref, wq_ref, wk_ref, wv_ref, wo_ref, wg_ref, wu_ref, wd_ref,
            y_ref, k_ref, v_ref, oall_ref,
            wqkv, wo_v, wg_v, wu_v, wd_v, x_buf, pos_buf, a_buf, q_scr, k_scr, v_scr, m_scr, l_scr, acc_scr, o_buf,
            o_blk, xh, hbuf, u_buf, r_buf, rsib, cp, rs1, rs2, sums, ych, hst,
            ld_w, ld_mlp, ld_x, ld_pos, kv_s,
            wo_a, wo_rel_s, wo_rel_r, wo_z_s, wo_z_r,
            o_s, o_rl, o_rr, o_rlr, o_rrr, o_rs, o_rel,
            ld_o, h_s, h_r, r_s, r_r, s1_s, s1_r, s2_s, s2_r, y_s, y_rl, y_rr, y_rlr, y_rrr, y_rs, y_rel):
    t, d = x_ref.shape
    qw = wq_ref.shape[1]
    f = wg_ref.shape[1]
    hl = qw // HEAD
    b = BLOCK
    nb = t // b
    dh = d // 2
    hb = b // 2
    nc = tp // 2
    ow = hb // nc
    hw = ow // 2
    kvt = min(2 * b, t)

    r = lax.axis_index("tp")
    c = r // 2
    s = r % 2
    c_r = (c + 1) % nc
    c_l = (c + nc - 1) % nc
    c_o = (c + 2) % nc
    right = {"tp": c_r * 2 + s}
    left = {"tp": c_l * 2 + s}
    sib = {"tp": c * 2 + 1 - s}
    share = dp % 2 == 0
    dpi = lax.axis_index("dp")
    par = dpi % 2
    peer = {"dp": dpi + 1 - 2 * par}

    def al(v, m):
        return pl.multiple_of(v, m)

    def send(src, dst, ss, rs, dev):
        pltpu.make_async_remote_copy(
            src_ref=src, dst_ref=dst, send_sem=ss, recv_sem=rs, device_id=dev, device_id_type=MESH).start()

    def put(src, dst, sem):
        pltpu.make_async_copy(src, dst, sem).start()

    def wait(region, sem):
        pltpu.make_async_copy(region, region, sem).wait()

    barrier = pltpu.get_barrier_semaphore()
    others = [right, left, sib] + ([peer] if share else [])
    for dev in others:
        pl.semaphore_signal(barrier, inc=1, device_id=dev, device_id_type=MESH)
    pl.semaphore_wait(barrier, len(others))

    ro = al(r * qw, 128)
    mine = al(s * dh, 128)
    other = al((1 - s) * dh, 128)
    send(wo_ref.at[:, pl.ds(other, dh)], wo_v.at[pl.ds(ro, qw)], wo_a.at[0], wo_a.at[1], sib)
    put(wo_ref.at[:, pl.ds(mine, dh)], wo_v.at[pl.ds(ro, qw)], wo_a.at[2])
    put(x_ref.at[pl.ds(0, b)], x_buf.at[0], ld_x.at[0])
    put(posf_ref.at[pl.ds(0, b)], pos_buf.at[0], ld_pos.at[0])
    rk = al(r * HEAD, 128)
    put(wq_ref, wqkv.at[:, pl.ds(0, qw)], ld_w.at[0])
    put(wk_ref.at[:, pl.ds(rk, HEAD)], wqkv.at[:, pl.ds(qw, HEAD)], ld_w.at[1])
    put(wv_ref.at[:, pl.ds(rk, HEAD)], wqkv.at[:, pl.ds(qw + HEAD, HEAD)], ld_w.at[2])
    put(wg_ref, wg_v, ld_mlp.at[0])
    put(wu_ref, wu_v, ld_mlp.at[1])
    put(wd_ref, wd_v, ld_mlp.at[2])

    wr = qw if share else 2 * qw
    woff = par * qw if share else 0

    def wrow(chip, half=None):
        base = al(chip * (2 * qw) + woff, 64)
        if half is None:
            return wo_v.at[pl.ds(base, wr)]
        return wo_v.at[pl.ds(al(base + half * (wr // 2), 64), wr // 2)]

    rs_sib = al((r + 1 - 2 * s) * qw, 128)
    wait(wo_v.at[pl.ds(rs_sib, qw)], wo_a.at[1])
    wait(wo_v.at[pl.ds(ro, qw)], wo_a.at[2])
    send(wrow(c), wrow(c), wo_a.at[3], wo_a.at[4], right)
    send(wrow(c), wrow(c), wo_a.at[5], wo_a.at[6], left)

    def wo_stage2():
        wait(wrow(c_l), wo_a.at[4])
        send(wrow(c_l, 0), wrow(c_l, 0), wo_rel_s.at[0], wo_rel_r.at[0], right)
        if share:
            send(wrow(c_l), wrow(c_l), wo_z_s, wo_z_r, peer)
        wait(wrow(c_r), wo_a.at[6])
        send(wrow(c_r, 1), wrow(c_r, 1), wo_rel_s.at[1], wo_rel_r.at[1], left)
        if share:
            send(wrow(c_r), wrow(c_r), wo_z_s, wo_z_r, peer)

    def wo_stage3():
        wait(wrow(c_o, 0), wo_rel_r.at[0])
        wait(wrow(c_o, 1), wo_rel_r.at[1])
        if share:
            send(wrow(c_o), wrow(c_o), wo_z_s, wo_z_r, peer)

    def ocol(chip, core):
        return pl.ds(al((chip * 2 + core) * qw, 128), qw)

    def orow(j):
        return pl.ds(al(j * b, b), b)

    def orow_half(j, half):
        return pl.ds(al(j * b + half * hb, hb), hb)

    def o_stage2(j):
        @pl.when((j >= 0) & (j < nb))
        def _():
            reg = oall_ref.at[orow(j), ocol(c_l, s)]
            top = oall_ref.at[orow_half(j, 0), ocol(c_l, s)]
            wait(reg, o_rl.at[j])
            send(top, top, o_rel.at[0], o_rlr.at[j], right)
            send(reg, reg, o_rel.at[2], o_rs.at[j], sib)
            reg = oall_ref.at[orow(j), ocol(c_r, s)]
            bot = oall_ref.at[orow_half(j, 1), ocol(c_r, s)]
            wait(reg, o_rr.at[j])
            send(bot, bot, o_rel.at[1], o_rrr.at[j], left)
            send(reg, reg, o_rel.at[2], o_rs.at[j], sib)

    def o_stage3(j):
        @pl.when((j >= 0) & (j < nb))
        def _():
            top = oall_ref.at[orow_half(j, 0), ocol(c_o, s)]
            bot = oall_ref.at[orow_half(j, 1), ocol(c_o, s)]
            reg = oall_ref.at[orow(j), ocol(c_o, s)]
            wait(top, o_rlr.at[j])
            wait(bot, o_rrr.at[j])
            send(reg, reg, o_rel.at[2], o_rs.at[j], sib)

    scale = HEAD ** -0.5 * 1.4426950408889634
    for h in range(t // kvt):
        v_scr[h * kvt:(h + 1) * kvt, :] = jnp.zeros((kvt, HEAD), BF)
        k_scr[h * kvt:(h + 1) * kvt, :] = jnp.zeros((kvt, HEAD), BF)
    wait(wqkv.at[:, pl.ds(0, qw)], ld_w.at[0])
    wait(wqkv.at[:, pl.ds(qw, HEAD)], ld_w.at[1])
    wait(wqkv.at[:, pl.ds(qw, HEAD)], ld_w.at[2])
    lane = lax.broadcasted_iota(jnp.int32, (b, HEAD), 1)

    def tile(i, j, masked):
        keys = pl.ds(al(j * kvt, kvt), kvt)
        kk = k_scr[keys, :]
        vv = v_scr[keys, :]
        for h in range(hl):
            sc = lax.dot_general(q_scr[h], kk, (((1,), (1,)), ((), ())), preferred_element_type=F32)
            if masked:
                rows = i * b + lax.broadcasted_iota(jnp.int32, (b, kvt), 0)
                cols = j * kvt + lax.broadcasted_iota(jnp.int32, (b, kvt), 1)
                sc = jnp.where(cols <= rows, sc, -jnp.inf)
            m_prev = m_scr[h]
            m_new = jnp.maximum(m_prev, jnp.max(sc, axis=1, keepdims=True))
            parts = [jnp.exp2((sc[:, e * HEAD:(e + 1) * HEAD] - m_new) * scale) for e in range(kvt // HEAD)]
            alpha = jnp.exp2((m_prev - m_new) * scale)
            l_scr[h] = l_scr[h] * alpha + functools.reduce(lambda p, q: p + q, parts)
            pr = jnp.concatenate([p.astype(BF) for p in parts], axis=1)
            acc_scr[h] = acc_scr[h] * alpha + jnp.dot(pr, vv, preferred_element_type=F32)
            m_scr[h] = m_new

    def phase1(i, carry):
        slot = i % 2
        wait(x_buf.at[slot], ld_x.at[slot])
        wait(pos_buf.at[slot], ld_pos.at[slot])

        @pl.when(i + 1 < nb)
        def _():
            put(x_ref.at[pl.ds(al((i + 1) * b, b), b)], x_buf.at[1 - slot], ld_x.at[1 - slot])
            put(posf_ref.at[pl.ds(al((i + 1) * b, b), b)], pos_buf.at[1 - slot], ld_pos.at[1 - slot])

        def norm(j, carry):
            rows = pl.ds(al(j * 16, 16), 16)
            v32 = x_buf[slot, rows, :].astype(F32)
            inv = lax.rsqrt(jnp.mean(v32 * v32, axis=1, keepdims=True) + EPS)
            a_buf[rows, :] = (v32 * inv * g1_ref[...].astype(F32)).astype(BF)
            return carry

        lax.fori_loop(0, b // 16, norm, 0)
        co, si = _sincos(pos_buf[slot] * inv_ref[...])
        si = jnp.where(lane < HEAD // 2, -si, si)
        qkv = jnp.dot(a_buf[...], wqkv[...], preferred_element_type=F32)

        def rope(v32):
            return (v32 * co + pltpu.roll(v32, HEAD // 2, 1) * si).astype(BF)

        rows = pl.ds(al(i * b, b), b)
        for h in range(hl):
            q_scr[h] = rope(qkv[:, h * HEAD:(h + 1) * HEAD])
        k_scr[rows, :] = rope(qkv[:, qw:qw + HEAD])
        v_scr[rows, :] = qkv[:, qw + HEAD:qw + 2 * HEAD].astype(BF)
        for h in range(hl):
            m_scr[h] = jnp.full((b, HEAD), -jnp.inf, F32)
            l_scr[h] = jnp.zeros((b, HEAD), F32)
            acc_scr[h] = jnp.zeros((b, HEAD), F32)
        last = (i * b) // kvt

        def inner(j, carry):
            tile(i, j, False)
            return carry

        lax.fori_loop(0, last, inner, 0)
        tile(i, last, True)
        for h in range(hl):
            o_buf[rows, h * HEAD:(h + 1) * HEAD] = (
                acc_scr[h] / jnp.sum(l_scr[h], axis=1, keepdims=True)).astype(BF)
        src = o_buf.at[rows]
        dst = oall_ref.at[orow(i), ocol(c, s)]
        send(src, dst, o_s.at[0], o_rl.at[i], right)
        send(src, dst, o_s.at[1], o_rr.at[i], left)
        send(src, dst, o_s.at[2], o_rs.at[i], sib)
        put(src, dst, o_s.at[3])

        @pl.when(i == w2)
        def _():
            wo_stage2()

        @pl.when(i == w3)
        def _():
            wo_stage3()

        o_stage2(i - l1)
        o_stage3(i - l2)
        return carry

    lax.fori_loop(0, nb, phase1, 0)
    put(k_scr, k_ref, kv_s.at[0])
    put(v_scr, v_ref, kv_s.at[1])
    wait(o_buf, o_s.at[3])
    wait(wg_v, ld_mlp.at[0])
    wait(wu_v, ld_mlp.at[1])
    wait(wd_v, ld_mlp.at[2])
    if share:
        wait(wo_v.at[pl.ds(0, 3 * wr)], wo_z_r)

    def load_o(j):
        wait(oall_ref.at[orow(j), pl.ds(0, 4 * qw)], o_rs.at[j])
        put(oall_ref.at[orow(j)], o_blk, ld_o.at[0])
        put(x_ref.at[orow(j), pl.ds(mine, dh)], xh, ld_o.at[1])

    nt_h = min(512, dh)
    nt_f = min(256, f)
    nt_d = min(512, d)

    def sum_start(j):
        @pl.when((j >= 0) & (j < nb))
        def _():
            two = j % 2
            q4 = j % 4
            wait(rsib.at[two], r_r.at[two])
            wait(rsib.at[two], r_s)

            def add(e, carry):
                rows = pl.ds(al(e * 16, 16), 16)
                own = r_buf[pl.ds(al(s * hb + e * 16, 16), 16), :]
                cp[q4, rows, :] = (own.astype(F32) + rsib[two, rows, :].astype(F32)).astype(BF)
                return carry

            lax.fori_loop(0, hb // 16, add, 0)

            def part(chip, half):
                return cp.at[q4, pl.ds(al(chip * ow + half * hw, hw), hw)]

            send(part(c_o, 0), rs1.at[q4, 0], s1_s.at[q4, 0], s1_r.at[q4, 0], right)
            send(part(c_o, 1), rs1.at[q4, 2], s1_s.at[q4, 2], s1_r.at[q4, 2], left)
            send(part(c_r, 1), rs1.at[q4, 1], s1_s.at[q4, 1], s1_r.at[q4, 1], right)
            send(part(c_l, 0), rs1.at[q4, 3], s1_s.at[q4, 3], s1_r.at[q4, 3], left)

    def own_h(j):
        @pl.when(j < nb)
        def _():
            two = j % 2
            wait(o_blk, ld_o.at[0])
            wait(xh, ld_o.at[1])

            def col(n, carry):
                cols = pl.ds(al(n * nt_h, nt_h), nt_h)
                v32 = jnp.dot(o_blk[...], wo_v[:, cols], preferred_element_type=F32)
                hbuf[two, :, pl.ds(al(s * dh + n * nt_h, 128), nt_h)] = (xh[:, cols].astype(F32) + v32).astype(BF)
                return carry

            lax.fori_loop(0, dh // nt_h, col, 0)
            half = hbuf.at[two, :, pl.ds(mine, dh)]
            send(half, half, h_s.at[two], h_r.at[two], sib)

        @pl.when(j + 1 < nb)
        def _():
            load_o(j + 1)

    def mlp_norm(j):
        @pl.when((j >= 0) & (j < nb))
        def _():
            two = j % 2
            wait(hbuf.at[two, :, pl.ds(other, dh)], h_r.at[two])
            wait(hbuf.at[two, :, pl.ds(mine, dh)], h_s.at[two])

            def norm(e, carry):
                rows = pl.ds(al(e * 16, 16), 16)
                v32 = hbuf[two, rows, :].astype(F32)
                inv = lax.rsqrt(jnp.mean(v32 * v32, axis=1, keepdims=True) + EPS)
                a_buf[rows, :] = (v32 * inv * g2_ref[...].astype(F32)).astype(BF)
                return carry

            lax.fori_loop(0, b // 16, norm, 0)
            hst[j % 4] = hbuf[two, pl.ds(al(s * hb + c * ow, 16), ow), :]

    def mlp_up(j):
        @pl.when((j >= 0) & (j < nb))
        def _():
            def col(n, carry):
                cols = pl.ds(al(n * nt_f, nt_f), nt_f)
                gt = jnp.dot(a_buf[...], wg_v[:, cols], preferred_element_type=F32)
                up = jnp.dot(a_buf[...], wu_v[:, cols], preferred_element_type=F32)
                u_buf[:, cols] = (gt * (1.0 / (1.0 + jnp.exp(-gt))) * up).astype(BF)
                return carry

            lax.fori_loop(0, f // nt_f, col, 0)

    def mlp_down(j):
        @pl.when((j >= 0) & (j < nb))
        def _():
            def col(n, carry):
                cols = pl.ds(al(n * nt_d, nt_d), nt_d)
                r_buf[:, cols] = jnp.dot(u_buf[...], wd_v[:, cols], preferred_element_type=F32).astype(BF)
                return carry

            lax.fori_loop(0, d // nt_d, col, 0)
            send(r_buf.at[pl.ds(al((1 - s) * hb, hb), hb)], rsib.at[j % 2], r_s, r_r.at[j % 2], sib)

    def sum_relay(j):
        @pl.when((j >= 0) & (j < nb))
        def _():
            q4 = j % 4

            @pl.when(j >= 4)
            def _():
                wait(sums.at[q4, 0], s2_s.at[q4, 0])
                wait(sums.at[q4, 1], s2_s.at[q4, 1])

            wait(rs1.at[q4, 0], s1_r.at[q4, 0])
            sums[q4, 0] = (rs1[q4, 0].astype(F32) + cp[q4, pl.ds(al(c_r * ow, 16), hw), :].astype(F32)).astype(BF)
            send(sums.at[q4, 0], rs2.at[q4, 0], s2_s.at[q4, 0], s2_r.at[q4, 0], right)
            wait(rs1.at[q4, 2], s1_r.at[q4, 2])
            sums[q4, 1] = (rs1[q4, 2].astype(F32) + cp[q4, pl.ds(al(c_l * ow + hw, 16), hw), :].astype(F32)).astype(BF)
            send(sums.at[q4, 1], rs2.at[q4, 1], s2_s.at[q4, 1], s2_r.at[q4, 1], left)

    def yrow(j, core, chip):
        return y_ref.at[pl.ds(al(j * b + core * hb + chip * ow, ow), ow)]

    def yrow_half(j, core, chip, half):
        return y_ref.at[pl.ds(al(j * b + core * hb + chip * ow + half * hw, hw), hw)]

    def sum_end(j):
        @pl.when((j >= 0) & (j < nb))
        def _():
            q4 = j % 4

            @pl.when(j >= 4)
            def _():
                for e in range(4):
                    wait(ych.at[q4], y_s.at[q4, e])

            for e in range(4):
                wait(rs1.at[q4, e], s1_s.at[q4, e])
            wait(rs1.at[q4, 1], s1_r.at[q4, 1])
            wait(rs1.at[q4, 3], s1_r.at[q4, 3])
            wait(rs2.at[q4, 0], s2_r.at[q4, 0])
            wait(rs2.at[q4, 1], s2_r.at[q4, 1])
            for half, (near, far) in enumerate(((3, 0), (1, 1))):
                own = cp[q4, pl.ds(al(c * ow + half * hw, 16), hw), :].astype(F32)
                tot = own + rs1[q4, near].astype(F32) + rs2[q4, far].astype(F32)
                hh = hst[q4, half * hw:(half + 1) * hw, :].astype(F32)
                ych[q4, half * hw:(half + 1) * hw, :] = (hh + tot).astype(BF)
            dst = yrow(j, s, c)
            send(ych.at[q4], dst, y_s.at[q4, 0], y_rl.at[j], right)
            send(ych.at[q4], dst, y_s.at[q4, 1], y_rr.at[j], left)
            send(ych.at[q4], dst, y_s.at[q4, 2], y_rs.at[j], sib)
            put(ych.at[q4], dst, y_s.at[q4, 3])

    def y_stage2(j):
        @pl.when((j >= 0) & (j < nb))
        def _():
            reg = yrow(j, s, c_l)
            top = yrow_half(j, s, c_l, 0)
            wait(reg, y_rl.at[j])
            send(top, top, y_rel.at[0], y_rlr.at[j], right)
            send(reg, reg, y_rel.at[2], y_rs.at[j], sib)
            reg = yrow(j, s, c_r)
            bot = yrow_half(j, s, c_r, 1)
            wait(reg, y_rr.at[j])
            send(bot, bot, y_rel.at[1], y_rrr.at[j], left)
            send(reg, reg, y_rel.at[2], y_rs.at[j], sib)

    def y_stage3(j):
        @pl.when((j >= 0) & (j < nb))
        def _():
            wait(yrow_half(j, s, c_o, 0), y_rlr.at[j])
            wait(yrow_half(j, s, c_o, 1), y_rrr.at[j])
            reg = yrow(j, s, c_o)
            send(reg, reg, y_rel.at[2], y_rs.at[j], sib)

    load_o(0)

    def phase2(i, carry):
        sum_start(i - 2)
        own_h(i)
        mlp_norm(i - 1)
        sum_relay(i - 3)
        mlp_up(i - 1)
        sum_end(i - 4)
        mlp_down(i - 1)
        y_stage2(i - 5)
        y_stage3(i - 6)
        o_stage2(nb + i - l1)
        o_stage3(nb + i - l2)
        return carry

    lax.fori_loop(0, nb + 6, phase2, 0)

    def drain(j, carry):
        wait(y_ref.at[pl.ds(0, hb)], y_rs.at[j])
        return carry

    lax.fori_loop(0, nb, drain, 0)
    for q4 in range(4):
        for e in range(4):
            wait(ych.at[q4], y_s.at[q4, e])
        for e in range(2):
            wait(sums.at[q4, e], s2_s.at[q4, e])
    wait(y_ref.at[pl.ds(0, nb * hw)], y_rel.at[0])
    wait(y_ref.at[pl.ds(0, nb * hw)], y_rel.at[1])
    wait(y_ref.at[pl.ds(0, nb * ow * 3)], y_rel.at[2])
    for e in range(3):
        wait(o_buf, o_s.at[e])
    wait(oall_ref.at[pl.ds(0, t // 2), pl.ds(0, qw)], o_rel.at[0])
    wait(oall_ref.at[pl.ds(0, t // 2), pl.ds(0, qw)], o_rel.at[1])
    wait(oall_ref.at[:, pl.ds(0, 3 * qw)], o_rel.at[2])
    wait(wo_v.at[pl.ds(0, qw)], wo_a.at[0])
    wait(wo_v.at[pl.ds(0, wr)], wo_a.at[3])
    wait(wo_v.at[pl.ds(0, wr)], wo_a.at[5])
    for e in range(2):
        wait(wo_v.at[pl.ds(0, wr // 2)], wo_rel_s.at[e])
    if share:
        wait(wo_v.at[pl.ds(0, 3 * wr)], wo_z_s)
    wait(k_scr, kv_s.at[0])
    wait(v_scr, kv_s.at[1])


def _layer(tp, dp, x, posf, inv, g1, g2, wq, wk, wv, wo, wg, wu, wd):
    t, d = x.shape
    qw = wq.shape[1]
    f = wg.shape[1]
    hl = qw // HEAD
    b = BLOCK
    nb = t // b
    hb = b // 2
    nc = tp // 2
    ow = hb // nc
    hw = ow // 2
    assert nc == 4 and t % b == 0 and wk.shape[1] == tp * HEAD
    l1 = max(1, nb * 3 // 8)
    l2 = l1 + max(1, nb // 8)
    w2 = nb * 5 // 16
    w3 = nb * 9 // 16
    dma = pltpu.SemaphoreType.DMA
    hbm = pl.BlockSpec(memory_space=pl.ANY)
    vm = pl.BlockSpec(memory_space=pltpu.VMEM)
    scratch = [
        pltpu.VMEM((d, qw + 2 * HEAD), BF),
        pltpu.VMEM((tp * qw, d // 2), BF),
        pltpu.VMEM((d, f), BF),
        pltpu.VMEM((d, f), BF),
        pltpu.VMEM((f, d), BF),
        pltpu.VMEM((2, b, d), BF),
        pltpu.VMEM((2, b, HEAD), F32),
        pltpu.VMEM((b, d), BF),
        pltpu.VMEM((hl, b, HEAD), BF),
        pltpu.VMEM((t, HEAD), BF),
        pltpu.VMEM((t, HEAD), BF),
        pltpu.VMEM((hl, b, HEAD), F32),
        pltpu.VMEM((hl, b, HEAD), F32),
        pltpu.VMEM((hl, b, HEAD), F32),
        pltpu.VMEM((t, qw), BF),
        pltpu.VMEM((b, tp * qw), BF),
        pltpu.VMEM((b, d // 2), BF),
        pltpu.VMEM((2, b, d), BF),
        pltpu.VMEM((b, f), BF),
        pltpu.VMEM((b, d), BF),
        pltpu.VMEM((2, hb, d), BF),
        pltpu.VMEM((4, hb, d), BF),
        pltpu.VMEM((4, 4, hw, d), BF),
        pltpu.VMEM((4, 2, hw, d), BF),
        pltpu.VMEM((4, 2, hw, d), BF),
        pltpu.VMEM((4, ow, d), BF),
        pltpu.VMEM((4, ow, d), BF),
        dma((3,)), dma((3,)), dma((2,)), dma((2,)), dma((2,)),
        dma((7,)), dma((2,)), dma((2,)), dma(()), dma(()),
        dma((4,)), dma((nb,)), dma((nb,)), dma((nb,)), dma((nb,)), dma((nb,)), dma((3,)),
        dma((2,)), dma((2,)), dma((2,)), dma(()), dma((2,)), dma((4, 4)), dma((4, 4)), dma((4, 2)), dma((4, 2)),
        dma((4, 4)), dma((nb,)), dma((nb,)), dma((nb,)), dma((nb,)), dma((nb,)), dma((3,)),
    ]
    flops = 2 * t * (d * (qw + 2 * HEAD) + qw * t + tp * qw * d // 2 + 3 * d * f)
    return pl.pallas_call(
        functools.partial(_kernel, tp, dp, l1, l2, w2, w3),
        name="layer",
        out_shape=(
            jax.ShapeDtypeStruct((t, d), BF),
            jax.ShapeDtypeStruct((t, HEAD), BF),
            jax.ShapeDtypeStruct((t, HEAD), BF),
            jax.ShapeDtypeStruct((t, tp * qw), BF),
        ),
        in_specs=[hbm, hbm, vm, vm, vm] + [hbm] * 7,
        out_specs=(hbm, hbm, hbm, hbm),
        scratch_shapes=scratch,
        compiler_params=pltpu.CompilerParams(
            collective_id=0, has_side_effects=True, vmem_limit_bytes=66 * 1000 * 1000),
        cost_estimate=pl.CostEstimate(flops=flops, bytes_accessed=8 * t * d, transcendentals=t * t * hl),
    )(x, posf, inv, g1, g2, wq, wk, wv, wo, wg, wu, wd)


def solution(mesh):
    tp = mesh.shape["tp"]
    dp = mesh.shape["dp"]

    def local(x, pos, g1, g2, wq, wk, wv, wo, wg, wu, wd):
        t, d = x.shape
        half = HEAD // 2
        inv = ROPE_BASE ** (-2.0 * jnp.arange(half, dtype=F32) / HEAD)
        inv = jnp.concatenate([inv, inv])[None, :]
        posf = jnp.broadcast_to(pos.astype(F32)[:, None], (t, HEAD))
        y, k, v, _ = _layer(tp, dp, x, posf, inv, g1[None, :], g2[None, :], wq, wk, wv, wo, wg, wu, wd)
        return y, k.reshape(t, 1, HEAD), v.reshape(t, 1, HEAD)

    return jax.shard_map(
        local,
        mesh=mesh,
        in_specs=(P("dp", None), P("dp"), P(), P(), P(None, "tp"), P(), P(), P("tp", None),
                  P(None, "tp"), P(None, "tp"), P("tp", None)),
        out_specs=(P("dp", None), P("dp", "tp", None), P("dp", "tp", None)),
        check_vma=False,
    )
```

```python
import functools

import jax
import jax.numpy as jnp
import numpy as np
from jax import lax
from jax.experimental import pallas as pl
from jax.experimental.pallas import tpu as pltpu
from jax.sharding import PartitionSpec as P

HEAD = 128
EPS = 1e-5
ROPE_BASE = 500000.0
MESH = pl.DeviceIdType.MESH
BLOCK = 256
NR = 64
BF = jnp.bfloat16
F32 = jnp.float32


def _sincos(ang):
    n = jnp.floor(ang * 0.6366197723675814 + 0.5)
    r = ((ang - n * 1.5703125) - n * 4.837512969970703125e-4) - n * 7.54978995489188216e-8
    z = r * r
    s = ((-1.9515295891e-4 * z + 8.3321608736e-3) * z - 1.6666654611e-1) * z * r + r
    c = ((2.443315711809948e-5 * z - 1.388731625493765e-3) * z + 4.166664568298827e-2) * z * z - 0.5 * z + 1.0
    m = n.astype(jnp.int32)
    odd = (m & 1) == 1
    cs = jnp.where(odd, s, c)
    sn = jnp.where(odd, c, s)
    cs = jnp.where(((m + 1) & 2) == 2, -cs, cs)
    sn = jnp.where((m & 2) == 2, -sn, sn)
    return cs, sn


def _kernel(tp, dp, l1, l2, w2, w3,
            x_ref, pos_ref, inv_ref, g1_ref, g2_ref, wq_ref, wk_ref, wv_ref, wo_ref, wg_ref, wu_ref, wd_ref,
            y_ref, k_ref, v_ref, oall_ref,
            wqkv, wo_v, wg_v, wu_v, wd_v, x_buf, g_scr, a_buf, q_scr, k_scr, v_scr, m_scr, l_scr, acc_scr, o_buf,
            o_blk, xh, hbuf, u_buf, r_buf, rsib, cp, rs1, rs2, sums, ych, hst,
            ld_w, ld_mlp, ld_x, kv_s,
            wo_a, wo_rel_s, wo_rel_r, wo_z_s, wo_z_r,
            o_s, o_rl, o_rr, o_rlr, o_rrr, o_rs, o_rel,
            ld_o, h_s, h_r, r_s, r_r, s1_s, s1_r, s2_s, s2_r, y_s, y_rl, y_rr, y_rlr, y_rrr, y_rs, y_rel):
    t, d = x_ref.shape
    qw = wq_ref.shape[1]
    f = wg_ref.shape[1]
    hl = qw // HEAD
    b = BLOCK
    nb = t // b
    dh = d // 2
    hb = b // 2
    nc = tp // 2
    ow = hb // nc
    hw = ow // 2
    kvt = min(2 * b, t)

    r = lax.axis_index("tp")
    c = r // 2
    s = r % 2
    c_r = (c + 1) % nc
    c_l = (c + nc - 1) % nc
    c_o = (c + 2) % nc
    right = {"tp": c_r * 2 + s}
    left = {"tp": c_l * 2 + s}
    sib = {"tp": c * 2 + 1 - s}
    share = dp % 2 == 0
    dpi = lax.axis_index("dp")
    par = dpi % 2
    peer = {"dp": dpi + 1 - 2 * par}

    def al(v, m):
        return pl.multiple_of(v, m)

    def send(src, dst, ss, rs, dev):
        pltpu.make_async_remote_copy(
            src_ref=src, dst_ref=dst, send_sem=ss, recv_sem=rs, device_id=dev, device_id_type=MESH).start()

    def put(src, dst, sem):
        pltpu.make_async_copy(src, dst, sem).start()

    def wait(region, sem, tag=None):
        if tag is None:
            pltpu.make_async_copy(region, region, sem).wait()
        else:
            with jax.named_scope("w_" + tag):
                pltpu.make_async_copy(region, region, sem).wait()

    barrier = pltpu.get_barrier_semaphore()
    others = [right, left, sib] + ([peer] if share else [])
    for dev in others:
        pl.semaphore_signal(barrier, inc=1, device_id=dev, device_id_type=MESH)
    pl.semaphore_wait(barrier, len(others))

    ro = al(r * qw, 128)
    mine = al(s * dh, 128)
    other = al((1 - s) * dh, 128)
    send(wo_ref.at[:, pl.ds(other, dh)], wo_v.at[pl.ds(ro, qw)], wo_a.at[0], wo_a.at[1], sib)
    put(wo_ref.at[:, pl.ds(mine, dh)], wo_v.at[pl.ds(ro, qw)], wo_a.at[2])
    put(x_ref.at[pl.ds(0, b)], x_buf.at[0], ld_x.at[0])
    rk = al(r * HEAD, 128)
    put(wq_ref, wqkv.at[:, pl.ds(0, qw)], ld_w.at[0])
    put(wk_ref.at[:, pl.ds(rk, HEAD)], wqkv.at[:, pl.ds(qw, HEAD)], ld_w.at[1])
    put(wv_ref.at[:, pl.ds(rk, HEAD)], wqkv.at[:, pl.ds(qw + HEAD, HEAD)], ld_w.at[2])
    wr = qw if share else 2 * qw
    woff = par * qw if share else 0

    def wrow(chip, half=None):
        base = al(chip * (2 * qw) + woff, 64)
        if half is None:
            return wo_v.at[pl.ds(base, wr)]
        return wo_v.at[pl.ds(al(base + half * (wr // 2), 64), wr // 2)]

    rs_sib = al((r + 1 - 2 * s) * qw, 128)
    wait(wo_v.at[pl.ds(rs_sib, qw)], wo_a.at[1], "wo")
    wait(wo_v.at[pl.ds(ro, qw)], wo_a.at[2])
    send(wrow(c), wrow(c), wo_a.at[3], wo_a.at[4], right)
    send(wrow(c), wrow(c), wo_a.at[5], wo_a.at[6], left)

    def wo_stage2():
        wait(wrow(c_l), wo_a.at[4], "wo2")
        send(wrow(c_l, 0), wrow(c_l, 0), wo_rel_s.at[0], wo_rel_r.at[0], right)
        if share:
            send(wrow(c_l), wrow(c_l), wo_z_s, wo_z_r, peer)
        wait(wrow(c_r), wo_a.at[6], "wo2")
        send(wrow(c_r, 1), wrow(c_r, 1), wo_rel_s.at[1], wo_rel_r.at[1], left)
        if share:
            send(wrow(c_r), wrow(c_r), wo_z_s, wo_z_r, peer)

    def wo_stage3():
        wait(wrow(c_o, 0), wo_rel_r.at[0], "wo3")
        wait(wrow(c_o, 1), wo_rel_r.at[1], "wo3")
        if share:
            send(wrow(c_o), wrow(c_o), wo_z_s, wo_z_r, peer)

    def ocol(chip, core):
        return pl.ds(al((chip * 2 + core) * qw, 128), qw)

    def orow(j):
        return pl.ds(al(j * b, b), b)

    def orow_half(j, half):
        return pl.ds(al(j * b + half * hb, hb), hb)

    def o_stage2(j):
        @pl.when((j >= 0) & (j < nb))
        def _():
            reg = oall_ref.at[orow(j), ocol(c_l, s)]
            top = oall_ref.at[orow_half(j, 0), ocol(c_l, s)]
            wait(reg, o_rl.at[j], "o2")
            send(top, top, o_rel.at[0], o_rlr.at[j], right)
            send(reg, reg, o_rel.at[2], o_rs.at[j], sib)
            reg = oall_ref.at[orow(j), ocol(c_r, s)]
            bot = oall_ref.at[orow_half(j, 1), ocol(c_r, s)]
            wait(reg, o_rr.at[j], "o2")
            send(bot, bot, o_rel.at[1], o_rrr.at[j], left)
            send(reg, reg, o_rel.at[2], o_rs.at[j], sib)

    def o_stage3(j):
        @pl.when((j >= 0) & (j < nb))
        def _():
            top = oall_ref.at[orow_half(j, 0), ocol(c_o, s)]
            bot = oall_ref.at[orow_half(j, 1), ocol(c_o, s)]
            reg = oall_ref.at[orow(j), ocol(c_o, s)]
            wait(top, o_rlr.at[j], "o3")
            wait(bot, o_rrr.at[j], "o3")
            send(reg, reg, o_rel.at[2], o_rs.at[j], sib)

    def unrolled(n, body):
        for e in range(n):
            body(e, 0)

    def norm_rows(src, which):
        def step(e, carry):
            for q in range(NR // 16):
                rows = pl.ds(al(e * NR + q * 16, 16), 16)
                v32 = src[rows, :].astype(F32)
                inv = lax.rsqrt(jnp.mean(v32 * v32, axis=1, keepdims=True) + EPS)
                a_buf[rows, :] = (v32 * inv * g_scr[which]).astype(BF)
            return carry

        lax.fori_loop(0, b // NR, step, 0)

    g_scr[0] = g1_ref[...].astype(F32).reshape(1, d)
    g_scr[1] = g2_ref[...].astype(F32).reshape(1, d)

    scale = HEAD ** -0.5 * 1.4426950408889634
    for h in range(t // kvt):
        v_scr[h * kvt:(h + 1) * kvt, :] = jnp.zeros((kvt, HEAD), BF)
        k_scr[h * kvt:(h + 1) * kvt, :] = jnp.zeros((kvt, HEAD), BF)
    wait(wqkv.at[:, pl.ds(0, qw)], ld_w.at[0])
    wait(wqkv.at[:, pl.ds(qw, HEAD)], ld_w.at[1])
    wait(wqkv.at[:, pl.ds(qw, HEAD)], ld_w.at[2])
    lane = lax.broadcasted_iota(jnp.int32, (b, HEAD), 1)

    def tile(i, j, masked):
        keys = pl.ds(al(j * kvt, kvt), kvt)
        kk = k_scr[keys, :]
        vv = v_scr[keys, :]
        sc = lax.dot_general(q_scr[...], kk, (((1,), (1,)), ((), ())), preferred_element_type=F32)
        if masked:
            rows = i * b + lax.broadcasted_iota(jnp.int32, (b, kvt), 0)
            cols = j * kvt + lax.broadcasted_iota(jnp.int32, (b, kvt), 1)
            keep = cols <= rows
            sc = jnp.concatenate([jnp.where(keep, sc[h * b:(h + 1) * b], -jnp.inf) for h in range(hl)], axis=0)
        m_prev = m_scr[...]
        m_new = jnp.maximum(m_prev, jnp.max(sc, axis=1, keepdims=True))
        parts = [jnp.exp2((sc[:, e * HEAD:(e + 1) * HEAD] - m_new) * scale) for e in range(kvt // HEAD)]
        alpha = jnp.exp2((m_prev - m_new) * scale)
        l_scr[...] = l_scr[...] * alpha + functools.reduce(lambda p, q: p + q, parts)
        pr = jnp.concatenate([p.astype(BF) for p in parts], axis=1)
        acc_scr[...] = acc_scr[...] * alpha + jnp.dot(pr, vv, preferred_element_type=F32)
        m_scr[...] = m_new

    def phase1(i, carry):
        with jax.named_scope("slot1"):
            return phase1_slot(i, carry)

    def phase1_slot(i, carry):
        slot = i % 2
        wait(x_buf.at[slot], ld_x.at[slot], "x")

        @pl.when(i + 1 < nb)
        def _():
            put(x_ref.at[pl.ds(al((i + 1) * b, b), b)], x_buf.at[1 - slot], ld_x.at[1 - slot])

        with jax.named_scope("norm1"):
            norm_rows(x_buf.at[slot], 0)
        pcol = []
        for e in range(b // 128):
            prow = pos_ref[pl.ds(i * (b // 128) + e, 1), :].astype(F32)
            pcol.append(jnp.transpose(jnp.broadcast_to(prow, (128, 128))))
        co, si = _sincos(jnp.concatenate(pcol, axis=0) * inv_ref[...])
        si = jnp.where(lane < HEAD // 2, -si, si)
        q32 = jnp.dot(a_buf[...], wqkv[:, 0:qw + HEAD], preferred_element_type=F32)
        v32 = jnp.dot(a_buf[...], wqkv[:, qw + HEAD:qw + 2 * HEAD], preferred_element_type=F32)

        def rope(v32):
            return (v32 * co + pltpu.roll(v32, HEAD // 2, 1) * si).astype(BF)

        rows = pl.ds(al(i * b, b), b)
        for h in range(hl):
            q_scr[h * b:(h + 1) * b, :] = rope(q32[:, h * HEAD:(h + 1) * HEAD])
        k_scr[rows, :] = rope(q32[:, qw:qw + HEAD])
        v_scr[rows, :] = v32.astype(BF)
        m_scr[...] = jnp.full((hl * b, HEAD), -jnp.inf, F32)
        l_scr[...] = jnp.zeros((hl * b, HEAD), F32)
        acc_scr[...] = jnp.zeros((hl * b, HEAD), F32)
        last = (i * b) // kvt

        def inner(j, carry):
            tile(i, j, False)
            return carry

        with jax.named_scope("tiles"):
            lax.fori_loop(0, last, inner, 0)
        tile(i, last, True)
        for h in range(hl):
            o_buf[rows, h * HEAD:(h + 1) * HEAD] = (
                acc_scr[h * b:(h + 1) * b, :] / jnp.sum(l_scr[h * b:(h + 1) * b, :], axis=1, keepdims=True)).astype(BF)
        src = o_buf.at[rows]
        dst = oall_ref.at[orow(i), ocol(c, s)]
        send(src, dst, o_s.at[0], o_rl.at[i], right)
        send(src, dst, o_s.at[1], o_rr.at[i], left)
        send(src, dst, o_s.at[2], o_rs.at[i], sib)
        put(src, dst, o_s.at[3])

        @pl.when(i == 1)
        def _():
            put(wg_ref, wg_v, ld_mlp.at[0])
            put(wu_ref, wu_v, ld_mlp.at[1])
            put(wd_ref, wd_v, ld_mlp.at[2])

        @pl.when(i == w2)
        def _():
            wo_stage2()

        @pl.when(i == w3)
        def _():
            wo_stage3()

        o_stage2(i - l1)
        o_stage3(i - l2)
        return carry

    lax.fori_loop(0, nb, phase1, 0)
    put(k_scr, k_ref, kv_s.at[0])
    put(v_scr, v_ref, kv_s.at[1])
    wait(o_buf, o_s.at[3])
    wait(wg_v, ld_mlp.at[0])
    wait(wu_v, ld_mlp.at[1])
    wait(wd_v, ld_mlp.at[2])
    if share:
        wait(wo_v.at[pl.ds(0, 3 * wr)], wo_z_r, "woz")

    def load_o(j):
        wait(oall_ref.at[orow(j), pl.ds(0, 4 * qw)], o_rs.at[j], "os")
        put(oall_ref.at[orow(j)], o_blk, ld_o.at[0])
        put(x_ref.at[orow(j), pl.ds(mine, dh)], xh, ld_o.at[1])

    nt_h = min(512, dh)
    nt_f = min(512, f)
    nt_d = min(512, d)

    def sum_start(j):
        @pl.when((j >= 0) & (j < nb))
        def _():
            two = j % 2
            q4 = j % 4
            wait(rsib.at[two], r_r.at[two], "r")
            wait(rsib.at[two], r_s, "rs")

            def add(e, carry):
                rows = pl.ds(al(e * 16, 16), 16)
                own = r_buf[pl.ds(al(s * hb + e * 16, 16), 16), :]
                cp[q4, rows, :] = (own.astype(F32) + rsib[two, rows, :].astype(F32)).astype(BF)
                return carry

            with jax.named_scope("add"):
                lax.fori_loop(0, hb // 16, add, 0)

            def part(chip, half):
                return cp.at[q4, pl.ds(al(chip * ow + half * hw, hw), hw)]

            send(part(c_o, 0), rs1.at[q4, 0], s1_s.at[q4, 0], s1_r.at[q4, 0], right)
            send(part(c_o, 1), rs1.at[q4, 2], s1_s.at[q4, 2], s1_r.at[q4, 2], left)
            send(part(c_r, 1), rs1.at[q4, 1], s1_s.at[q4, 1], s1_r.at[q4, 1], right)
            send(part(c_l, 0), rs1.at[q4, 3], s1_s.at[q4, 3], s1_r.at[q4, 3], left)

    def own_h(j):
        @pl.when(j < nb)
        def _():
            two = j % 2
            wait(o_blk, ld_o.at[0], "ldo")
            wait(xh, ld_o.at[1], "ldo")

            def col(n, carry):
                cols = pl.ds(n * nt_h, nt_h)
                v32 = jnp.dot(o_blk[...], wo_v[:, cols], preferred_element_type=F32)
                hbuf[two, :, pl.ds(al(s * dh + n * nt_h, 128), nt_h)] = (xh[:, cols].astype(F32) + v32).astype(BF)
                return carry

            with jax.named_scope("own_h"):
                unrolled(dh // nt_h, col)

    def swap_h(j):
        @pl.when(j < nb)
        def _():
            two = j % 2
            half = hbuf.at[two, :, pl.ds(mine, dh)]
            send(half, half, h_s.at[two], h_r.at[two], sib)

        @pl.when(j + 1 < nb)
        def _():
            load_o(j + 1)

    def mlp_norm(j):
        @pl.when((j >= 0) & (j < nb))
        def _():
            two = j % 2
            wait(hbuf.at[two, :, pl.ds(other, dh)], h_r.at[two], "h")
            wait(hbuf.at[two, :, pl.ds(mine, dh)], h_s.at[two], "hs")

            with jax.named_scope("norm2"):
                norm_rows(hbuf.at[two], 1)
            hst[j % 4] = hbuf[two, pl.ds(al(s * hb + c * ow, 16), ow), :]

    def mlp_up(j):
        @pl.when((j >= 0) & (j < nb))
        def _():
            def col(n, carry):
                cols = pl.ds(n * nt_f, nt_f)
                gt = jnp.dot(a_buf[...], wg_v[:, cols], preferred_element_type=F32)
                up = jnp.dot(a_buf[...], wu_v[:, cols], preferred_element_type=F32)
                u_buf[:, cols] = (gt * (1.0 / (1.0 + jnp.exp(-gt))) * up).astype(BF)
                return carry

            with jax.named_scope("up"):
                unrolled(f // nt_f, col)

    def mlp_down(j):
        @pl.when((j >= 0) & (j < nb))
        def _():
            def col(n, carry):
                cols = pl.ds(n * nt_d, nt_d)
                r_buf[:, cols] = jnp.dot(u_buf[...], wd_v[:, cols], preferred_element_type=F32).astype(BF)
                return carry

            with jax.named_scope("down"):
                unrolled(d // nt_d, col)
            send(r_buf.at[pl.ds(al((1 - s) * hb, hb), hb)], rsib.at[j % 2], r_s, r_r.at[j % 2], sib)

    def sum_relay(j):
        @pl.when((j >= 0) & (j < nb))
        def _():
            q4 = j % 4

            @pl.when(j >= 4)
            def _():
                wait(sums.at[q4, 0], s2_s.at[q4, 0])
                wait(sums.at[q4, 1], s2_s.at[q4, 1])

            wait(rs1.at[q4, 0], s1_r.at[q4, 0], "s1")
            sums[q4, 0] = (rs1[q4, 0].astype(F32) + cp[q4, pl.ds(al(c_r * ow, 16), hw), :].astype(F32)).astype(BF)
            send(sums.at[q4, 0], rs2.at[q4, 0], s2_s.at[q4, 0], s2_r.at[q4, 0], right)
            wait(rs1.at[q4, 2], s1_r.at[q4, 2], "s1")
            sums[q4, 1] = (rs1[q4, 2].astype(F32) + cp[q4, pl.ds(al(c_l * ow + hw, 16), hw), :].astype(F32)).astype(BF)
            send(sums.at[q4, 1], rs2.at[q4, 1], s2_s.at[q4, 1], s2_r.at[q4, 1], left)

    def yrow(j, core, chip):
        return y_ref.at[pl.ds(al(j * b + core * hb + chip * ow, ow), ow)]

    def yrow_half(j, core, chip, half):
        return y_ref.at[pl.ds(al(j * b + core * hb + chip * ow + half * hw, hw), hw)]

    def sum_end(j):
        @pl.when((j >= 0) & (j < nb))
        def _():
            q4 = j % 4

            @pl.when(j >= 4)
            def _():
                for e in range(4):
                    wait(ych.at[q4], y_s.at[q4, e])

            for e in range(4):
                wait(rs1.at[q4, e], s1_s.at[q4, e], "s1s")
            wait(rs1.at[q4, 1], s1_r.at[q4, 1], "s2")
            wait(rs1.at[q4, 3], s1_r.at[q4, 3], "s2")
            wait(rs2.at[q4, 0], s2_r.at[q4, 0], "s2")
            wait(rs2.at[q4, 1], s2_r.at[q4, 1], "s2")
            for half, (near, far) in enumerate(((3, 0), (1, 1))):
                own = cp[q4, pl.ds(al(c * ow + half * hw, 16), hw), :].astype(F32)
                tot = own + rs1[q4, near].astype(F32) + rs2[q4, far].astype(F32)
                hh = hst[q4, half * hw:(half + 1) * hw, :].astype(F32)
                ych[q4, half * hw:(half + 1) * hw, :] = (hh + tot).astype(BF)
            dst = yrow(j, s, c)
            send(ych.at[q4], dst, y_s.at[q4, 0], y_rl.at[j], right)
            send(ych.at[q4], dst, y_s.at[q4, 1], y_rr.at[j], left)
            send(ych.at[q4], dst, y_s.at[q4, 2], y_rs.at[j], sib)
            put(ych.at[q4], dst, y_s.at[q4, 3])

    def y_stage2(j):
        @pl.when((j >= 0) & (j < nb))
        def _():
            reg = yrow(j, s, c_l)
            top = yrow_half(j, s, c_l, 0)
            wait(reg, y_rl.at[j], "y2")
            send(top, top, y_rel.at[0], y_rlr.at[j], right)
            send(reg, reg, y_rel.at[2], y_rs.at[j], sib)
            reg = yrow(j, s, c_r)
            bot = yrow_half(j, s, c_r, 1)
            wait(reg, y_rr.at[j], "y2")
            send(bot, bot, y_rel.at[1], y_rrr.at[j], left)
            send(reg, reg, y_rel.at[2], y_rs.at[j], sib)

    def y_stage3(j):
        @pl.when((j >= 0) & (j < nb))
        def _():
            wait(yrow_half(j, s, c_o, 0), y_rlr.at[j], "y3")
            wait(yrow_half(j, s, c_o, 1), y_rrr.at[j], "y3")
            reg = yrow(j, s, c_o)
            send(reg, reg, y_rel.at[2], y_rs.at[j], sib)

    load_o(0)

    def phase2(i, carry):
        with jax.named_scope("slot2"):
            return phase2_slot(i, carry)

    def phase2_slot(i, carry):
        own_h(i)
        sum_start(i - 2)
        swap_h(i)
        mlp_norm(i - 1)
        sum_relay(i - 3)
        mlp_up(i - 1)
        sum_end(i - 4)
        mlp_down(i - 1)
        y_stage2(i - 5)
        y_stage3(i - 6)
        o_stage2(nb + i - l1)
        o_stage3(nb + i - l2)
        return carry

    lax.fori_loop(0, nb + 6, phase2, 0)

    def drain(j, carry):
        wait(y_ref.at[pl.ds(0, hb)], y_rs.at[j], "ys")
        return carry

    lax.fori_loop(0, nb, drain, 0)
    for q4 in range(4):
        for e in range(4):
            wait(ych.at[q4], y_s.at[q4, e])
        for e in range(2):
            wait(sums.at[q4, e], s2_s.at[q4, e])
    wait(y_ref.at[pl.ds(0, nb * hw)], y_rel.at[0])
    wait(y_ref.at[pl.ds(0, nb * hw)], y_rel.at[1])
    wait(y_ref.at[pl.ds(0, nb * ow * 3)], y_rel.at[2])
    for e in range(3):
        wait(o_buf, o_s.at[e])
    wait(oall_ref.at[pl.ds(0, t // 2), pl.ds(0, qw)], o_rel.at[0])
    wait(oall_ref.at[pl.ds(0, t // 2), pl.ds(0, qw)], o_rel.at[1])
    wait(oall_ref.at[:, pl.ds(0, 3 * qw)], o_rel.at[2])
    wait(wo_v.at[pl.ds(0, qw)], wo_a.at[0])
    wait(wo_v.at[pl.ds(0, wr)], wo_a.at[3])
    wait(wo_v.at[pl.ds(0, wr)], wo_a.at[5])
    for e in range(2):
        wait(wo_v.at[pl.ds(0, wr // 2)], wo_rel_s.at[e])
    if share:
        wait(wo_v.at[pl.ds(0, 3 * wr)], wo_z_s)
    wait(k_scr, kv_s.at[0])
    wait(v_scr, kv_s.at[1])


def _layer(tp, dp, x, pos, inv, g1, g2, wq, wk, wv, wo, wg, wu, wd):
    t, d = x.shape
    qw = wq.shape[1]
    f = wg.shape[1]
    hl = qw // HEAD
    b = BLOCK
    nb = t // b
    hb = b // 2
    nc = tp // 2
    ow = hb // nc
    hw = ow // 2
    assert nc == 4 and t % b == 0 and wk.shape[1] == tp * HEAD
    l1 = min(nb * 3 // 8, nb - 3)
    l2 = min(nb * 3 // 4, nb - 2)
    w2 = nb * 5 // 16
    w3 = nb * 9 // 16
    dma = pltpu.SemaphoreType.DMA
    hbm = pl.BlockSpec(memory_space=pl.ANY)
    vm = pl.BlockSpec(memory_space=pltpu.VMEM)
    scratch = [
        pltpu.VMEM((d, qw + 2 * HEAD), BF),
        pltpu.VMEM((tp * qw, d // 2), BF),
        pltpu.VMEM((d, f), BF),
        pltpu.VMEM((d, f), BF),
        pltpu.VMEM((f, d), BF),
        pltpu.VMEM((2, b, d), BF),
        pltpu.VMEM((2, 1, d), F32),
        pltpu.VMEM((b, d), BF),
        pltpu.VMEM((hl * b, HEAD), BF),
        pltpu.VMEM((t, HEAD), BF),
        pltpu.VMEM((t, HEAD), BF),
        pltpu.VMEM((hl * b, HEAD), F32),
        pltpu.VMEM((hl * b, HEAD), F32),
        pltpu.VMEM((hl * b, HEAD), F32),
        pltpu.VMEM((t, qw), BF),
        pltpu.VMEM((b, tp * qw), BF),
        pltpu.VMEM((b, d // 2), BF),
        pltpu.VMEM((2, b, d), BF),
        pltpu.VMEM((b, f), BF),
        pltpu.VMEM((b, d), BF),
        pltpu.VMEM((2, hb, d), BF),
        pltpu.VMEM((4, hb, d), BF),
        pltpu.VMEM((4, 4, hw, d), BF),
        pltpu.VMEM((4, 2, hw, d), BF),
        pltpu.VMEM((4, 2, hw, d), BF),
        pltpu.VMEM((4, ow, d), BF),
        pltpu.VMEM((4, ow, d), BF),
        dma((3,)), dma((3,)), dma((2,)), dma((2,)),
        dma((7,)), dma((2,)), dma((2,)), dma(()), dma(()),
        dma((4,)), dma((nb,)), dma((nb,)), dma((nb,)), dma((nb,)), dma((nb,)), dma((3,)),
        dma((2,)), dma((2,)), dma((2,)), dma(()), dma((2,)), dma((4, 4)), dma((4, 4)), dma((4, 2)), dma((4, 2)),
        dma((4, 4)), dma((nb,)), dma((nb,)), dma((nb,)), dma((nb,)), dma((nb,)), dma((3,)),
    ]
    flops = 2 * t * (d * (qw + 2 * HEAD) + qw * t + tp * qw * d // 2 + 3 * d * f)
    return pl.pallas_call(
        functools.partial(_kernel, tp, dp, l1, l2, w2, w3),
        name="layer",
        out_shape=(
            jax.ShapeDtypeStruct((t, d), BF),
            jax.ShapeDtypeStruct((t, HEAD), BF),
            jax.ShapeDtypeStruct((t, HEAD), BF),
            jax.ShapeDtypeStruct((t, tp * qw), BF),
        ),
        in_specs=[hbm, vm, vm, vm, vm] + [hbm] * 7,
        out_specs=(hbm, hbm, hbm, hbm),
        scratch_shapes=scratch,
        compiler_params=pltpu.CompilerParams(
            collective_id=0, has_side_effects=True, vmem_limit_bytes=66 * 1000 * 1000),
        cost_estimate=pl.CostEstimate(flops=flops, bytes_accessed=8 * t * d, transcendentals=t * t * hl),
    )(x, pos, inv, g1, g2, wq, wk, wv, wo, wg, wu, wd)


def _copy_kernel(src, k_src, v_src, dst, k_dst, v_dst, buf, kv, rd, wr, kv_sem):
    n, rows = buf.shape[0], buf.shape[1]
    steps = src.shape[0] // rows

    def read(i):
        return pltpu.make_async_copy(src.at[pl.ds(i * rows, rows)], buf.at[i % n], rd.at[i % n])

    def write(i):
        return pltpu.make_async_copy(buf.at[i % n], dst.at[pl.ds(i * rows, rows)], wr.at[i % n])

    small = [(k_src, k_dst), (v_src, v_dst)]
    kv_in = [pltpu.make_async_copy(a, kv.at[e], kv_sem.at[e]) for e, (a, _) in enumerate(small)]
    kv_out = [pltpu.make_async_copy(kv.at[e], z, kv_sem.at[e]) for e, (_, z) in enumerate(small)]
    for i in range(min(n, steps)):
        read(i).start()
    for e in range(2):
        kv_in[e].start()
    for i in range(steps):
        read(i).wait()
        write(i).start()
        if i >= 1 and i - 1 + n < steps:
            write(i - 1).wait()
            read(i - 1 + n).start()
    for e in range(2):
        kv_in[e].wait()
        kv_out[e].start()
    for i in range(max(0, steps - n), steps):
        write(i).wait()
    for e in range(2):
        kv_out[e].wait()


def _copy(y, k, v):
    t, d = y.shape
    rows, n = min(256, t), min(16, t // 256)
    hbm = pl.BlockSpec(memory_space=pl.ANY)
    dma = pltpu.SemaphoreType.DMA
    return pl.pallas_call(
        _copy_kernel,
        name="copy_out",
        out_shape=tuple(jax.ShapeDtypeStruct(a.shape, a.dtype) for a in (y, k, v)),
        in_specs=[hbm] * 3,
        out_specs=(hbm,) * 3,
        scratch_shapes=[pltpu.VMEM((n, rows, d), y.dtype), pltpu.VMEM((2,) + k.shape, k.dtype),
                        dma((n,)), dma((n,)), dma((2,))],
        compiler_params=pltpu.CompilerParams(vmem_limit_bytes=66 * 1000 * 1000),
        cost_estimate=pl.CostEstimate(flops=0, bytes_accessed=4 * t * d, transcendentals=0),
    )(y, k, v)


def solution(mesh):
    tp = mesh.shape["tp"]
    dp = mesh.shape["dp"]

    def local(x, pos, g1, g2, wq, wk, wv, wo, wg, wu, wd):
        t, d = x.shape
        half = ROPE_BASE ** (-2.0 * np.arange(HEAD // 2) / HEAD)
        inv = jnp.asarray(np.concatenate([half, half])[None, :].astype(np.float32))
        y, k, v, _ = _layer(tp, dp, x, pos.reshape(t // 128, 128), inv, g1, g2, wq, wk, wv, wo, wg, wu, wd)
        y, k, v = _copy(y, k, v)
        return y, k.reshape(t, 1, HEAD), v.reshape(t, 1, HEAD)

    return jax.shard_map(
        local,
        mesh=mesh,
        in_specs=(P("dp", None), P("dp"), P(), P(), P(None, "tp"), P(), P(), P("tp", None),
                  P(None, "tp"), P(None, "tp"), P("tp", None)),
        out_specs=(P("dp", None), P("dp", "tp", None), P("dp", "tp", None)),
        check_vma=False,
    )
```

```python
import functools

import jax
import jax.numpy as jnp
import numpy as np
from jax import lax
from jax.experimental import pallas as pl
from jax.experimental.pallas import tpu as pltpu
from jax.sharding import PartitionSpec as P

HEAD = 128
LANES = 128
SUB = 16
EPS = 1e-5
ROPE_BASE = 500000.0
MESH = pl.DeviceIdType.MESH
BLOCK = 256
NR = 64
SLOTS = 4
SIDES = (0, 1)
BF = jnp.bfloat16
F32 = jnp.float32
VMEM_BYTES = 66000000
TWO_OVER_PI = 0.6366197723675814
PI_2 = (1.5703125, 4.837512969970703125e-4, 7.54978995489188216e-8)
SIN = (-1.9515295891e-4, 8.3321608736e-3, -1.6666654611e-1)
COS = (2.443315711809948e-5, -1.388731625493765e-3, 4.166664568298827e-2)
LOG2E = 1.4426950408889634


def _sincos(ang):
    n = jnp.floor(ang * TWO_OVER_PI + 0.5)
    r = ang
    for p in PI_2:
        r = r - n * p
    z = r * r
    s = functools.reduce(lambda a, p: a * z + p, SIN[1:], SIN[0]) * z * r + r
    c = functools.reduce(lambda a, p: a * z + p, COS[1:], COS[0]) * z * z - 0.5 * z + 1.0
    m = n.astype(jnp.int32)
    odd = (m & 1) == 1
    cs = jnp.where(odd, s, c)
    sn = jnp.where(odd, c, s)
    return jnp.where(((m + 1) & 2) == 2, -cs, cs), jnp.where((m & 2) == 2, -sn, sn)


def _al(v, m):
    return pl.multiple_of(v, m)


def _first(ref, n):
    return ref.at[pl.ds(0, n)]


def _kernel(tp, dp, zn, l1, l2, w2, w3, w4,
            x_ref, pos_ref, inv_ref, g1_ref, g2_ref, wq_ref, wk_ref, wv_ref, wo_ref, wg_ref, wu_ref, wd_ref,
            y_ref, k_ref, v_ref, oall_ref,
            pos_v, inv_v, g1_v, g2_v, wqkv, wo_v, wg_v, wu_v, wd_v, x_buf, g_scr, a_buf, q_scr, k_scr, v_scr, m_scr, l_scr, acc_scr, o_buf,
            o_blk, xh, hbuf, u_buf, r_buf, rsib, cp, rs_far, rs_near, rs_sum, sums, ych, hst,
            ld_s, ld_w, ld_mlp, ld_x, kv_s,
            wo_d, wo_s, wo_r, wo_fs, wo_fr, wo_ps, wo_pr,
            o_s, o_sx, o_r, o_f, o_rs, o_rel, o_fwd,
            ld_o, h_s, h_r, r_s, r_r, far_s, far_r, near_s, near_r, sum_s, sum_r,
            y_s, y_sx, y_r, y_f, y_rs, y_rel, y_fwd):
    t, d = x_ref.shape
    qw = wq_ref.shape[1]
    f = wg_ref.shape[1]
    hl = qw // HEAD
    b = BLOCK
    nb = t // b
    dh = d // 2
    hb = b // 2
    nc = tp // 2
    ow = hb // nc
    hw = ow // 2
    kvt = 2 * b

    r = lax.axis_index("tp")
    c = r // 2
    s = r % 2
    c_r = (c + 1) % nc
    c_l = (c + nc - 1) % nc
    c_o = (c + 2) % nc
    dest = ({"tp": c_r * 2 + s}, {"tp": c_l * 2 + s})
    origin = (c_l, c_r)
    target = (c_r, c_l)
    sib = {"tp": c * 2 + 1 - s}
    dpi = lax.axis_index("dp")
    par = dpi % 2
    peers = [{"dp": dpi + 1 - 2 * par}] if dp % 2 == 0 else []
    if zn:
        par_y = (dpi // zn) % 2
        peers.append({"dp": dpi + zn * (1 - 2 * par_y)})

    def send(src, dst, ss, rs, dev):
        pltpu.make_async_remote_copy(
            src_ref=src, dst_ref=dst, send_sem=ss, recv_sem=rs, device_id=dev, device_id_type=MESH).start()

    def put(src, dst, sem):
        pltpu.make_async_copy(src, dst, sem).start()

    def wait(region, sem, tag=None):
        with jax.named_scope("w_" + (tag or "end")):
            pltpu.make_async_copy(region, region, sem).wait()

    def when_block(j, body):
        @pl.when((j >= 0) & (j < nb))
        def _():
            body()

    barrier = pltpu.get_barrier_semaphore()
    cross = [{"tp": target[e] * 2 + 1 - s} for e in SIDES]
    others = [*dest, *cross, sib, *peers]
    for dev in others:
        pl.semaphore_signal(barrier, inc=1, device_id=dev, device_id_type=MESH)

    rk = _al(r * HEAD, HEAD)
    wq_dst = wqkv.at[:, pl.ds(0, qw)]
    kv_dst = [wqkv.at[:, pl.ds(qw + e * HEAD, HEAD)] for e in SIDES]
    small = ((pos_ref, pos_v), (inv_ref, inv_v), (g1_ref, g1_v), (g2_ref, g2_v))
    put(_first(x_ref, b), x_buf.at[0], ld_x.at[0])
    for e, (src, dst) in enumerate(small):
        put(src, dst, ld_s.at[e])
    put(wq_ref, wq_dst, ld_w.at[2])
    for e, ref in enumerate((wk_ref, wv_ref)):
        put(ref.at[:, pl.ds(rk, HEAD)], kv_dst[e], ld_w.at[e])
    with jax.named_scope("barrier"):
        pl.semaphore_wait(barrier, len(others))

    mine = _al(s * dh, LANES)
    other = _al((1 - s) * dh, LANES)
    parts = 4 if zn else len(peers) + 1
    wr = qw // parts
    part = (2 * par_y + par) if zn else (par if peers else 0)

    def shard(dev):
        return wo_v.at[pl.ds(_al(dev * qw, LANES), qw)]

    def piece(chip, core, q=None):
        return wo_v.at[pl.ds(_al((chip * 2 + core) * qw + (part if q is None else q) * wr, 32), wr)]

    rows = pl.ds(_al(part * wr, 32), wr)
    for e in SIDES:
        for k, (cols, dev) in enumerate(((mine, dest[e]), (other, cross[e]))):
            send(wo_ref.at[rows, pl.ds(cols, dh)], piece(c, s), wo_s.at[e, k], wo_r.at[e, s], dev)
    send(wo_ref.at[:, pl.ds(other, dh)], shard(r), wo_d.at[0], wo_d.at[1], sib)
    put(wo_ref.at[:, pl.ds(mine, dh)], shard(r), wo_d.at[2])

    def wo_swap(chip):
        for e, dev in enumerate(peers):
            for core in SIDES:
                send(piece(chip, core), piece(chip, core), wo_ps.at[0, e], wo_pr.at[0, e], dev)

    def wo_stage2():
        for e in SIDES:
            for core in SIDES:
                wait(piece(origin[e], core), wo_r.at[e, core], "wo2")
            reg = piece(origin[e], e)
            send(reg, reg, wo_fs.at[e], wo_fr.at[e], dest[e])
            wo_swap(origin[e])

    def wo_stage3():
        for e in SIDES:
            wait(piece(c_o, e), wo_fr.at[e], "wo3")
        wo_swap(c_o)

    def wo_stage4():
        for e in range(len(peers)):
            wait(_first(wo_v, 6 * wr), wo_pr.at[0, e], "wo4")
        if zn:
            for chip in (*origin, c_o):
                for e, q in enumerate((2 * (1 - par_y) + par, 2 * par_y + 1 - par)):
                    reg = piece(chip, e, q)
                    send(reg, reg, wo_ps.at[1, e], wo_pr.at[1, e], peers[e])

    def wo_end(which):
        for e in SIDES if zn else ():
            wait(_first(wo_v, 3 * wr), which.at[1, e], "wo5")

    def ocol(chip, core):
        return pl.ds(_al((chip * 2 + core) * qw, LANES), qw)

    def oreg(j, chip):
        return oall_ref.at[pl.ds(_al(j * b, b), b), ocol(chip, s)]

    def ohalf(j, chip, half):
        return oall_ref.at[pl.ds(_al(j * b + half * hb, hb), hb), ocol(chip, s)]

    def orow(j):
        return pl.ds(_al(j * b, b), b)

    def o_stage2(j):
        def body():
            for e in SIDES:
                reg = oreg(j, origin[e])
                wait(reg, o_r.at[e, j], "o2")
                half = ohalf(j, origin[e], e)
                send(half, half, o_rel.at[e], o_f.at[e, j], dest[e])
                send(reg, reg, o_fwd, o_rs.at[j], sib)

        when_block(j, body)

    def o_stage3(j):
        def body():
            for e in SIDES:
                wait(ohalf(j, c_o, e), o_f.at[e, j], "o3")
            send(oreg(j, c_o), oreg(j, c_o), o_fwd, o_rs.at[j], sib)

        when_block(j, body)

    def unrolled(n, body):
        for e in range(n):
            body(e)

    def norm_rows(src, which):
        def step(e, carry):
            for q in range(NR // SUB):
                rows = pl.ds(_al(e * NR + q * SUB, SUB), SUB)
                v32 = src[rows, :].astype(F32)
                inv = lax.rsqrt(jnp.mean(v32 * v32, axis=1, keepdims=True) + EPS)
                a_buf[rows, :] = (v32 * inv * g_scr[which]).astype(BF)
            return carry

        with jax.named_scope("norm"):
            lax.fori_loop(0, b // NR, step, 0)

    for e, (src, dst) in enumerate(small):
        wait(dst, ld_s.at[e], "small")
    for e, ref in enumerate((g1_v, g2_v)):
        g_scr[e] = ref[...].astype(F32).reshape(1, d)

    scale = HEAD ** -0.5 * LOG2E
    lane = lax.broadcasted_iota(jnp.int32, (b, HEAD), 1)

    def heads(ref, h):
        return ref.at[pl.ds(h * b, b)]

    def tile(first, n, masked=False):
        keys = pl.ds(_al(first, n), n)
        kk = k_scr[keys, :]
        vv = v_scr[keys, :]
        sc = lax.dot_general(q_scr[...], kk, (((1,), (1,)), ((), ())), preferred_element_type=F32)
        if masked:
            keep = lax.broadcasted_iota(jnp.int32, (b, n), 1) <= lax.broadcasted_iota(jnp.int32, (b, n), 0)
            sc = jnp.concatenate([jnp.where(keep, sc[h * b:(h + 1) * b], -jnp.inf) for h in range(hl)], axis=0)
        m_prev = m_scr[...]
        m_new = jnp.maximum(m_prev, jnp.max(sc, axis=1, keepdims=True))
        ps = [jnp.exp2((sc[:, e * HEAD:(e + 1) * HEAD] - m_new) * scale) for e in range(n // HEAD)]
        alpha = jnp.exp2((m_prev - m_new) * scale)
        l_scr[...] = l_scr[...] * alpha + functools.reduce(lambda p, q: p + q, ps)
        pr = jnp.concatenate([p.astype(BF) for p in ps], axis=1)
        acc_scr[...] = acc_scr[...] * alpha + jnp.dot(pr, vv, preferred_element_type=F32)
        m_scr[...] = m_new

    def phase1(i, carry):
        with jax.named_scope("slot1"):
            phase1_slot(i)
        return carry

    def phase1_slot(i):
        slot = i % 2
        wait(x_buf.at[slot], ld_x.at[slot], "x")

        @pl.when(i + 1 < nb)
        def _():
            put(x_ref.at[pl.ds(_al((i + 1) * b, b), b)], x_buf.at[1 - slot], ld_x.at[1 - slot])

        norm_rows(x_buf.at[slot], 0)

        @pl.when(i == 0)
        def _():
            wait(wq_dst, ld_w.at[2], "w")
            for e in SIDES:
                wait(kv_dst[e], ld_w.at[e], "w")

        for e, (src, dst) in enumerate(((wg_ref, wg_v), (wu_ref, wu_v), (wd_ref, wd_v))):
            @pl.when(i == w2 + e)
            def _(src=src, dst=dst, e=e):
                put(src, dst, ld_mlp.at[e])

        pcol = []
        for e in range(b // LANES):
            prow = pos_v[pl.ds(i * (b // LANES) + e, 1), :].astype(F32)
            pcol.append(jnp.transpose(jnp.broadcast_to(prow, (LANES, LANES))))
        co, si = _sincos(jnp.concatenate(pcol, axis=0) * inv_v[...])
        si = jnp.where(lane < HEAD // 2, -si, si)
        qk32 = jnp.dot(a_buf[...], wqkv[:, :qw + HEAD], preferred_element_type=F32)
        v32 = jnp.dot(a_buf[...], wqkv[:, qw + HEAD:], preferred_element_type=F32)
        rows = pl.ds(_al(i * b, b), b)
        for h in range(hl + 1):
            head = qk32[:, h * HEAD:(h + 1) * HEAD]
            head = (head * co + pltpu.roll(head, HEAD // 2, 1) * si).astype(BF)
            if h < hl:
                heads(q_scr, h)[...] = head
            else:
                k_scr[rows, :] = head
        v_scr[rows, :] = v32.astype(BF)
        m_scr[...] = jnp.full(m_scr.shape, -jnp.inf, F32)
        l_scr[...] = jnp.zeros(l_scr.shape, F32)
        acc_scr[...] = jnp.zeros(acc_scr.shape, F32)
        full = i // 2

        def inner(j, carry):
            for e in SIDES:
                tile((2 * j + e) * kvt, kvt)
            return carry

        with jax.named_scope("tiles"):
            lax.fori_loop(0, full // 2, inner, 0)

        @pl.when(full % 2 == 1)
        def _():
            tile((full - 1) * kvt, kvt)

        @pl.when(i % 2 == 1)
        def _():
            tile((i - 1) * b, b)

        tile(i * b, b, masked=True)
        for h in range(hl):
            o_buf[rows, h * HEAD:(h + 1) * HEAD] = (
                heads(acc_scr, h)[...] / jnp.sum(heads(l_scr, h)[...], axis=1, keepdims=True)).astype(BF)
        src = o_buf.at[rows]
        dst = oreg(i, c)
        for e in SIDES:
            send(src, dst, o_s.at[e], o_r.at[e, i], dest[e])
        send(src, dst, o_sx.at[0], o_rs.at[i], sib)
        put(src, dst, o_sx.at[1])
        for when, stage in ((w2, wo_stage2), (w3, wo_stage3), (w4, wo_stage4)):
            pl.when(i == when)(stage)
        o_stage2(i - l1)
        o_stage3(i - l2)

    lax.fori_loop(0, nb, phase1, 0)
    for e, (src, dst) in enumerate(((k_scr, k_ref), (v_scr, v_ref))):
        put(src, dst, kv_s.at[e])
    wait(o_buf, o_sx.at[1])
    for e, dst in enumerate((wg_v, wu_v, wd_v)):
        wait(dst, ld_mlp.at[e])
    wait(shard(r + 1 - 2 * s), wo_d.at[1])
    wait(shard(r), wo_d.at[2])
    wo_end(wo_pr)

    def load_o(j):
        wait(oall_ref.at[orow(j), pl.ds(0, 4 * qw)], o_rs.at[j], "os")
        put(oall_ref.at[orow(j)], o_blk, ld_o.at[0])
        put(x_ref.at[orow(j), pl.ds(mine, dh)], xh, ld_o.at[1])

    nt_h = min(512, dh)
    nt_f = min(512, f)
    nt_d = min(512, d)

    def cpart(q4, chip, half):
        return cp.at[q4, pl.ds(_al(chip * ow + half * hw, hw), hw)]

    def sum_start(j):
        def body():
            two = j % 2
            q4 = j % SLOTS
            wait(rsib.at[two], r_r.at[two], "r")
            wait(rsib.at[two], r_s, "rs")

            def add(e, carry):
                rows = pl.ds(_al(e * SUB, SUB), SUB)
                own = r_buf[pl.ds(_al(s * hb + e * SUB, SUB), SUB), :]
                cp[q4, rows, :] = (own.astype(F32) + rsib[two, rows, :].astype(F32)).astype(BF)
                return carry

            with jax.named_scope("add"):
                lax.fori_loop(0, hb // SUB, add, 0)
            for e in SIDES:
                send(cpart(q4, c_o, e), rs_far.at[q4, e], far_s.at[q4, e], far_r.at[q4, e], dest[e])
            for e in SIDES:
                send(cpart(q4, target[e], 1 - e), rs_near.at[q4, e], near_s.at[q4, e], near_r.at[q4, e], dest[e])

        when_block(j, body)

    def own_h(j):
        @pl.when(j < nb)
        def _():
            wait(o_blk, ld_o.at[0], "ldo")
            wait(xh, ld_o.at[1], "ldo")

            def col(n):
                cols = pl.ds(n * nt_h, nt_h)
                v32 = jnp.dot(o_blk[...], wo_v[:, cols], preferred_element_type=F32)
                hbuf[j % 2, :, pl.ds(_al(s * dh + n * nt_h, LANES), nt_h)] = (xh[:, cols].astype(F32) + v32).astype(BF)

            with jax.named_scope("own_h"):
                unrolled(dh // nt_h, col)

    def swap_h(j):
        @pl.when(j < nb)
        def _():
            half = hbuf.at[j % 2, :, pl.ds(mine, dh)]
            send(half, half, h_s.at[j % 2], h_r.at[j % 2], sib)

        @pl.when(j + 1 < nb)
        def _():
            load_o(j + 1)

    def mlp_norm(j):
        def body():
            two = j % 2
            wait(hbuf.at[two, :, pl.ds(other, dh)], h_r.at[two], "h")
            wait(hbuf.at[two, :, pl.ds(mine, dh)], h_s.at[two], "hs")
            norm_rows(hbuf.at[two], 1)
            hst[j % SLOTS] = hbuf[two, pl.ds(_al(s * hb + c * ow, SUB), ow), :]

        when_block(j, body)

    def mlp_up(j):
        def body():
            def col(n):
                cols = pl.ds(n * nt_f, nt_f)
                gt = jnp.dot(a_buf[...], wg_v[:, cols], preferred_element_type=F32)
                up = jnp.dot(a_buf[...], wu_v[:, cols], preferred_element_type=F32)
                u_buf[:, cols] = (gt * (1.0 / (1.0 + jnp.exp(-gt))) * up).astype(BF)

            with jax.named_scope("up"):
                unrolled(f // nt_f, col)

        when_block(j, body)

    def mlp_down(j):
        def body():
            def col(n):
                cols = pl.ds(n * nt_d, nt_d)
                r_buf[:, cols] = jnp.dot(u_buf[...], wd_v[:, cols], preferred_element_type=F32).astype(BF)

            with jax.named_scope("down"):
                unrolled(d // nt_d, col)
            send(r_buf.at[pl.ds(_al((1 - s) * hb, hb), hb)], rsib.at[j % 2], r_s, r_r.at[j % 2], sib)

        when_block(j, body)

    def sum_relay(j):
        def body():
            q4 = j % SLOTS
            for e in SIDES:
                @pl.when(j >= SLOTS)
                def _():
                    wait(sums.at[q4, e], sum_s.at[q4, e], "sums")

                wait(rs_far.at[q4, e], far_r.at[q4, e], "s1")
                sums[q4, e] = (rs_far[q4, e].astype(F32) + cpart(q4, target[e], e)[...].astype(F32)).astype(BF)
                send(sums.at[q4, e], rs_sum.at[q4, e], sum_s.at[q4, e], sum_r.at[q4, e], dest[e])

        when_block(j, body)

    def yrow(j, chip):
        return y_ref.at[pl.ds(_al(j * b + s * hb + chip * ow, ow), ow)]

    def yhalf(j, chip, half):
        return y_ref.at[pl.ds(_al(j * b + s * hb + chip * ow + half * hw, hw), hw)]

    def y_sent(q4):
        for e in SIDES:
            wait(ych.at[q4], y_s.at[q4, e], "ysent")
            wait(ych.at[q4], y_sx.at[q4, e], "ysent")

    def sum_end(j):
        def body():
            q4 = j % SLOTS

            @pl.when(j >= SLOTS)
            def _():
                y_sent(q4)

            for e in SIDES:
                wait(rs_far.at[q4, e], far_s.at[q4, e], "s1s")
                wait(rs_near.at[q4, e], near_s.at[q4, e], "s1s")
                wait(rs_near.at[q4, e], near_r.at[q4, e], "s2")
                wait(rs_sum.at[q4, e], sum_r.at[q4, e], "s2")
            for e in SIDES:
                rows = pl.ds(e * hw, hw)
                tot = cpart(q4, c, e)[...].astype(F32) + rs_near[q4, 1 - e].astype(F32) + rs_sum[q4, e].astype(F32)
                ych[q4, rows, :] = (hst[q4, rows, :].astype(F32) + tot).astype(BF)
            for e in SIDES:
                send(ych.at[q4], yrow(j, c), y_s.at[q4, e], y_r.at[e, j], dest[e])
            send(ych.at[q4], yrow(j, c), y_sx.at[q4, 0], y_rs.at[j], sib)
            put(ych.at[q4], yrow(j, c), y_sx.at[q4, 1])

        when_block(j, body)

    def y_stage2(j):
        def body():
            for e in SIDES:
                reg = yrow(j, origin[e])
                wait(reg, y_r.at[e, j], "y2")
                half = yhalf(j, origin[e], e)
                send(half, half, y_rel.at[e], y_f.at[e, j], dest[e])
                send(reg, reg, y_fwd, y_rs.at[j], sib)

        when_block(j, body)

    def y_stage3(j):
        def body():
            for e in SIDES:
                wait(yhalf(j, c_o, e), y_f.at[e, j], "y3")
            send(yrow(j, c_o), yrow(j, c_o), y_fwd, y_rs.at[j], sib)

        when_block(j, body)

    load_o(0)

    def phase2(i, carry):
        with jax.named_scope("slot2"):
            own_h(i)
            sum_start(i - 2)
            swap_h(i)
            mlp_norm(i - 1)
            sum_relay(i - 3)
            mlp_up(i - 1)
            sum_end(i - 4)
            mlp_down(i - 1)
            y_stage2(i - 5)
            y_stage3(i - 6)
            o_stage2(nb + i - l1)
            o_stage3(nb + i - l2)
        return carry

    lax.fori_loop(0, nb + 6, phase2, 0)

    def drain(j, carry):
        wait(_first(y_ref, hb), y_rs.at[j])
        return carry

    lax.fori_loop(0, nb, drain, 0)
    for q4 in range(SLOTS):
        y_sent(q4)
        for e in SIDES:
            wait(sums.at[q4, e], sum_s.at[q4, e])
    for e in SIDES:
        wait(_first(y_ref, nb * hw), y_rel.at[e])
        wait(o_buf, o_s.at[e])
        wait(oall_ref.at[pl.ds(0, t // 2), pl.ds(0, qw)], o_rel.at[e])
        wait(_first(wo_v, wr), wo_fs.at[e])
        for k in SIDES:
            wait(_first(wo_v, wr), wo_s.at[e, k])
    wait(_first(y_ref, nb * ow * 3), y_fwd)
    wait(o_buf, o_sx.at[0])
    wait(oall_ref.at[:, pl.ds(0, 3 * qw)], o_fwd)
    wait(_first(wo_v, qw), wo_d.at[0])
    for e in range(len(peers)):
        wait(_first(wo_v, 6 * wr), wo_ps.at[0, e])
    wo_end(wo_ps)
    for e, src in enumerate((k_scr, v_scr)):
        wait(src, kv_s.at[e])


def _layer(tp, dp, zn, x, pos, inv, g1, g2, wq, wk, wv, wo, wg, wu, wd):
    t, d = x.shape
    qw = wq.shape[1]
    f = wg.shape[1]
    hl = qw // HEAD
    b = BLOCK
    nb = t // b
    hb = b // 2
    nc = tp // 2
    ow = hb // nc
    hw = ow // 2
    dh = d // 2
    assert nc == SLOTS and t % b == 0 and wk.shape[1] == tp * HEAD
    l1 = max(nb // 4, 1)
    l2 = min(nb * 3 // 4, nb - 2)
    hbm = pl.BlockSpec(memory_space=pl.ANY)
    bufs = [
        (d, qw + 2 * HEAD), (tp * qw, dh), (d, f), (d, f), (f, d), (2, b, d), None, (b, d),
        (hl * b, HEAD), (t, HEAD), (t, HEAD), None, None, None, (t, qw),
        (b, tp * qw), (b, dh), (2, b, d), (b, f), (b, d), (2, hb, d), (SLOTS, hb, d),
        (SLOTS, 2, hw, d), (SLOTS, 2, hw, d), (SLOTS, 2, hw, d), (SLOTS, 2, hw, d), (SLOTS, ow, d), (SLOTS, ow, d),
    ]
    wide = iter([(2, 1, d)] + [(hl * b, HEAD)] * 3)
    scratch = [pltpu.VMEM(a.shape, a.dtype) for a in (pos, inv, g1, g2)]
    scratch += [pltpu.VMEM(next(wide), F32) if shape is None else pltpu.VMEM(shape, BF) for shape in bufs]
    two, four, ring, per = (2,), (SLOTS, 2), (2, nb), (nb,)
    sems = [(4,), (3,), (3,), two, two,
            (3,), (2, 2), (2, 2), two, two, (2, 2), (2, 2),
            two, two, ring, ring, per, two, (),
            two, two, two, (), two, four, four, four, four, four, four,
            four, four, ring, ring, per, two, ()]
    scratch += [pltpu.SemaphoreType.DMA(shape) for shape in sems]
    flops = 2 * t * (d * (qw + 2 * HEAD) + qw * t + tp * qw * dh + 3 * d * f)
    outs = [(t, d), (t, HEAD), (t, HEAD), (t, tp * qw)]
    return pl.pallas_call(
        functools.partial(_kernel, tp, dp, zn, l1, l2, nb // 4, nb // 2, nb * 3 // 4),
        name="layer",
        out_shape=tuple(jax.ShapeDtypeStruct(shape, BF) for shape in outs),
        in_specs=[hbm] * 12,
        out_specs=(hbm,) * len(outs),
        scratch_shapes=scratch,
        compiler_params=pltpu.CompilerParams(collective_id=0, has_side_effects=True, vmem_limit_bytes=VMEM_BYTES),
        cost_estimate=pl.CostEstimate(flops=flops, bytes_accessed=8 * t * d, transcendentals=t * t * hl),
    )(x, pos, inv, g1, g2, wq, wk, wv, wo, wg, wu, wd)


def _copy_kernel(src, k_src, v_src, dst, k_dst, v_dst, buf, kv, rd, wr, kv_sem):
    n, rows = buf.shape[0], buf.shape[1]
    steps = src.shape[0] // rows

    def read(i):
        return pltpu.make_async_copy(src.at[pl.ds(i * rows, rows)], buf.at[i % n], rd.at[i % n])

    def write(i):
        return pltpu.make_async_copy(buf.at[i % n], dst.at[pl.ds(i * rows, rows)], wr.at[i % n])

    small = ((k_src, k_dst), (v_src, v_dst))
    kv_in = [pltpu.make_async_copy(a, kv.at[e], kv_sem.at[e]) for e, (a, _) in enumerate(small)]
    kv_out = [pltpu.make_async_copy(kv.at[e], z, kv_sem.at[e]) for e, (_, z) in enumerate(small)]
    for i in range(min(n, steps)):
        read(i).start()
    for copy in kv_in:
        copy.start()
    for i in range(steps):
        read(i).wait()
        write(i).start()
        if i >= 1 and i - 1 + n < steps:
            write(i - 1).wait()
            read(i - 1 + n).start()
    for e in SIDES:
        kv_in[e].wait()
        kv_out[e].start()
    for i in range(max(0, steps - n), steps):
        write(i).wait()
    for copy in kv_out:
        copy.wait()


def _copy(y, k, v):
    t, d = y.shape
    rows, n = 128, 32
    hbm = pl.BlockSpec(memory_space=pl.ANY)
    dma = pltpu.SemaphoreType.DMA
    n = min(n, t // rows)
    return pl.pallas_call(
        _copy_kernel,
        name="copy_out",
        out_shape=tuple(jax.ShapeDtypeStruct(a.shape, a.dtype) for a in (y, k, v)),
        in_specs=[hbm] * 3,
        out_specs=(hbm,) * 3,
        scratch_shapes=[pltpu.VMEM((n, rows, d), y.dtype), pltpu.VMEM((2,) + k.shape, k.dtype),
                        dma((n,)), dma((n,)), dma((2,))],
        compiler_params=pltpu.CompilerParams(vmem_limit_bytes=VMEM_BYTES),
        cost_estimate=pl.CostEstimate(flops=0, bytes_accessed=4 * t * d, transcendentals=0),
    )(y, k, v)


def _row_length(mesh):
    at = [getattr(dev, "coords", None) for dev in mesh.devices.reshape(mesh.shape["dp"], -1)[:, 0]]
    if any(p is None for p in at):
        return None
    n = len(at)

    def apart(i, j):
        return sum(abs(p - q) for p, q in zip(at[i], at[j]))

    length = next((i for i in range(1, n) if at[i][-1] == at[0][-1]), n)
    if length % 2 or n % (2 * length):
        return None
    rows = all(apart(i, i + 1) == 1 for i in range(0, n, 2))
    across = all(apart(i, i + length) == 1 for i in range(n) if (i // length) % 2 == 0)
    return length if rows and across else None


def solution(mesh):
    tp = mesh.shape["tp"]
    dp = mesh.shape["dp"]
    zn = _row_length(mesh)

    def local(x, pos, g1, g2, wq, wk, wv, wo, wg, wu, wd):
        t = x.shape[0]
        half = ROPE_BASE ** (-2.0 * np.arange(HEAD // 2) / HEAD)
        inv = jnp.asarray(np.concatenate([half, half])[None, :].astype(np.float32))
        y, k, v, _ = _layer(tp, dp, zn, x, pos.reshape(t // LANES, LANES), inv, g1, g2, wq, wk, wv, wo, wg, wu, wd)
        y, k, v = _copy(y, k, v)
        return y, k.reshape(t, 1, HEAD), v.reshape(t, 1, HEAD)

    return jax.shard_map(
        local,
        mesh=mesh,
        in_specs=(P("dp", None), P("dp"), P(), P(), P(None, "tp"), P(), P(), P("tp", None),
                  P(None, "tp"), P(None, "tp"), P("tp", None)),
        out_specs=(P("dp", None), P("dp", "tp", None), P("dp", "tp", None)),
        check_vma=False,
    )
```

```python
import functools

import jax
import jax.numpy as jnp
import numpy as np
from jax import lax
from jax.experimental import pallas as pl
from jax.experimental.pallas import tpu as pltpu
from jax.sharding import PartitionSpec as P

HEAD = 128
LANES = 128
SUB = 16
EPS = 1e-5
ROPE_BASE = 500000.0
MESH = pl.DeviceIdType.MESH
BLOCK = 256
NR = 64
SLOTS = 4
LATE = 8
SIDES = (0, 1)
BF = jnp.bfloat16
F32 = jnp.float32
VMEM_BYTES = 67000000
Y_VMEM = 8
TWO_OVER_PI = 0.6366197723675814
PI_2 = (1.5703125, 4.837512969970703125e-4, 7.54978995489188216e-8)
SIN = (-1.9515295891e-4, 8.3321608736e-3, -1.6666654611e-1)
COS = (2.443315711809948e-5, -1.388731625493765e-3, 4.166664568298827e-2)
LOG2E = 1.4426950408889634


def _sincos(ang):
    n = jnp.floor(ang * TWO_OVER_PI + 0.5)
    r = ang
    for p in PI_2:
        r = r - n * p
    z = r * r
    s = functools.reduce(lambda a, p: a * z + p, SIN[1:], SIN[0]) * z * r + r
    c = functools.reduce(lambda a, p: a * z + p, COS[1:], COS[0]) * z * z - 0.5 * z + 1.0
    m = n.astype(jnp.int32)
    odd = (m & 1) == 1
    cs = jnp.where(odd, s, c)
    sn = jnp.where(odd, c, s)
    return jnp.where(((m + 1) & 2) == 2, -cs, cs), jnp.where((m & 2) == 2, -sn, sn)


def _al(v, m):
    return pl.multiple_of(v, m)


def _first(ref, n):
    return ref.at[pl.ds(0, n)]


def _kernel(tp, dp, zn, split, l1, l2, w2, w3, w4,
            x_ref, pos_ref, inv_ref, g1_ref, g2_ref, wq_ref, wk_ref, wv_ref, wo_ref, wg_ref, wu_ref, wd_ref,
            y_ref, y_vm, k_ref, v_ref, oall_ref,
            pos_v, inv_v, g1_v, g2_v, wo_v, wg_v, wu_v, wd_v, g_scr, a_buf, o_buf,
            hbuf, rsib, rs_far, rs_near, rs_sum,
            ld_s, ld_w, ld_mlp, ld_x, kv_s,
            wo_d, wo_s, wo_r, wo_fs, wo_fr, wo_ps, wo_pr,
            o_s, o_sx, o_r, o_f, o_rs, o_rel, o_fwd,
            ld_o, h_s, h_r, r_s, r_r, part_s, far_r, near_r, sum_s, sum_r,
            y_s, y_r, y_f, y_rs, y_rel, y_fwd):
    t, d = x_ref.shape
    qw = wq_ref.shape[1]
    f = wg_ref.shape[1]
    hl = qw // HEAD
    b = BLOCK
    nb = t // b
    dh = d // 2
    hb = b // 2
    nc = tp // 2
    ow = hb // nc
    hw = ow // 2
    kvt = 2 * b

    r = lax.axis_index("tp")
    c = r // 2
    s = r % 2
    c_r = (c + 1) % nc
    c_l = (c + nc - 1) % nc
    c_o = (c + 2) % nc
    dest = ({"tp": c_r * 2 + s}, {"tp": c_l * 2 + s})
    origin = (c_l, c_r)
    target = (c_r, c_l)
    sib = {"tp": c * 2 + 1 - s}
    dpi = lax.axis_index("dp")
    par = dpi % 2
    peers = [{"dp": dpi + 1 - 2 * par}] if dp % 2 == 0 else []
    if zn:
        par_y = (dpi // zn) % 2
        peers.append({"dp": dpi + zn * (1 - 2 * par_y)})

    def send(src, dst, ss, rs, dev):
        pltpu.make_async_remote_copy(
            src_ref=src, dst_ref=dst, send_sem=ss, recv_sem=rs, device_id=dev, device_id_type=MESH).start()

    def put(src, dst, sem):
        pltpu.make_async_copy(src, dst, sem).start()

    def wait(region, sem, tag=None):
        with jax.named_scope("w_" + (tag or "end")):
            pltpu.make_async_copy(region, region, sem).wait()

    def when_block(j, body):
        @pl.when((j >= 0) & (j < nb))
        def _():
            body()

    barrier = pltpu.get_barrier_semaphore()
    cross = [{"tp": target[e] * 2 + 1 - s} for e in SIDES]
    others = [*dest, *cross, sib, *peers]
    for dev in others:
        pl.semaphore_signal(barrier, inc=1, device_id=dev, device_id_type=MESH)

    small = ((pos_ref, pos_v), (inv_ref, inv_v), (g1_ref, g1_v), (g2_ref, g2_v))
    for e, (src, dst) in enumerate(small):
        put(src, dst, ld_s.at[e])
    with jax.named_scope("barrier"):
        pl.semaphore_wait(barrier, len(others))

    mine = _al(s * dh, LANES)
    other = _al((1 - s) * dh, LANES)
    parts = 4 if zn else len(peers) + 1
    wr = qw // parts
    part = (2 * par_y + par) if zn else (par if peers else 0)

    def shard(dev):
        return wo_v.at[pl.ds(_al(dev * qw, LANES), qw)]

    def piece(chip, core, q=None):
        return wo_v.at[pl.ds(_al((chip * 2 + core) * qw + (part if q is None else q) * wr, 32), wr)]

    rows = pl.ds(_al(part * wr, 32), wr)
    for e in SIDES:
        for k, (cols, dev) in enumerate(((mine, dest[e]), (other, cross[e]))):
            send(wo_ref.at[rows, pl.ds(cols, dh)], piece(c, s), wo_s.at[e, k], wo_r.at[e, s], dev)
    send(wo_ref.at[:, pl.ds(other, dh)], shard(r), wo_d.at[0], wo_d.at[1], sib)
    put(wo_ref.at[:, pl.ds(mine, dh)], shard(r), wo_d.at[2])

    def wo_swap(chip):
        for e, dev in enumerate(peers):
            for core in SIDES:
                send(piece(chip, core), piece(chip, core), wo_ps.at[0, e], wo_pr.at[0, e], dev)

    def wo_stage2():
        for e in SIDES:
            for core in SIDES:
                wait(piece(origin[e], core), wo_r.at[e, core], "wo2")
            reg = piece(origin[e], e)
            send(reg, reg, wo_fs.at[e], wo_fr.at[e], dest[e])
            wo_swap(origin[e])

    def wo_stage3():
        for e in SIDES:
            wait(piece(c_o, e), wo_fr.at[e], "wo3")
        wo_swap(c_o)

    def wo_stage4():
        for e in range(len(peers)):
            wait(_first(wo_v, 6 * wr), wo_pr.at[0, e], "wo4")
        if zn:
            for chip in (*origin, c_o):
                for e, q in enumerate((2 * (1 - par_y) + par, 2 * par_y + 1 - par)):
                    reg = piece(chip, e, q)
                    send(reg, reg, wo_ps.at[1, e], wo_pr.at[1, e], peers[e])

    def wo_end(which):
        for e in SIDES if zn else ():
            wait(_first(wo_v, 3 * wr), which.at[1, e], "wo5")

    def ocol(chip, core):
        return pl.ds(_al((chip * 2 + core) * qw, LANES), qw)

    def oreg(j, chip):
        return oall_ref.at[pl.ds(_al(j * b, b), b), ocol(chip, s)]

    def ohalf(j, chip, half):
        return oall_ref.at[pl.ds(_al(j * b + half * hb, hb), hb), ocol(chip, s)]

    def orow(j):
        return pl.ds(_al(j * b, b), b)

    def o_stage2(j):
        def body():
            for e in SIDES:
                reg = oreg(j, origin[e])
                wait(reg, o_r.at[e, j], "o2")
                half = ohalf(j, origin[e], e)
                send(half, half, o_rel.at[e], o_f.at[e, j], dest[e])
                send(reg, reg, o_fwd, o_rs.at[j], sib)

        when_block(j, body)

    def o_stage3(j):
        def body():
            for e in SIDES:
                wait(ohalf(j, c_o, e), o_f.at[e, j], "o3")
            send(oreg(j, c_o), oreg(j, c_o), o_fwd, o_rs.at[j], sib)

        when_block(j, body)

    def unrolled(n, body):
        for e in range(n):
            body(e)

    def norm_rows(src, which):
        def step(e, carry):
            for q in range(NR // SUB):
                rows = pl.ds(_al(e * NR + q * SUB, SUB), SUB)
                v32 = src[rows, :].astype(F32)
                inv = lax.rsqrt(jnp.mean(v32 * v32, axis=1, keepdims=True) + EPS)
                a_buf[rows, :] = (v32 * inv * g_scr[which]).astype(BF)
            return carry

        with jax.named_scope("norm"):
            lax.fori_loop(0, b // NR, step, 0)

    for e, (src, dst) in enumerate(small):
        wait(dst, ld_s.at[e], "small")
    for e, ref in enumerate((g1_v, g2_v)):
        g_scr[e] = ref[...].astype(F32).reshape(1, d)

    def attention(wqkv, x_buf, q_scr, k_scr, v_scr, m_scr, l_scr, acc_scr):
        rk = _al(r * HEAD, HEAD)
        wq_dst = wqkv.at[:, pl.ds(0, qw)]
        kv_dst = [wqkv.at[:, pl.ds(qw + e * HEAD, HEAD)] for e in SIDES]
        put(_first(x_ref, b), x_buf.at[0], ld_x.at[0])
        put(wq_ref, wq_dst, ld_w.at[2])
        for e, ref in enumerate((wk_ref, wv_ref)):
            put(ref.at[:, pl.ds(rk, HEAD)], kv_dst[e], ld_w.at[e])
        caches = ((k_scr, k_ref), (v_scr, v_ref))
        scale = HEAD ** -0.5 * LOG2E
        lane = lax.broadcasted_iota(jnp.int32, (b, HEAD), 1)

        def heads(ref, h):
            return ref.at[pl.ds(h * b, b)]

        def tile(first, n, masked=False):
            keys = pl.ds(_al(first, n), n)
            kk = k_scr[keys, :]
            vv = v_scr[keys, :]
            sc = lax.dot_general(q_scr[...], kk, (((1,), (1,)), ((), ())), preferred_element_type=F32)
            if masked:
                keep = lax.broadcasted_iota(jnp.int32, (b, n), 1) <= lax.broadcasted_iota(jnp.int32, (b, n), 0)
                sc = jnp.concatenate([jnp.where(keep, sc[h * b:(h + 1) * b], -jnp.inf) for h in range(hl)], axis=0)
            m_prev = m_scr[...]
            m_new = jnp.maximum(m_prev, jnp.max(sc, axis=1, keepdims=True))
            ps = [jnp.exp2((sc[:, e * HEAD:(e + 1) * HEAD] - m_new) * scale) for e in range(n // HEAD)]
            alpha = jnp.exp2((m_prev - m_new) * scale)
            l_scr[...] = l_scr[...] * alpha + functools.reduce(lambda p, q: p + q, ps)
            pr = jnp.concatenate([p.astype(BF) for p in ps], axis=1)
            acc_scr[...] = acc_scr[...] * alpha + jnp.dot(pr, vv, preferred_element_type=F32)
            m_scr[...] = m_new

        def phase1(i, carry):
            with jax.named_scope("slot1"):
                phase1_slot(i)
            return carry

        def phase1_slot(i):
            slot = i % 2
            wait(x_buf.at[slot], ld_x.at[slot], "x")

            @pl.when(i + 1 < nb)
            def _():
                put(x_ref.at[pl.ds(_al((i + 1) * b, b), b)], x_buf.at[1 - slot], ld_x.at[1 - slot])

            norm_rows(x_buf.at[slot], 0)

            @pl.when(i == 0)
            def _():
                wait(wq_dst, ld_w.at[2], "w")
                for e in SIDES:
                    wait(kv_dst[e], ld_w.at[e], "w")

            for e, (src, dst) in enumerate(((wg_ref, wg_v), (wu_ref, wu_v), (wd_ref, wd_v))):
                @pl.when(i == w2 + e)
                def _(src=src, dst=dst, e=e):
                    put(src, dst, ld_mlp.at[e])

            pcol = []
            for e in range(b // LANES):
                prow = pos_v[pl.ds(i * (b // LANES) + e, 1), :].astype(F32)
                pcol.append(jnp.transpose(jnp.broadcast_to(prow, (LANES, LANES))))
            co, si = _sincos(jnp.concatenate(pcol, axis=0) * inv_v[...])
            si = jnp.where(lane < HEAD // 2, -si, si)
            qk32 = jnp.dot(a_buf[...], wqkv[:, :qw + HEAD], preferred_element_type=F32)
            v32 = jnp.dot(a_buf[...], wqkv[:, qw + HEAD:], preferred_element_type=F32)
            rows = pl.ds(_al(i * b, b), b)
            for h in range(hl + 1):
                head = qk32[:, h * HEAD:(h + 1) * HEAD]
                head = (head * co + pltpu.roll(head, HEAD // 2, 1) * si).astype(BF)
                if h < hl:
                    heads(q_scr, h)[...] = head
                else:
                    k_scr[rows, :] = head
            v_scr[rows, :] = v32.astype(BF)
            for e, (src, dst) in enumerate(caches):
                @pl.when(i > 0)
                def _(src=src, e=e):
                    wait(_first(src, b), kv_s.at[e])

                put(src.at[rows], dst.at[rows], kv_s.at[e])
            m_scr[...] = jnp.full(m_scr.shape, -jnp.inf, F32)
            l_scr[...] = jnp.zeros(l_scr.shape, F32)
            acc_scr[...] = jnp.zeros(acc_scr.shape, F32)
            full = i // 2

            def inner(j, carry):
                for e in SIDES:
                    tile((2 * j + e) * kvt, kvt)
                return carry

            with jax.named_scope("tiles"):
                lax.fori_loop(0, full // 2, inner, 0)

            @pl.when(full % 2 == 1)
            def _():
                tile((full - 1) * kvt, kvt)

            @pl.when(i % 2 == 1)
            def _():
                tile((i - 1) * b, b)

            tile(i * b, b, masked=True)
            for h in range(hl):
                o_buf[rows, h * HEAD:(h + 1) * HEAD] = (
                    heads(acc_scr, h)[...] / jnp.sum(heads(l_scr, h)[...], axis=1, keepdims=True)).astype(BF)
            src = o_buf.at[rows]
            dst = oreg(i, c)
            for e in SIDES:
                send(src, dst, o_s.at[e], o_r.at[e, i], dest[e])
            send(src, dst, o_sx.at[0], o_rs.at[i], sib)
            put(src, dst, o_sx.at[1])
            for when, stage in ((w2, wo_stage2), (w3, wo_stage3), (w4, wo_stage4)):
                pl.when(i == when)(stage)
            o_stage2(i - l1)
            o_stage3(i - l2)

        lax.fori_loop(0, nb, phase1, 0)
        for e, (src, _) in enumerate(caches):
            wait(_first(src, b), kv_s.at[e])

    loc = pltpu.VMEM
    pl.run_scoped(
        attention, loc((d, qw + 2 * HEAD), BF), loc((2, b, d), BF), loc((hl * b, HEAD), BF), loc((t, HEAD), BF),
        loc((t, HEAD), BF), *[loc((hl * b, HEAD), F32)] * 3)
    wait(o_buf, o_sx.at[1])
    for e, dst in enumerate((wg_v, wu_v, wd_v)):
        wait(dst, ld_mlp.at[e])
    wait(shard(r + 1 - 2 * s), wo_d.at[1])
    wait(shard(r), wo_d.at[2])
    wo_end(wo_pr)

    def rest(o_blk, xh, u_buf, r_buf, cp, sums, ych, hst):
        def load_o(j):
            wait(oall_ref.at[orow(j), pl.ds(0, 4 * qw)], o_rs.at[j], "os")
            put(oall_ref.at[orow(j)], o_blk, ld_o.at[0])
            put(x_ref.at[orow(j), pl.ds(mine, dh)], xh, ld_o.at[1])

        nt_h = min(512, dh)
        nt_f = min(512, f)
        nt_d = min(512, d)

        def cpart(q4, chip, half):
            return cp.at[q4, pl.ds(_al(chip * ow + half * hw, hw), hw)]

        def sum_start(j):
            def body():
                two = j % 2
                q4 = j % SLOTS
                wait(rsib.at[two], r_r.at[two], "r")
                wait(rsib.at[two], r_s, "rs")

                def add(e, carry):
                    rows = pl.ds(_al(e * SUB, SUB), SUB)
                    own = r_buf[pl.ds(_al(s * hb + e * SUB, SUB), SUB), :]
                    cp[q4, rows, :] = (own.astype(F32) + rsib[two, rows, :].astype(F32)).astype(BF)
                    return carry

                with jax.named_scope("add"):
                    lax.fori_loop(0, hb // SUB, add, 0)
                for e in SIDES:
                    send(cpart(q4, c_o, e), rs_far.at[q4, e], part_s.at[q4], far_r.at[q4, e], dest[e])
                for e in SIDES:
                    send(cpart(q4, target[e], 1 - e), rs_near.at[q4, e], part_s.at[q4], near_r.at[q4, e], dest[e])

            when_block(j, body)

        def own_h(j):
            @pl.when(j < nb)
            def _():
                wait(o_blk, ld_o.at[0], "ldo")
                wait(xh, ld_o.at[1], "ldo")

                def col(n):
                    cols = pl.ds(n * nt_h, nt_h)
                    v32 = jnp.dot(o_blk[...], wo_v[:, cols], preferred_element_type=F32)
                    hbuf[j % 2, :, pl.ds(_al(s * dh + n * nt_h, LANES), nt_h)] = (xh[:, cols].astype(F32) + v32).astype(BF)

                with jax.named_scope("own_h"):
                    unrolled(dh // nt_h, col)

        def swap_h(j):
            @pl.when(j < nb)
            def _():
                half = hbuf.at[j % 2, :, pl.ds(mine, dh)]
                send(half, half, h_s.at[j % 2], h_r.at[j % 2], sib)

            @pl.when(j + 1 < nb)
            def _():
                load_o(j + 1)

        def mlp_norm(j):
            def body():
                two = j % 2
                wait(hbuf.at[two, :, pl.ds(other, dh)], h_r.at[two], "h")
                wait(hbuf.at[two, :, pl.ds(mine, dh)], h_s.at[two], "hs")
                norm_rows(hbuf.at[two], 1)
                hst[j % SLOTS] = hbuf[two, pl.ds(_al(s * hb + c * ow, SUB), ow), :]

            when_block(j, body)

        def mlp_up(j):
            def body():
                def col(n):
                    cols = pl.ds(n * nt_f, nt_f)
                    gt = jnp.dot(a_buf[...], wg_v[:, cols], preferred_element_type=F32)
                    up = jnp.dot(a_buf[...], wu_v[:, cols], preferred_element_type=F32)
                    u_buf[:, cols] = (gt * (1.0 / (1.0 + jnp.exp(-gt))) * up).astype(BF)

                with jax.named_scope("up"):
                    unrolled(f // nt_f, col)

            when_block(j, body)

        def mlp_down(j):
            def body():
                def col(n):
                    cols = pl.ds(n * nt_d, nt_d)
                    r_buf[:, cols] = jnp.dot(u_buf[...], wd_v[:, cols], preferred_element_type=F32).astype(BF)

                with jax.named_scope("down"):
                    unrolled(d // nt_d, col)
                send(r_buf.at[pl.ds(_al((1 - s) * hb, hb), hb)], rsib.at[j % 2], r_s, r_r.at[j % 2], sib)

            when_block(j, body)

        def sum_relay(j):
            def body():
                q4 = j % SLOTS
                @pl.when(j >= SLOTS)
                def _():
                    wait(sums.at[q4], sum_s.at[q4], "sums")

                for e in SIDES:
                    wait(rs_far.at[q4, e], far_r.at[q4, e], "s1")
                    sums[q4, e] = (rs_far[q4, e].astype(F32) + cpart(q4, target[e], e)[...].astype(F32)).astype(BF)
                    send(sums.at[q4, e], rs_sum.at[q4, e], sum_s.at[q4], sum_r.at[q4, e], dest[e])

            when_block(j, body)

        def on_y(j, body):
            @pl.when((j >= 0) & (j < split))
            def _():
                body(y_ref, j * b, False)

            @pl.when((j >= split) & (j < nb))
            def _():
                body(y_vm, (j - split) * b, True)

        def yrow(ref, row, chip):
            return ref.at[pl.ds(_al(row + s * hb + chip * ow, ow), ow)]

        def yhalf(ref, row, chip, half):
            return ref.at[pl.ds(_al(row + s * hb + chip * ow + half * hw, hw), hw)]

        def y_sent(j, vmem):
            wait(cp.at[j % SLOTS, pl.ds(0, (3 if vmem else 4) * ow)], y_s.at[j % SLOTS], "ysent")

        def sum_end(j):
            on_y(j - SLOTS, lambda ref, row, vmem: pl.when(j < nb)(lambda: y_sent(j - SLOTS, vmem)))

            def body(ref, row, vmem):
                q4 = j % SLOTS
                wait(cp.at[q4, pl.ds(0, 4 * hw)], part_s.at[q4], "s1s")
                for e in SIDES:
                    wait(rs_near.at[q4, e], near_r.at[q4, e], "s2")
                    wait(rs_sum.at[q4, e], sum_r.at[q4, e], "s2")
                own = yrow(ref, row, c)
                src = own if vmem else ych.at[q4]
                for e in SIDES:
                    rows = pl.ds(e * hw, hw)
                    tot = cpart(q4, c, e)[...].astype(F32) + rs_near[q4, 1 - e].astype(F32) + rs_sum[q4, e].astype(F32)
                    dst = yhalf(ref, row, c, e) if vmem else ych.at[q4, rows]
                    dst[...] = (hst[q4, rows, :].astype(F32) + tot).astype(BF)
                for e in SIDES:
                    send(src, own, y_s.at[q4], y_r.at[e, q4], dest[e])
                send(src, own, y_s.at[q4], y_rs.at[j % LATE], sib)
                if not vmem:
                    put(src, own, y_s.at[q4])

            on_y(j, body)

        def y_stage2(j):
            def body(ref, row, vmem):
                for e in SIDES:
                    reg = yrow(ref, row, origin[e])
                    wait(reg, y_r.at[e, j % SLOTS], "y2")
                    half = yhalf(ref, row, origin[e], e)
                    send(half, half, y_rel.at[e], y_f.at[e, j % SLOTS], dest[e])
                    send(reg, reg, y_fwd, y_rs.at[j % LATE], sib)

            on_y(j, body)

        def y_stage3(j):
            def body(ref, row, vmem):
                for e in SIDES:
                    wait(yhalf(ref, row, c_o, e), y_f.at[e, j % SLOTS], "y3")
                reg = yrow(ref, row, c_o)
                send(reg, reg, y_fwd, y_rs.at[j % LATE], sib)

            on_y(j, body)

        def y_seen(j):
            when_block(j, lambda: wait(cp.at[0], y_rs.at[j % LATE], "ys"))

        load_o(0)

        def phase2(i, carry):
            with jax.named_scope("slot2"):
                own_h(i)
                sum_start(i - 2)
                swap_h(i)
                mlp_norm(i - 1)
                sum_relay(i - 3)
                mlp_up(i - 1)
                sum_end(i - 4)
                mlp_down(i - 1)
                y_stage2(i - 5)
                y_stage3(i - 6)
                y_seen(i - LATE)
                o_stage2(nb + i - l1)
                o_stage3(nb + i - l2)
            return carry

        lax.fori_loop(0, nb + 6, phase2, 0)

        for j in range(nb + 6 - LATE, nb):
            wait(cp.at[0], y_rs.at[j % LATE])
        for j in range(nb - SLOTS, nb):
            y_sent(j, j >= split)
            wait(sums.at[j % SLOTS], sum_s.at[j % SLOTS])
        for e in SIDES:
            wait(_first(y_ref, nb * hw), y_rel.at[e])
            wait(o_buf, o_s.at[e])
            wait(oall_ref.at[pl.ds(0, t // 2), pl.ds(0, qw)], o_rel.at[e])
            wait(_first(wo_v, wr), wo_fs.at[e])
            for k in SIDES:
                wait(_first(wo_v, wr), wo_s.at[e, k])
        wait(_first(y_ref, nb * ow * 3), y_fwd)
        wait(o_buf, o_sx.at[0])
        wait(oall_ref.at[:, pl.ds(0, 3 * qw)], o_fwd)
        wait(_first(wo_v, qw), wo_d.at[0])
        for e in range(len(peers)):
            wait(_first(wo_v, 6 * wr), wo_ps.at[0, e])
        wo_end(wo_ps)

    pl.run_scoped(
        rest, loc((b, tp * qw), BF), loc((b, dh), BF), loc((b, f), BF), loc((b, d), BF), loc((SLOTS, hb, d), BF),
        loc((SLOTS, 2, hw, d), BF), *[loc((SLOTS, ow, d), BF)] * 2)


def _held(rows, d):
    return pltpu.VMEM((rows, d), BF)


def _keep(a, space):
    return pltpu.with_memory_space_constraint(a, space)


def _layer(tp, dp, zn, x, pos, inv, g1, g2, wq, wk, wv, wo, wg, wu, wd):
    t, d = x.shape
    qw = wq.shape[1]
    f = wg.shape[1]
    hl = qw // HEAD
    b = BLOCK
    nb = t // b
    hb = b // 2
    nc = tp // 2
    ow = hb // nc
    hw = ow // 2
    dh = d // 2
    assert nc == SLOTS and t % b == 0 and wk.shape[1] == tp * HEAD
    l1 = max(nb // 4, 1)
    l2 = min(nb * 3 // 4, nb - 2)
    hbm = pl.BlockSpec(memory_space=pl.ANY)
    bufs = [
        (tp * qw, dh), (d, f), (d, f), (f, d), None, (b, d), (t, qw),
        (2, b, d), (2, hb, d), *[(SLOTS, 2, hw, d)] * 3,
    ]
    scratch = [pltpu.VMEM(a.shape, a.dtype) for a in (pos, inv, g1, g2)]
    scratch += [pltpu.VMEM((2, 1, d), F32) if shape is None else pltpu.VMEM(shape, BF) for shape in bufs]
    two, four, ring, per = (2,), (SLOTS, 2), (2, nb), (nb,)
    sems = [(4,), (3,), (3,), two, two,
            (3,), (2, 2), (2, 2), two, two, (2, 2), (2, 2),
            two, two, ring, ring, per, two, (),
            two, two, two, (), two, (SLOTS,), four, four, (SLOTS,), four,
            (SLOTS,), (2, SLOTS), (2, SLOTS), (LATE,), two, ()]
    scratch += [pltpu.SemaphoreType.DMA(shape) for shape in sems]
    flops = 2 * t * (d * (qw + 2 * HEAD) + qw * t + tp * qw * dh + 3 * d * f)
    split = nb - Y_VMEM * nb // 16
    outs = [(split * b, d), None, (t, HEAD), (t, HEAD), (t, tp * qw)]
    vm = _held((nb - split) * b, d)
    return pl.pallas_call(
        functools.partial(_kernel, tp, dp, zn, split, l1, l2, nb // 4, nb // 2, nb * 3 // 4),
        name="layer",
        out_shape=tuple(jax.ShapeDtypeStruct(shape, BF) if shape else vm for shape in outs),
        in_specs=[hbm] * 12,
        out_specs=tuple(hbm if shape else pl.BlockSpec(memory_space=pltpu.VMEM) for shape in outs),
        scratch_shapes=scratch,
        compiler_params=pltpu.CompilerParams(collective_id=0, has_side_effects=True,
                                             vmem_limit_bytes=VMEM_BYTES - 2 * (nb - split) * b * d),
        cost_estimate=pl.CostEstimate(flops=flops, bytes_accessed=8 * t * d, transcendentals=t * t * hl),
    )(x, pos, inv, g1, g2, wq, wk, wv, wo, wg, wu, wd)


def _copy_kernel(src, held, k_src, v_src, dst, k_dst, v_dst, buf, kv, rd, wr, kv_sem):
    rows = buf.shape[1]
    steps = src.shape[0] // rows
    small = ((k_src, k_dst), (v_src, v_dst))
    reads, writes, late = [], [], []
    for i in range(steps):
        part = pl.ds(i * rows, rows)
        reads.append(pltpu.make_async_copy(src.at[part], buf.at[i], rd.at[i]))
        writes.append(pltpu.make_async_copy(buf.at[i], dst.at[part], rd.at[i]))
    for e, (a, z) in enumerate(small):
        reads.append(pltpu.make_async_copy(a, kv.at[e], kv_sem.at[e]))
        writes.append(pltpu.make_async_copy(kv.at[e], z, kv_sem.at[e]))
    for i in range(held.shape[0] // rows):
        to = pl.ds(src.shape[0] + i * rows, rows)
        late.append(pltpu.make_async_copy(held.at[pl.ds(i * rows, rows)], dst.at[to], wr.at[i]))
    for copy in reads:
        copy.start()
    for copy in late:
        copy.start()
    for read, write in zip(reads, writes):
        read.wait()
        write.start()
    for copy in (*late, *writes):
        copy.wait()


def _copy(y, held, k, v):
    d = y.shape[1]
    t = y.shape[0] + held.shape[0]
    rows = 256
    hbm = pl.BlockSpec(memory_space=pltpu.HBM)
    dma = pltpu.SemaphoreType.DMA
    n = y.shape[0] // rows
    shapes = ((t, d), k.shape, v.shape)
    return pl.pallas_call(
        _copy_kernel,
        name="copy_out",
        out_shape=tuple(jax.ShapeDtypeStruct(shape, BF) for shape in shapes),
        in_specs=[hbm, pl.BlockSpec(memory_space=pltpu.VMEM), hbm, hbm],
        out_specs=(hbm,) * 3,
        scratch_shapes=[pltpu.VMEM((n, rows, d), BF), pltpu.VMEM((2,) + k.shape, BF),
                        dma((n,)), dma((held.shape[0] // rows,)), dma((2,))],
        compiler_params=pltpu.CompilerParams(vmem_limit_bytes=VMEM_BYTES - 3 * held.size),
        cost_estimate=pl.CostEstimate(flops=0, bytes_accessed=4 * t * d, transcendentals=0),
    )(y, held, k, v)


def _row_length(mesh):
    at = [getattr(dev, "coords", None) for dev in mesh.devices.reshape(mesh.shape["dp"], -1)[:, 0]]
    if any(p is None for p in at):
        return None
    n = len(at)

    def apart(i, j):
        return sum(abs(p - q) for p, q in zip(at[i], at[j]))

    length = next((i for i in range(1, n) if at[i][-1] == at[0][-1]), n)
    if length % 2 or n % (2 * length):
        return None
    rows = all(apart(i, i + 1) == 1 for i in range(0, n, 2))
    across = all(apart(i, i + length) == 1 for i in range(n) if (i // length) % 2 == 0)
    return length if rows and across else None


def solution(mesh):
    tp = mesh.shape["tp"]
    dp = mesh.shape["dp"]
    zn = _row_length(mesh)

    def local(x, pos, g1, g2, wq, wk, wv, wo, wg, wu, wd):
        t = x.shape[0]
        half = ROPE_BASE ** (-2.0 * np.arange(HEAD // 2) / HEAD)
        inv = jnp.asarray(np.concatenate([half, half])[None, :].astype(np.float32))
        y, held, k, v, _ = _layer(tp, dp, zn, x, pos.reshape(t // LANES, LANES), inv, g1, g2, wq, wk, wv, wo, wg, wu, wd)
        y, k, v = (_keep(a, pltpu.HBM) for a in (y, k, v))
        y, k, v = _copy(y, _keep(held, pltpu.VMEM), k, v)
        return y, k.reshape(t, 1, HEAD), v.reshape(t, 1, HEAD)

    return jax.shard_map(
        local,
        mesh=mesh,
        in_specs=(P("dp", None), P("dp"), P(), P(), P(None, "tp"), P(), P(), P("tp", None),
                  P(None, "tp"), P(None, "tp"), P("tp", None)),
        out_specs=(P("dp", None), P("dp", "tp", None), P("dp", "tp", None)),
        check_vma=False,
    )
```

```python
import functools

import jax
import jax.numpy as jnp
import numpy as np
from jax import lax
from jax.experimental import pallas as pl
from jax.experimental.pallas import tpu as pltpu
from jax.sharding import PartitionSpec as P

HEAD = 128
LANES = 128
SUB = 16
EPS = 1e-5
ROPE_BASE = 500000.0
MESH = pl.DeviceIdType.MESH
BLOCK = 256
NR = 64
SLOTS = 4
LATE = 8
CHIP = 3
SIDES = (0, 1)
BF = jnp.bfloat16
F32 = jnp.float32
VMEM_BYTES = 67040000
Y_VMEM = 11
TWO_OVER_PI = 0.6366197723675814
PI_2 = (1.5703125, 4.837512969970703125e-4, 7.54978995489188216e-8)
SIN = (-1.9515295891e-4, 8.3321608736e-3, -1.6666654611e-1)
COS = (2.443315711809948e-5, -1.388731625493765e-3, 4.166664568298827e-2)
LOG2E = 1.4426950408889634


def _sincos(ang):
    n = jnp.floor(ang * TWO_OVER_PI + 0.5)
    r = ang
    for p in PI_2:
        r = r - n * p
    z = r * r
    s = functools.reduce(lambda a, p: a * z + p, SIN[1:], SIN[0]) * z * r + r
    c = functools.reduce(lambda a, p: a * z + p, COS[1:], COS[0]) * z * z - 0.5 * z + 1.0
    m = n.astype(jnp.int32)
    odd = (m & 1) == 1
    cs = jnp.where(odd, s, c)
    sn = jnp.where(odd, c, s)
    return jnp.where(((m + 1) & 2) == 2, -cs, cs), jnp.where((m & 2) == 2, -sn, sn)


def _al(v, m):
    return pl.multiple_of(v, m)


def _first(ref, n):
    return ref.at[pl.ds(0, n)]


def _kernel(tp, dp, zn, split, l1, l2, w2, w3, w4,
            x_ref, pos_ref, inv_ref, g1_ref, g2_ref, wq_ref, wk_ref, wv_ref, wo_ref, wg_ref, wu_ref, wd_ref,
            y_ref, y_vm, k_ref, v_ref, oall_ref,
            pos_v, inv_v, g1_v, g2_v, wo_v, wg_v, wu_v, wd_v, g_scr, a_buf, o_buf,
            hbuf, rsib, rs_far, rs_near, rs_sum,
            ld_s, ld_w, ld_mlp, ld_x, kv_s,
            wo_d, wo_s, wo_r, wo_fs, wo_fr, wo_ps, wo_pr,
            o_s, o_sx, o_r, o_f, o_rs, o_rel, o_fwd,
            ld_o, h_s, h_r, r_s, r_r, part_s, far_r, near_r, sum_s, sum_r,
            y_s, y_r, y_f, y_rs, y_rel, y_fwd):
    t, d = x_ref.shape
    qw = wq_ref.shape[1]
    f = wg_ref.shape[1]
    hl = qw // HEAD
    b = BLOCK
    nb = t // b
    dh = d // 2
    hb = b // 2
    fh = f // 2
    nc = tp // 2
    ow = hb // nc
    hw = ow // 2
    kvt = 2 * b

    wd_late = y_vm.at[pl.ds((nb - split) * b - fh, fh)]

    r = lax.axis_index("tp")
    c = r // 2
    s = r % 2
    c_r = (c + 1) % nc
    c_l = (c + nc - 1) % nc
    c_o = (c + 2) % nc
    dest = ({"tp": c_r * 2 + s}, {"tp": c_l * 2 + s})
    origin = (c_l, c_r)
    target = (c_r, c_l)
    sib = {"tp": c * 2 + 1 - s}
    dpi = lax.axis_index("dp")
    par = dpi % 2
    peers = [{"dp": dpi + 1 - 2 * par}] if dp % 2 == 0 else []
    if zn:
        par_y = (dpi // zn) % 2
        peers.append({"dp": dpi + zn * (1 - 2 * par_y)})

    def send(src, dst, ss, rs, dev):
        pltpu.make_async_remote_copy(
            src_ref=src, dst_ref=dst, send_sem=ss, recv_sem=rs, device_id=dev, device_id_type=MESH).start()

    def put(src, dst, sem):
        pltpu.make_async_copy(src, dst, sem).start()

    def wait(region, sem, tag=None):
        with jax.named_scope("w_" + (tag or "end")):
            pltpu.make_async_copy(region, region, sem).wait()

    def when_block(j, body):
        @pl.when((j >= 0) & (j < nb))
        def _():
            body()

    barrier = pltpu.get_barrier_semaphore()
    cross = [{"tp": target[e] * 2 + 1 - s} for e in SIDES]
    others = [*dest, *cross, sib, *peers]
    for dev in others:
        pl.semaphore_signal(barrier, inc=1, device_id=dev, device_id_type=MESH)

    small = ((pos_ref, pos_v), (inv_ref, inv_v), (g1_ref, g1_v), (g2_ref, g2_v))
    for e, (src, dst) in enumerate(small):
        put(src, dst, ld_s.at[e])
    with jax.named_scope("barrier"):
        pl.semaphore_wait(barrier, len(others))

    mine = _al(s * dh, LANES)
    other = _al((1 - s) * dh, LANES)
    parts = 4 if zn else len(peers) + 1
    wr = qw // parts
    part = (2 * par_y + par) if zn else (par if peers else 0)

    def shard(dev):
        return wo_v.at[pl.ds(_al(dev * qw, LANES), qw)]

    def piece(chip, core, q=None):
        return wo_v.at[pl.ds(_al((chip * 2 + core) * qw + (part if q is None else q) * wr, 32), wr)]

    rows = pl.ds(_al(part * wr, 32), wr)
    for e in SIDES:
        for k, (cols, dev) in enumerate(((mine, dest[e]), (other, cross[e]))):
            send(wo_ref.at[rows, pl.ds(cols, dh)], piece(c, s), wo_s.at[e, k], wo_r.at[e, s], dev)
    send(wo_ref.at[:, pl.ds(other, dh)], shard(r), wo_d.at[0], wo_d.at[1], sib)
    put(wo_ref.at[:, pl.ds(mine, dh)], shard(r), wo_d.at[2])

    def wo_swap(chip):
        for e, dev in enumerate(peers):
            for core in SIDES:
                send(piece(chip, core), piece(chip, core), wo_ps.at[0, e], wo_pr.at[0, e], dev)

    def wo_stage2():
        for e in SIDES:
            for core in SIDES:
                wait(piece(origin[e], core), wo_r.at[e, core], "wo2")
            reg = piece(origin[e], e)
            send(reg, reg, wo_fs.at[e], wo_fr.at[e], dest[e])
            wo_swap(origin[e])

    def wo_stage3():
        for e in SIDES:
            wait(piece(c_o, e), wo_fr.at[e], "wo3")
        wo_swap(c_o)

    def wo_stage4():
        for e in range(len(peers)):
            wait(_first(wo_v, 6 * wr), wo_pr.at[0, e], "wo4")
        if zn:
            for chip in (*origin, c_o):
                for e, q in enumerate((2 * (1 - par_y) + par, 2 * par_y + 1 - par)):
                    reg = piece(chip, e, q)
                    send(reg, reg, wo_ps.at[1, e], wo_pr.at[1, e], peers[e])

    def wo_end(which):
        for e in SIDES if zn else ():
            wait(_first(wo_v, 3 * wr), which.at[1, e], "wo5")

    def ocol(chip, core):
        return pl.ds(_al((chip * 2 + core) * qw, LANES), qw)

    def oreg(j, chip):
        return oall_ref.at[pl.ds(_al(j * b, b), b), ocol(chip, s)]

    def ohalf(j, chip, half):
        return oall_ref.at[pl.ds(_al(j * b + half * hb, hb), hb), ocol(chip, s)]

    def orow(j):
        return pl.ds(_al(j * b, b), b)

    def o_stage2(j):
        def body():
            for e in SIDES:
                reg = oreg(j, origin[e])
                wait(reg, o_r.at[e, j], "o2")
                half = ohalf(j, origin[e], e)
                send(half, half, o_rel.at[e], o_f.at[e, j], dest[e])
                send(reg, reg, o_fwd, o_rs.at[j], sib)

        when_block(j, body)

    def o_stage3(j):
        def body():
            for e in SIDES:
                wait(ohalf(j, c_o, e), o_f.at[e, j], "o3")
            send(oreg(j, c_o), oreg(j, c_o), o_fwd, o_rs.at[j], sib)

        when_block(j, body)

    def unrolled(n, body):
        for e in range(n):
            body(e)

    def norm_rows(src, which):
        def step(e, carry):
            for q in range(NR // SUB):
                rows = pl.ds(_al(e * NR + q * SUB, SUB), SUB)
                v32 = src[rows, :].astype(F32)
                inv = lax.rsqrt(jnp.mean(v32 * v32, axis=1, keepdims=True) + EPS)
                a_buf[rows, :] = (v32 * inv * g_scr[which:which + 1, :]).astype(BF)
            return carry

        with jax.named_scope("norm"):
            lax.fori_loop(0, b // NR, step, 0)

    for e, (src, dst) in enumerate(small):
        wait(dst, ld_s.at[e], "small")
    for e, ref in enumerate((g1_v, g2_v)):
        g_scr[e:e + 1, :] = ref[...].astype(F32).reshape(1, d)

    def attention(wqkv, x_buf, q_scr, k_scr, v_scr, m_scr, l_scr, acc_scr):
        rk = _al(r * HEAD, HEAD)
        wq_dst = wqkv.at[:, pl.ds(0, qw)]
        kv_dst = [wqkv.at[:, pl.ds(qw + e * HEAD, HEAD)] for e in SIDES]
        put(_first(x_ref, b), x_buf, ld_x)
        put(wq_ref, wq_dst, ld_w.at[2])
        for e, ref in enumerate((wk_ref, wv_ref)):
            put(ref.at[:, pl.ds(rk, HEAD)], kv_dst[e], ld_w.at[e])
        caches = ((k_scr, k_ref), (v_scr, v_ref))
        mlp = ((wg_ref, wg_v), (wu_ref, wu_v), (_first(wd_ref, fh), wd_v), (wd_ref.at[pl.ds(fh, fh)], wd_late))
        scale = HEAD ** -0.5 * LOG2E
        lane = lax.broadcasted_iota(jnp.int32, (b, HEAD), 1)

        def heads(ref, h):
            return ref.at[pl.ds(h * b, b)]

        def tile(first, n, masked=False):
            keys = pl.ds(_al(first, n), n)
            kk = k_scr[keys, :]
            vv = v_scr[keys, :]
            sc = lax.dot_general(q_scr[...], kk, (((1,), (1,)), ((), ())), preferred_element_type=F32)
            if masked:
                keep = lax.broadcasted_iota(jnp.int32, (b, n), 1) <= lax.broadcasted_iota(jnp.int32, (b, n), 0)
                sc = jnp.concatenate([jnp.where(keep, sc[h * b:(h + 1) * b], -jnp.inf) for h in range(hl)], axis=0)
            m_prev = m_scr[...]
            m_new = jnp.maximum(m_prev, jnp.max(sc, axis=1, keepdims=True))
            ps = [jnp.exp2((sc[:, e * HEAD:(e + 1) * HEAD] - m_new) * scale) for e in range(n // HEAD)]
            alpha = jnp.exp2((m_prev - m_new) * scale)
            l_scr[...] = l_scr[...] * alpha + functools.reduce(lambda p, q: p + q, ps)
            pr = jnp.concatenate([p.astype(BF) for p in ps], axis=1)
            acc_scr[...] = acc_scr[...] * alpha + jnp.dot(pr, vv, preferred_element_type=F32)
            m_scr[...] = m_new

        def phase1(i, carry):
            with jax.named_scope("slot1"):
                phase1_slot(i)
            return carry

        def phase1_slot(i):
            wait(x_buf, ld_x, "x")
            norm_rows(x_buf, 0)

            @pl.when(i + 1 < nb)
            def _():
                put(x_ref.at[pl.ds(_al((i + 1) * b, b), b)], x_buf, ld_x)

            @pl.when(i == 0)
            def _():
                wait(wq_dst, ld_w.at[2], "w")
                for e in SIDES:
                    wait(kv_dst[e], ld_w.at[e], "w")

            for e, (src, dst) in enumerate(mlp):
                @pl.when(i == min(w2 + e, nb - 1))
                def _(src=src, dst=dst, e=e):
                    put(src, dst, ld_mlp.at[e])

            pcol = []
            for e in range(b // LANES):
                prow = pos_v[pl.ds(i * (b // LANES) + e, 1), :].astype(F32)
                pcol.append(jnp.transpose(jnp.broadcast_to(prow, (LANES, LANES))))
            co, si = _sincos(jnp.concatenate(pcol, axis=0) * inv_v[...])
            si = jnp.where(lane < HEAD // 2, -si, si)
            qk32 = jnp.dot(a_buf[...], wqkv[:, :qw + HEAD], preferred_element_type=F32)
            v32 = jnp.dot(a_buf[...], wqkv[:, qw + HEAD:], preferred_element_type=F32)
            rows = pl.ds(_al(i * b, b), b)
            for h in range(hl + 1):
                head = qk32[:, h * HEAD:(h + 1) * HEAD]
                head = (head * co + pltpu.roll(head, HEAD // 2, 1) * si).astype(BF)
                if h < hl:
                    heads(q_scr, h)[...] = head
                else:
                    k_scr[rows, :] = head
            v_scr[rows, :] = v32.astype(BF)
            for e, (src, dst) in enumerate(caches):
                @pl.when(i > 0)
                def _(src=src, e=e):
                    wait(_first(src, b), kv_s.at[e])

                put(src.at[rows], dst.at[rows], kv_s.at[e])
            m_scr[...] = jnp.full(m_scr.shape, -jnp.inf, F32)
            l_scr[...] = jnp.zeros(l_scr.shape, F32)
            acc_scr[...] = jnp.zeros(acc_scr.shape, F32)
            full = i // 2

            def inner(j, carry):
                for e in SIDES:
                    tile((2 * j + e) * kvt, kvt)
                return carry

            with jax.named_scope("tiles"):
                lax.fori_loop(0, full // 2, inner, 0)

            @pl.when(full % 2 == 1)
            def _():
                tile((full - 1) * kvt, kvt)

            @pl.when(i % 2 == 1)
            def _():
                tile((i - 1) * b, b)

            tile(i * b, b, masked=True)
            for h in range(hl):
                o_buf[rows, h * HEAD:(h + 1) * HEAD] = (
                    heads(acc_scr, h)[...] / jnp.sum(heads(l_scr, h)[...], axis=1, keepdims=True)).astype(BF)
            src = o_buf.at[rows]
            dst = oreg(i, c)
            for e in SIDES:
                send(src, dst, o_s.at[e], o_r.at[e, i], dest[e])
            send(src, dst, o_sx.at[0], o_rs.at[i], sib)
            put(src, dst, o_sx.at[1])
            for when, stage in ((w2, wo_stage2), (w3, wo_stage3), (w4, wo_stage4)):
                pl.when(i == when)(stage)
            o_stage2(i - l1)
            o_stage3(i - l2)

        lax.fori_loop(0, nb, phase1, 0)
        for e, (src, _) in enumerate(caches):
            wait(_first(src, b), kv_s.at[e])

    loc = pltpu.VMEM
    pl.run_scoped(
        attention, loc((d, qw + 2 * HEAD), BF), loc((b, d), BF), loc((hl * b, HEAD), BF), loc((t, HEAD), BF),
        loc((t, HEAD), BF), *[loc((hl * b, HEAD), F32)] * 3)
    wait(o_buf, o_sx.at[1])
    for e, dst in enumerate((wg_v, wu_v, wd_v, wd_late)):
        wait(dst, ld_mlp.at[e])
    wait(shard(r + 1 - 2 * s), wo_d.at[1])
    wait(shard(r), wo_d.at[2])
    wo_end(wo_pr)

    def rest(o_blk, xh, u_buf, r_buf, cp, sums, ych, hst):
        def load_o(j):
            wait(oall_ref.at[orow(j), pl.ds(0, 4 * qw)], o_rs.at[j], "os")
            put(oall_ref.at[orow(j)], o_blk, ld_o.at[0])
            put(x_ref.at[orow(j), pl.ds(mine, dh)], xh, ld_o.at[1])

        nt_h = min(512, dh)
        nt_f = min(512, f)
        nt_d = min(512, d)

        def cpart(j, chip, half):
            return cp.at[j % CHIP, pl.ds(_al(chip * ow + half * hw, hw), hw)]

        def sum_start(j):
            def body():
                two = j % 2
                q4 = j % SLOTS
                wait(rsib.at[two], r_r.at[two], "r")
                wait(rsib.at[two], r_s, "rs")

                def add(e, carry):
                    rows = pl.ds(_al(e * SUB, SUB), SUB)
                    own = r_buf[pl.ds(_al(s * hb + e * SUB, SUB), SUB), :]
                    cp[j % CHIP, rows, :] = (own.astype(F32) + rsib[two, rows, :].astype(F32)).astype(BF)
                    return carry

                with jax.named_scope("add"):
                    lax.fori_loop(0, hb // SUB, add, 0)
                for e in SIDES:
                    send(cpart(j, c_o, e), rs_far.at[q4, e], part_s.at[q4], far_r.at[q4, e], dest[e])
                for e in SIDES:
                    send(cpart(j, target[e], 1 - e), rs_near.at[q4, e], part_s.at[q4], near_r.at[q4, e], dest[e])

            when_block(j, body)

        def own_h(j):
            @pl.when(j < nb)
            def _():
                wait(o_blk, ld_o.at[0], "ldo")
                wait(xh, ld_o.at[1], "ldo")

                def col(n):
                    cols = pl.ds(n * nt_h, nt_h)
                    v32 = jnp.dot(o_blk[...], wo_v[:, cols], preferred_element_type=F32)
                    hbuf[j % 2, :, pl.ds(_al(s * dh + n * nt_h, LANES), nt_h)] = (xh[:, cols].astype(F32) + v32).astype(BF)

                with jax.named_scope("own_h"):
                    unrolled(dh // nt_h, col)

        def swap_h(j):
            @pl.when(j < nb)
            def _():
                half = hbuf.at[j % 2, :, pl.ds(mine, dh)]
                send(half, half, h_s.at[j % 2], h_r.at[j % 2], sib)

            @pl.when(j + 1 < nb)
            def _():
                load_o(j + 1)

        def mlp_norm(j):
            def body():
                two = j % 2
                wait(hbuf.at[two, :, pl.ds(other, dh)], h_r.at[two], "h")
                wait(hbuf.at[two, :, pl.ds(mine, dh)], h_s.at[two], "hs")
                norm_rows(hbuf.at[two], 1)
                hst[j % SLOTS] = hbuf[two, pl.ds(_al(s * hb + c * ow, SUB), ow), :]

            when_block(j, body)

        def mlp_up(j):
            def body():
                def col(n):
                    cols = pl.ds(n * nt_f, nt_f)
                    gt = jnp.dot(a_buf[...], wg_v[:, cols], preferred_element_type=F32)
                    up = jnp.dot(a_buf[...], wu_v[:, cols], preferred_element_type=F32)
                    u_buf[:, cols] = (gt * (1.0 / (1.0 + jnp.exp(-gt))) * up).astype(BF)

                with jax.named_scope("up"):
                    unrolled(f // nt_f, col)

            when_block(j, body)

        def mlp_down(j):
            def body():
                def col(n):
                    cols = pl.ds(n * nt_d, nt_d)
                    r32 = jnp.dot(u_buf[:, :fh], wd_v[:, cols], preferred_element_type=F32)
                    r32 = r32 + jnp.dot(u_buf[:, fh:], wd_late[:, cols], preferred_element_type=F32)
                    r_buf[:, cols] = r32.astype(BF)

                with jax.named_scope("down"):
                    unrolled(d // nt_d, col)
                send(r_buf.at[pl.ds(_al((1 - s) * hb, hb), hb)], rsib.at[j % 2], r_s, r_r.at[j % 2], sib)

            when_block(j, body)

        def sum_relay(j):
            def body():
                q4 = j % SLOTS
                two = j % 2

                @pl.when(j >= 2)
                def _():
                    wait(sums.at[two], sum_s.at[two], "sums")

                for e in SIDES:
                    wait(rs_far.at[q4, e], far_r.at[q4, e], "s1")
                    sums[two, e] = (rs_far[q4, e].astype(F32) + cpart(j, target[e], e)[...].astype(F32)).astype(BF)
                    send(sums.at[two, e], rs_sum.at[q4, e], sum_s.at[two], sum_r.at[q4, e], dest[e])

            when_block(j, body)

        def on_y(j, body):
            @pl.when((j >= 0) & (j < split))
            def _():
                body(y_ref, j * b, False)

            @pl.when((j >= split) & (j < nb))
            def _():
                body(y_vm, (j - split) * b, True)

        def yrow(ref, row, chip):
            return ref.at[pl.ds(_al(row + s * hb + chip * ow, ow), ow)]

        def yhalf(ref, row, chip, half):
            return ref.at[pl.ds(_al(row + s * hb + chip * ow + half * hw, hw), hw)]

        def y_sent(j, vmem):
            wait(cp.at[0, pl.ds(0, (3 if vmem else 4) * ow)], y_s.at[j % SLOTS], "ysent")

        def sum_end(j):
            @pl.when((j >= 2) & (j < split + 2))
            def _():
                y_sent(j - 2, False)

            @pl.when((j >= split + SLOTS) & (j < nb))
            def _():
                y_sent(j - SLOTS, True)

            def body(ref, row, vmem):
                q4 = j % SLOTS
                wait(cp.at[0, pl.ds(0, 4 * hw)], part_s.at[q4], "s1s")
                for e in SIDES:
                    wait(rs_near.at[q4, e], near_r.at[q4, e], "s2")
                    wait(rs_sum.at[q4, e], sum_r.at[q4, e], "s2")
                own = yrow(ref, row, c)
                src = own if vmem else ych.at[j % 2]
                for e in SIDES:
                    rows = pl.ds(e * hw, hw)
                    tot = cpart(j, c, e)[...].astype(F32) + rs_near[q4, 1 - e].astype(F32) + rs_sum[q4, e].astype(F32)
                    dst = yhalf(ref, row, c, e) if vmem else src.at[rows]
                    dst[...] = (hst[q4, rows, :].astype(F32) + tot).astype(BF)
                for e in SIDES:
                    send(src, own, y_s.at[q4], y_r.at[e, q4], dest[e])
                send(src, own, y_s.at[q4], y_rs.at[j % LATE], sib)
                if not vmem:
                    put(src, own, y_s.at[q4])

            on_y(j, body)

        def y_stage2(j):
            def body(ref, row, vmem):
                for e in SIDES:
                    reg = yrow(ref, row, origin[e])
                    wait(reg, y_r.at[e, j % SLOTS], "y2")
                    half = yhalf(ref, row, origin[e], e)
                    send(half, half, y_rel.at[e], y_f.at[e, j % SLOTS], dest[e])
                    send(reg, reg, y_fwd, y_rs.at[j % LATE], sib)

            on_y(j, body)

        def y_stage3(j):
            def body(ref, row, vmem):
                for e in SIDES:
                    wait(yhalf(ref, row, c_o, e), y_f.at[e, j % SLOTS], "y3")
                reg = yrow(ref, row, c_o)
                send(reg, reg, y_fwd, y_rs.at[j % LATE], sib)

            on_y(j, body)

        def y_seen(j):
            when_block(j, lambda: wait(cp.at[0], y_rs.at[j % LATE], "ys"))

        load_o(0)

        def phase2(i, carry):
            with jax.named_scope("slot2"):
                own_h(i)
                sum_start(i - 2)
                swap_h(i)
                mlp_norm(i - 1)
                sum_relay(i - 3)
                mlp_up(i - 1)
                sum_end(i - 4)
                mlp_down(i - 1)
                y_stage2(i - 5)
                y_stage3(i - 6)
                y_seen(i - LATE)
                o_stage2(nb + i - l1)
                o_stage3(nb + i - l2)
            return carry

        lax.fori_loop(0, nb + 6, phase2, 0)

        for j in range(nb + 6 - LATE, nb):
            wait(cp.at[0], y_rs.at[j % LATE])
        for j in range(max(nb - SLOTS, split), nb):
            y_sent(j, True)
        for e in SIDES:
            wait(sums.at[e], sum_s.at[e])
        for e in SIDES:
            wait(_first(y_vm, nb * hw), y_rel.at[e])
            wait(o_buf, o_s.at[e])
            wait(oall_ref.at[pl.ds(0, t // 2), pl.ds(0, qw)], o_rel.at[e])
            wait(_first(wo_v, wr), wo_fs.at[e])
            for k in SIDES:
                wait(_first(wo_v, wr), wo_s.at[e, k])
        wait(_first(y_vm, nb * ow * 3), y_fwd)
        wait(o_buf, o_sx.at[0])
        wait(oall_ref.at[:, pl.ds(0, 3 * qw)], o_fwd)
        wait(_first(wo_v, qw), wo_d.at[0])
        for e in range(len(peers)):
            wait(_first(wo_v, 6 * wr), wo_ps.at[0, e])
        wo_end(wo_ps)

    pl.run_scoped(
        rest, loc((b, tp * qw), BF), loc((b, dh), BF), loc((b, f), BF), loc((b, d), BF), loc((CHIP, hb, d), BF),
        loc((2, 2, hw, d), BF), loc((2, ow, d), BF), loc((SLOTS, ow, d), BF))


def _held(rows, d):
    return pltpu.VMEM((rows, d), BF)


def _keep(a, space):
    return pltpu.with_memory_space_constraint(a, space)


def _layer(tp, dp, zn, x, pos, inv, g1, g2, wq, wk, wv, wo, wg, wu, wd):
    t, d = x.shape
    qw = wq.shape[1]
    f = wg.shape[1]
    hl = qw // HEAD
    b = BLOCK
    nb = t // b
    hb = b // 2
    nc = tp // 2
    ow = hb // nc
    hw = ow // 2
    dh = d // 2
    assert nc == SLOTS and f <= 4 * b and t % b == 0 and wk.shape[1] == tp * HEAD
    l1 = max(nb // 4, 1)
    l2 = min(nb * 3 // 4, nb - 2)
    hbm = pl.BlockSpec(memory_space=pl.ANY)
    bufs = [
        (tp * qw, dh), (d, f), (d, f), (f // 2, d), None, (b, d), (t, qw),
        (2, b, d), (2, hb, d), *[(SLOTS, 2, hw, d)] * 3,
    ]
    scratch = [pltpu.VMEM(a.shape, a.dtype) for a in (pos, inv, g1, g2)]
    scratch += [pltpu.VMEM((2, d), F32) if shape is None else pltpu.VMEM(shape, BF) for shape in bufs]
    two, four, ring, per = (2,), (SLOTS, 2), (2, nb), (nb,)
    sems = [(4,), (3,), (4,), (), two,
            (3,), (2, 2), (2, 2), two, two, (2, 2), (2, 2),
            two, two, ring, ring, per, two, (),
            two, two, two, (), two, (SLOTS,), four, four, two, four,
            (SLOTS,), (2, SLOTS), (2, SLOTS), (LATE,), two, ()]
    scratch += [pltpu.SemaphoreType.DMA(shape) for shape in sems]
    flops = 2 * t * (d * (qw + 2 * HEAD) + qw * t + tp * qw * dh + 3 * d * f)
    split = nb - Y_VMEM * nb // 16
    outs = [(split * b, d), None, (t, HEAD), (t, HEAD), (t, tp * qw)]
    vm = _held((nb - split) * b, d)
    return pl.pallas_call(
        functools.partial(_kernel, tp, dp, zn, split, l1, l2, nb // 4, nb // 2, nb * 3 // 4),
        name="layer",
        out_shape=tuple(jax.ShapeDtypeStruct(shape, BF) if shape else vm for shape in outs),
        in_specs=[hbm] * 12,
        out_specs=tuple(hbm if shape else pl.BlockSpec(memory_space=pltpu.VMEM) for shape in outs),
        scratch_shapes=scratch,
        compiler_params=pltpu.CompilerParams(collective_id=0, has_side_effects=True,
                                             vmem_limit_bytes=VMEM_BYTES - 2 * (nb - split) * b * d),
        cost_estimate=pl.CostEstimate(flops=flops, bytes_accessed=8 * t * d, transcendentals=t * t * hl),
    )(x, pos, inv, g1, g2, wq, wk, wv, wo, wg, wu, wd)


def _copy_kernel(src, held, k_src, v_src, dst, k_dst, v_dst, buf, kv, rd, wr, kv_sem):
    rows = buf.shape[1]
    steps = src.shape[0] // rows
    small = ((k_src, k_dst), (v_src, v_dst))
    reads, writes, late = [], [], []
    for i in range(steps):
        part = pl.ds(i * rows, rows)
        reads.append(pltpu.make_async_copy(src.at[part], buf.at[i], rd.at[i]))
        writes.append(pltpu.make_async_copy(buf.at[i], dst.at[part], rd.at[i]))
    for e, (a, z) in enumerate(small):
        reads.append(pltpu.make_async_copy(a, kv.at[e], kv_sem.at[e]))
        writes.append(pltpu.make_async_copy(kv.at[e], z, kv_sem.at[e]))
    for i in range(held.shape[0] // rows):
        to = pl.ds(src.shape[0] + i * rows, rows)
        late.append(pltpu.make_async_copy(held.at[pl.ds(i * rows, rows)], dst.at[to], wr.at[i]))
    for copy in reads:
        copy.start()
    for copy in late:
        copy.start()
    for read, write in zip(reads, writes):
        read.wait()
        write.start()
    for copy in (*late, *writes):
        copy.wait()


def _copy(y, held, k, v):
    d = y.shape[1]
    t = y.shape[0] + held.shape[0]
    rows = 256
    hbm = pl.BlockSpec(memory_space=pltpu.HBM)
    dma = pltpu.SemaphoreType.DMA
    n = y.shape[0] // rows
    shapes = ((t, d), k.shape, v.shape)
    return pl.pallas_call(
        _copy_kernel,
        name="copy_out",
        out_shape=tuple(jax.ShapeDtypeStruct(shape, BF) for shape in shapes),
        in_specs=[hbm, pl.BlockSpec(memory_space=pltpu.VMEM), hbm, hbm],
        out_specs=(hbm,) * 3,
        scratch_shapes=[pltpu.VMEM((n, rows, d), BF), pltpu.VMEM((2,) + k.shape, BF),
                        dma((n,)), dma((held.shape[0] // rows,)), dma((2,))],
        compiler_params=pltpu.CompilerParams(vmem_limit_bytes=VMEM_BYTES - 3 * held.size),
        cost_estimate=pl.CostEstimate(flops=0, bytes_accessed=4 * t * d, transcendentals=0),
    )(y, held, k, v)


def _row_length(mesh):
    at = [getattr(dev, "coords", None) for dev in mesh.devices.reshape(mesh.shape["dp"], -1)[:, 0]]
    if any(p is None for p in at):
        return None
    n = len(at)

    def apart(i, j):
        return sum(abs(p - q) for p, q in zip(at[i], at[j]))

    length = next((i for i in range(1, n) if at[i][-1] == at[0][-1]), n)
    if length % 2 or n % (2 * length):
        return None
    rows = all(apart(i, i + 1) == 1 for i in range(0, n, 2))
    across = all(apart(i, i + length) == 1 for i in range(n) if (i // length) % 2 == 0)
    return length if rows and across else None


def solution(mesh):
    tp = mesh.shape["tp"]
    dp = mesh.shape["dp"]
    zn = _row_length(mesh)

    def local(x, pos, g1, g2, wq, wk, wv, wo, wg, wu, wd):
        t = x.shape[0]
        half = ROPE_BASE ** (-2.0 * np.arange(HEAD // 2) / HEAD)
        inv = jnp.asarray(np.concatenate([half, half])[None, :].astype(np.float32))
        y, held, k, v, _ = _layer(tp, dp, zn, x, pos.reshape(t // LANES, LANES), inv, g1, g2, wq, wk, wv, wo, wg, wu, wd)
        y, k, v = (_keep(a, pltpu.HBM) for a in (y, k, v))
        y, k, v = _copy(y, _keep(held, pltpu.VMEM), k, v)
        return y, k.reshape(t, 1, HEAD), v.reshape(t, 1, HEAD)

    return jax.shard_map(
        local,
        mesh=mesh,
        in_specs=(P("dp", None), P("dp"), P(), P(), P(None, "tp"), P(), P(), P("tp", None),
                  P(None, "tp"), P(None, "tp"), P("tp", None)),
        out_specs=(P("dp", None), P("dp", "tp", None), P("dp", "tp", None)),
        check_vma=False,
    )
```

```python
import functools

import jax
import jax.numpy as jnp
import numpy as np
from jax import lax
from jax.experimental import pallas as pl
from jax.experimental.pallas import tpu as pltpu
from jax.sharding import PartitionSpec as P

HEAD = 128
LANES = 128
SUB = 16
EPS = 1e-5
ROPE_BASE = 500000.0
MESH = pl.DeviceIdType.MESH
BLOCK = 256
NR = 64
SLOTS = 4
LATE = 8
CHIP = 3
O_SLOTS = 6
SIDES = (0, 1)
BF = jnp.bfloat16
F32 = jnp.float32
VMEM_BYTES = 67040000
Y_VMEM = 15
TWO_OVER_PI = 0.6366197723675814
PI_2 = (1.5703125, 4.837512969970703125e-4, 7.54978995489188216e-8)
SIN = (-1.9515295891e-4, 8.3321608736e-3, -1.6666654611e-1)
COS = (2.443315711809948e-5, -1.388731625493765e-3, 4.166664568298827e-2)
LOG2E = 1.4426950408889634


def _sincos(ang):
    n = jnp.floor(ang * TWO_OVER_PI + 0.5)
    r = ang
    for p in PI_2:
        r = r - n * p
    z = r * r
    s = functools.reduce(lambda a, p: a * z + p, SIN[1:], SIN[0]) * z * r + r
    c = functools.reduce(lambda a, p: a * z + p, COS[1:], COS[0]) * z * z - 0.5 * z + 1.0
    m = n.astype(jnp.int32)
    odd = (m & 1) == 1
    cs = jnp.where(odd, s, c)
    sn = jnp.where(odd, c, s)
    return jnp.where(((m + 1) & 2) == 2, -cs, cs), jnp.where((m & 2) == 2, -sn, sn)


def _al(v, m):
    return pl.multiple_of(v, m)


def _first(ref, n):
    return ref.at[pl.ds(0, n)]


def _kernel(tp, dp, zn, split, l1, l2, w2, w3, w4,
            x_ref, pos_ref, inv_ref, g1_ref, g2_ref, wq_ref, wk_ref, wv_ref, wo_ref, wg_ref, wu_ref, wd_ref,
            y_ref, y_vm, k_ref, v_ref, oall_ref,
            pos_v, inv_v, g1_v, g2_v, wo_v, wg_v, wu_v, wd_v, g_scr, a_buf, o_buf,
            hbuf, rsib, rs_far, rs_near, rs_sum,
            ld_s, ld_w, ld_mlp, ld_x, kv_s,
            wo_d, wo_s, wo_r, wo_fs, wo_fr, wo_ps, wo_pr,
            o_s, o_loc, o_r, o_f, o_rs, o_rel, o_fwd,
            ld_o, h_s, h_r, r_s, r_r, part_s, far_r, near_r, sum_s, sum_r,
            y_s, y_r, y_f, y_rs, y_rel, y_fwd):
    t, d = x_ref.shape
    qw = wq_ref.shape[1]
    f = wg_ref.shape[1]
    hl = qw // HEAD
    b = BLOCK
    nb = t // b
    dh = d // 2
    hb = b // 2
    fh = f // 2
    nc = tp // 2
    ow = hb // nc
    hw = ow // 2
    kvt = 2 * b

    last_y = (nb - split) * b
    wd_late = y_vm.at[pl.ds(last_y - fh, fh)]
    x_buf = o_blk = y_vm.at[pl.ds(last_y - 4 * b, b)]
    xh = y_vm.at[pl.ds(last_y - 3 * b, b), pl.ds(0, dh)]
    wqkv = wg_v.at[:, pl.ds(0, qw + 2 * HEAD)]

    r = lax.axis_index("tp")
    c = r // 2
    s = r % 2
    c_r = (c + 1) % nc
    c_l = (c + nc - 1) % nc
    c_o = (c + 2) % nc
    dest = ({"tp": c_r * 2 + s}, {"tp": c_l * 2 + s})
    origin = (c_l, c_r)
    target = (c_r, c_l)
    sib = {"tp": c * 2 + 1 - s}
    dpi = lax.axis_index("dp")
    par = dpi % 2
    peers = [{"dp": dpi + 1 - 2 * par}] if dp % 2 == 0 else []
    if zn:
        par_y = (dpi // zn) % 2
        peers.append({"dp": dpi + zn * (1 - 2 * par_y)})

    def send(src, dst, ss, rs, dev):
        pltpu.make_async_remote_copy(
            src_ref=src, dst_ref=dst, send_sem=ss, recv_sem=rs, device_id=dev, device_id_type=MESH).start()

    def put(src, dst, sem):
        pltpu.make_async_copy(src, dst, sem).start()

    def wait(region, sem, tag=None):
        with jax.named_scope("w_" + (tag or "end")):
            pltpu.make_async_copy(region, region, sem).wait()

    def when_block(j, body):
        @pl.when((j >= 0) & (j < nb))
        def _():
            body()

    barrier = pltpu.get_barrier_semaphore()
    cross = [{"tp": target[e] * 2 + 1 - s} for e in SIDES]
    others = [*dest, *cross, sib, *peers]
    for dev in others:
        pl.semaphore_signal(barrier, inc=1, device_id=dev, device_id_type=MESH)

    small = ((pos_ref, pos_v), (inv_ref, inv_v), (g1_ref, g1_v), (g2_ref, g2_v))
    for e, (src, dst) in enumerate(small):
        put(src, dst, ld_s.at[e])
    with jax.named_scope("barrier"):
        pl.semaphore_wait(barrier, len(others))

    mine = _al(s * dh, LANES)
    other = _al((1 - s) * dh, LANES)
    parts = 4 if zn else len(peers) + 1
    wr = qw // parts
    part = (2 * par_y + par) if zn else (par if peers else 0)

    def shard(dev):
        return wo_v.at[pl.ds(_al(dev * qw, LANES), qw)]

    def piece(chip, core, q=None):
        return wo_v.at[pl.ds(_al((chip * 2 + core) * qw + (part if q is None else q) * wr, 32), wr)]

    rows = pl.ds(_al(part * wr, 32), wr)
    for e in SIDES:
        for k, (cols, dev) in enumerate(((mine, dest[e]), (other, cross[e]))):
            send(wo_ref.at[rows, pl.ds(cols, dh)], piece(c, s), wo_s.at[e, k], wo_r.at[e, s], dev)
    send(wo_ref.at[:, pl.ds(other, dh)], shard(r), wo_d.at[0], wo_d.at[1], sib)
    put(wo_ref.at[:, pl.ds(mine, dh)], shard(r), wo_d.at[2])

    def wo_swap(chip):
        for e, dev in enumerate(peers):
            for core in SIDES:
                send(piece(chip, core), piece(chip, core), wo_ps.at[0, e], wo_pr.at[0, e], dev)

    def wo_stage2():
        for e in SIDES:
            for core in SIDES:
                wait(piece(origin[e], core), wo_r.at[e, core], "wo2")
            reg = piece(origin[e], e)
            send(reg, reg, wo_fs.at[e], wo_fr.at[e], dest[e])
            wo_swap(origin[e])

    def wo_stage3():
        for e in SIDES:
            wait(piece(c_o, e), wo_fr.at[e], "wo3")
        wo_swap(c_o)

    def wo_stage4():
        for e in range(len(peers)):
            wait(_first(wo_v, 6 * wr), wo_pr.at[0, e], "wo4")
        if zn:
            for chip in (*origin, c_o):
                for e, q in enumerate((2 * (1 - par_y) + par, 2 * par_y + 1 - par)):
                    reg = piece(chip, e, q)
                    send(reg, reg, wo_ps.at[1, e], wo_pr.at[1, e], peers[e])

    def wo_end(which):
        for e in SIDES if zn else ():
            wait(_first(wo_v, 3 * wr), which.at[1, e], "wo5")

    def ocol(chip, core):
        return pl.ds(_al((chip * 2 + core) * qw, LANES), qw)

    def oreg(j, chip):
        return oall_ref.at[pl.ds(_al(j * b, b), b), ocol(chip, s)]

    def ohalf(j, chip, half):
        return oall_ref.at[pl.ds(_al(j * b + half * hb, hb), hb), ocol(chip, s)]

    def orow(j):
        return pl.ds(_al(j * b, b), b)

    def o_stage2(j):
        def body():
            for e in SIDES:
                reg = oreg(j, origin[e])
                wait(reg, o_r.at[e, j], "o2")
                half = ohalf(j, origin[e], e)
                send(half, half, o_rel.at[e], o_f.at[e, j], dest[e])
                send(reg, reg, o_fwd, o_rs.at[j], sib)

        when_block(j, body)

    def o_stage3(j):
        def body():
            for e in SIDES:
                wait(ohalf(j, c_o, e), o_f.at[e, j], "o3")
            send(oreg(j, c_o), oreg(j, c_o), o_fwd, o_rs.at[j], sib)

        when_block(j, body)

    def unrolled(n, body):
        for e in range(n):
            body(e)

    def norm_rows(src, which):
        def step(e, carry):
            for q in range(NR // SUB):
                rows = pl.ds(_al(e * NR + q * SUB, SUB), SUB)
                v32 = src[rows, :].astype(F32)
                inv = lax.rsqrt(jnp.mean(v32 * v32, axis=1, keepdims=True) + EPS)
                a_buf[rows, :] = (v32 * inv * g_scr[which:which + 1, :]).astype(BF)
            return carry

        with jax.named_scope("norm"):
            lax.fori_loop(0, b // NR, step, 0)

    for e, (src, dst) in enumerate(small):
        wait(dst, ld_s.at[e], "small")
    for e, ref in enumerate((g1_v, g2_v)):
        g_scr[e:e + 1, :] = ref[...].astype(F32).reshape(1, d)

    def attention(q_scr, k_scr, v_scr, m_scr, l_scr, acc_scr):
        rk = _al(r * HEAD, HEAD)
        wq_dst = wqkv.at[:, pl.ds(0, qw)]
        kv_dst = [wqkv.at[:, pl.ds(qw + e * HEAD, HEAD)] for e in SIDES]
        put(_first(x_ref, b), x_buf, ld_x)
        put(wq_ref, wq_dst, ld_w.at[2])
        for e, ref in enumerate((wk_ref, wv_ref)):
            put(ref.at[:, pl.ds(rk, HEAD)], kv_dst[e], ld_w.at[e])
        caches = ((k_scr, k_ref), (v_scr, v_ref))
        mlp = ((wu_ref, wu_v), (_first(wd_ref, fh), wd_v), (wd_ref.at[pl.ds(fh, fh)], wd_late))
        scale = HEAD ** -0.5 * LOG2E
        lane = lax.broadcasted_iota(jnp.int32, (b, HEAD), 1)

        def heads(ref, h):
            return ref.at[pl.ds(h * b, b)]

        def o_sent(slot):
            wait(oall_ref.at[pl.ds(0, 3 * b), pl.ds(0, qw)], o_s.at[slot], "osent")

        def tile(first, n, masked=False):
            keys = pl.ds(_al(first, n), n)
            kk = k_scr[keys, :]
            vv = v_scr[keys, :]
            sc = lax.dot_general(q_scr[...], kk, (((1,), (1,)), ((), ())), preferred_element_type=F32)
            if masked:
                keep = lax.broadcasted_iota(jnp.int32, (b, n), 1) <= lax.broadcasted_iota(jnp.int32, (b, n), 0)
                sc = jnp.concatenate([jnp.where(keep, sc[h * b:(h + 1) * b], -jnp.inf) for h in range(hl)], axis=0)
            m_prev = m_scr[...]
            m_new = jnp.maximum(m_prev, jnp.max(sc, axis=1, keepdims=True))
            ps = [jnp.exp2((sc[:, e * HEAD:(e + 1) * HEAD] - m_new) * scale) for e in range(n // HEAD)]
            alpha = jnp.exp2((m_prev - m_new) * scale)
            l_scr[...] = l_scr[...] * alpha + functools.reduce(lambda p, q: p + q, ps)
            pr = jnp.concatenate([p.astype(BF) for p in ps], axis=1)
            acc_scr[...] = acc_scr[...] * alpha + jnp.dot(pr, vv, preferred_element_type=F32)
            m_scr[...] = m_new

        def phase1(i, carry):
            with jax.named_scope("slot1"):
                phase1_slot(i)
            return carry

        def phase1_slot(i):
            wait(x_buf, ld_x, "x")
            norm_rows(x_buf, 0)

            @pl.when(i + 1 < nb)
            def _():
                put(x_ref.at[pl.ds(_al((i + 1) * b, b), b)], x_buf, ld_x)

            @pl.when(i == 0)
            def _():
                wait(wq_dst, ld_w.at[2], "w")
                for e in SIDES:
                    wait(kv_dst[e], ld_w.at[e], "w")

            for e, (src, dst) in enumerate(mlp):
                @pl.when(i == min(w2 + e, nb - 1))
                def _(src=src, dst=dst, e=e):
                    put(src, dst, ld_mlp.at[e])

            pcol = []
            for e in range(b // LANES):
                prow = pos_v[pl.ds(i * (b // LANES) + e, 1), :].astype(F32)
                pcol.append(jnp.transpose(jnp.broadcast_to(prow, (LANES, LANES))))
            co, si = _sincos(jnp.concatenate(pcol, axis=0) * inv_v[...])
            si = jnp.where(lane < HEAD // 2, -si, si)
            qk32 = jnp.dot(a_buf[...], wg_v[:, :qw + HEAD], preferred_element_type=F32)
            v32 = jnp.dot(a_buf[...], wg_v[:, qw + HEAD:qw + 2 * HEAD], preferred_element_type=F32)
            rows = pl.ds(_al(i * b, b), b)
            for h in range(hl + 1):
                head = qk32[:, h * HEAD:(h + 1) * HEAD]
                head = (head * co + pltpu.roll(head, HEAD // 2, 1) * si).astype(BF)
                if h < hl:
                    heads(q_scr, h)[...] = head
                else:
                    k_scr[rows, :] = head
            v_scr[rows, :] = v32.astype(BF)
            for e, (src, dst) in enumerate(caches):
                @pl.when(i > 0)
                def _(src=src, e=e):
                    wait(_first(src, b), kv_s.at[e])

                put(src.at[rows], dst.at[rows], kv_s.at[e])
            m_scr[...] = jnp.full(m_scr.shape, -jnp.inf, F32)
            l_scr[...] = jnp.zeros(l_scr.shape, F32)
            acc_scr[...] = jnp.zeros(acc_scr.shape, F32)
            full = i // 2

            def inner(j, carry):
                for e in SIDES:
                    tile((2 * j + e) * kvt, kvt)
                return carry

            with jax.named_scope("tiles"):
                lax.fori_loop(0, full // 2, inner, 0)

            @pl.when(full % 2 == 1)
            def _():
                tile((full - 1) * kvt, kvt)

            @pl.when(i % 2 == 1)
            def _():
                tile((i - 1) * b, b)

            tile(i * b, b, masked=True)
            slot = i % O_SLOTS

            @pl.when(i >= O_SLOTS)
            def _():
                o_sent(slot)

            @pl.when(i > 0)
            def _():
                wait(o_buf.at[0], o_loc, "oloc")

            for h in range(hl):
                o_buf[slot, :, h * HEAD:(h + 1) * HEAD] = (
                    heads(acc_scr, h)[...] / jnp.sum(heads(l_scr, h)[...], axis=1, keepdims=True)).astype(BF)
            src = o_buf.at[slot]
            dst = oreg(i, c)
            for e in SIDES:
                send(src, dst, o_s.at[slot], o_r.at[e, i], dest[e])
            send(src, dst, o_s.at[slot], o_rs.at[i], sib)
            put(src, dst, o_loc)
            for when, stage in ((w2, wo_stage2), (w3, wo_stage3), (w4, wo_stage4)):
                pl.when(i == when)(stage)
            o_stage2(i - l1)
            o_stage3(i - l2)

        lax.fori_loop(0, nb, phase1, 0)
        put(wg_ref, wg_v, ld_mlp.at[3])
        for e, (src, _) in enumerate(caches):
            wait(_first(src, b), kv_s.at[e])

    loc = pltpu.VMEM
    pl.run_scoped(
        attention, loc((hl * b, HEAD), BF), loc((t, HEAD), BF),
        loc((t, HEAD), BF), *[loc((hl * b, HEAD), F32)] * 3)
    wait(o_buf.at[0], o_loc)
    wait(shard(r + 1 - 2 * s), wo_d.at[1])
    wait(shard(r), wo_d.at[2])
    wo_end(wo_pr)

    def rest(u_buf, r_buf, cp, sums, ych, hst):
        def load_o(j):
            wait(oall_ref.at[orow(j), pl.ds(0, 4 * qw)], o_rs.at[j], "os")
            put(oall_ref.at[orow(j)], o_blk, ld_o.at[0])
            put(x_ref.at[orow(j), pl.ds(mine, dh)], xh, ld_o.at[1])

        nt_h = min(512, dh)
        nt_f = min(512, f)
        nt_d = min(512, d)

        def cpart(j, chip, half):
            return cp.at[j % CHIP, pl.ds(_al(chip * ow + half * hw, hw), hw)]

        def sum_start(j):
            def body():
                two = j % 2
                q4 = j % SLOTS
                wait(rsib.at[two], r_r.at[two], "r")
                wait(rsib.at[two], r_s, "rs")

                def add(e, carry):
                    rows = pl.ds(_al(e * SUB, SUB), SUB)
                    own = r_buf[pl.ds(_al(s * hb + e * SUB, SUB), SUB), :]
                    cp[j % CHIP, rows, :] = (own.astype(F32) + rsib[two, rows, :].astype(F32)).astype(BF)
                    return carry

                with jax.named_scope("add"):
                    lax.fori_loop(0, hb // SUB, add, 0)
                for e in SIDES:
                    send(cpart(j, c_o, e), rs_far.at[q4, e], part_s.at[q4], far_r.at[q4, e], dest[e])
                for e in SIDES:
                    send(cpart(j, target[e], 1 - e), rs_near.at[q4, e], part_s.at[q4], near_r.at[q4, e], dest[e])

            when_block(j, body)

        def own_h(j):
            @pl.when(j < nb)
            def _():
                wait(o_blk, ld_o.at[0], "ldo")
                wait(xh, ld_o.at[1], "ldo")

                def col(n):
                    cols = pl.ds(n * nt_h, nt_h)
                    v32 = jnp.dot(o_blk[...], wo_v[:, cols], preferred_element_type=F32)
                    hbuf[j % 2, :, pl.ds(_al(s * dh + n * nt_h, LANES), nt_h)] = (xh[:, cols].astype(F32) + v32).astype(BF)

                with jax.named_scope("own_h"):
                    unrolled(dh // nt_h, col)

        def swap_h(j):
            @pl.when(j < nb)
            def _():
                half = hbuf.at[j % 2, :, pl.ds(mine, dh)]
                send(half, half, h_s.at[j % 2], h_r.at[j % 2], sib)

            @pl.when(j + 1 < nb)
            def _():
                load_o(j + 1)

        def mlp_norm(j):
            def body():
                two = j % 2
                wait(hbuf.at[two, :, pl.ds(other, dh)], h_r.at[two], "h")
                wait(hbuf.at[two, :, pl.ds(mine, dh)], h_s.at[two], "hs")

                @pl.when(j == 0)
                def _():
                    for e, dst in enumerate((wu_v, wd_v, wd_late, wg_v)):
                        wait(dst, ld_mlp.at[e], "mlp")

                norm_rows(hbuf.at[two], 1)
                hst[j % SLOTS] = hbuf[two, pl.ds(_al(s * hb + c * ow, SUB), ow), :]

            when_block(j, body)

        def mlp_up(j):
            def body():
                def col(n):
                    cols = pl.ds(n * nt_f, nt_f)
                    gt = jnp.dot(a_buf[...], wg_v[:, cols], preferred_element_type=F32)
                    up = jnp.dot(a_buf[...], wu_v[:, cols], preferred_element_type=F32)
                    u_buf[:, cols] = (gt * (1.0 / (1.0 + jnp.exp(-gt))) * up).astype(BF)

                with jax.named_scope("up"):
                    unrolled(f // nt_f, col)

            when_block(j, body)

        def mlp_down(j):
            def body():
                def col(n):
                    cols = pl.ds(n * nt_d, nt_d)
                    r32 = jnp.dot(u_buf[:, :fh], wd_v[:, cols], preferred_element_type=F32)
                    r32 = r32 + jnp.dot(u_buf[:, fh:], wd_late[:, cols], preferred_element_type=F32)
                    r_buf[:, cols] = r32.astype(BF)

                with jax.named_scope("down"):
                    unrolled(d // nt_d, col)
                send(r_buf.at[pl.ds(_al((1 - s) * hb, hb), hb)], rsib.at[j % 2], r_s, r_r.at[j % 2], sib)

            when_block(j, body)

        def sum_relay(j):
            def body():
                q4 = j % SLOTS
                two = j % 2

                @pl.when(j >= 2)
                def _():
                    wait(sums.at[two], sum_s.at[two], "sums")

                for e in SIDES:
                    wait(rs_far.at[q4, e], far_r.at[q4, e], "s1")
                    sums[two, e] = (rs_far[q4, e].astype(F32) + cpart(j, target[e], e)[...].astype(F32)).astype(BF)
                    send(sums.at[two, e], rs_sum.at[q4, e], sum_s.at[two], sum_r.at[q4, e], dest[e])

            when_block(j, body)

        def on_y(j, body):
            @pl.when((j >= 0) & (j < split))
            def _():
                body(y_ref, j * b, False)

            @pl.when((j >= split) & (j < nb))
            def _():
                body(y_vm, (j - split) * b, True)

        def yrow(ref, row, chip):
            return ref.at[pl.ds(_al(row + s * hb + chip * ow, ow), ow)]

        def yhalf(ref, row, chip, half):
            return ref.at[pl.ds(_al(row + s * hb + chip * ow + half * hw, hw), hw)]

        def y_sent(j, vmem):
            wait(cp.at[0, pl.ds(0, (3 if vmem else 4) * ow)], y_s.at[j % SLOTS], "ysent")

        def sum_end(j):
            @pl.when((j >= 2) & (j < split + 2))
            def _():
                y_sent(j - 2, False)

            @pl.when((j >= split + SLOTS) & (j < nb))
            def _():
                y_sent(j - SLOTS, True)

            def body(ref, row, vmem):
                q4 = j % SLOTS
                wait(cp.at[0, pl.ds(0, 4 * hw)], part_s.at[q4], "s1s")
                for e in SIDES:
                    wait(rs_near.at[q4, e], near_r.at[q4, e], "s2")
                    wait(rs_sum.at[q4, e], sum_r.at[q4, e], "s2")
                own = yrow(ref, row, c)
                src = own if vmem else ych.at[j % 2]
                for e in SIDES:
                    rows = pl.ds(e * hw, hw)
                    tot = cpart(j, c, e)[...].astype(F32) + rs_near[q4, 1 - e].astype(F32) + rs_sum[q4, e].astype(F32)
                    dst = yhalf(ref, row, c, e) if vmem else src.at[rows]
                    dst[...] = (hst[q4, rows, :].astype(F32) + tot).astype(BF)
                for e in SIDES:
                    send(src, own, y_s.at[q4], y_r.at[e, q4], dest[e])
                send(src, own, y_s.at[q4], y_rs.at[j % LATE], sib)
                if not vmem:
                    put(src, own, y_s.at[q4])

            on_y(j, body)

        def y_stage2(j):
            def body(ref, row, vmem):
                for e in SIDES:
                    reg = yrow(ref, row, origin[e])
                    wait(reg, y_r.at[e, j % SLOTS], "y2")
                    half = yhalf(ref, row, origin[e], e)
                    send(half, half, y_rel.at[e], y_f.at[e, j % SLOTS], dest[e])
                    send(reg, reg, y_fwd, y_rs.at[j % LATE], sib)

            on_y(j, body)

        def y_stage3(j):
            def body(ref, row, vmem):
                for e in SIDES:
                    wait(yhalf(ref, row, c_o, e), y_f.at[e, j % SLOTS], "y3")
                reg = yrow(ref, row, c_o)
                send(reg, reg, y_fwd, y_rs.at[j % LATE], sib)

            on_y(j, body)

        def y_seen(j):
            when_block(j, lambda: wait(cp.at[0], y_rs.at[j % LATE], "ys"))

        load_o(0)

        def phase2(i, carry):
            with jax.named_scope("slot2"):
                own_h(i)
                sum_start(i - 2)
                swap_h(i)
                mlp_norm(i - 1)
                sum_relay(i - 3)
                mlp_up(i - 1)
                sum_end(i - 4)
                mlp_down(i - 1)
                y_stage2(i - 5)
                y_stage3(i - 6)
                y_seen(i - LATE)
                o_stage2(nb + i - l1)
                o_stage3(nb + i - l2)
            return carry

        lax.fori_loop(0, nb + 6, phase2, 0)

        for j in range(nb + 6 - LATE, nb):
            wait(cp.at[0], y_rs.at[j % LATE])
        for j in range(max(nb - SLOTS, split), nb):
            y_sent(j, True)
        for e in SIDES:
            wait(sums.at[e], sum_s.at[e])
        for e in SIDES:
            wait(_first(y_vm, nb * hw), y_rel.at[e])
            wait(oall_ref.at[pl.ds(0, t // 2), pl.ds(0, qw)], o_rel.at[e])
            wait(_first(wo_v, wr), wo_fs.at[e])
            for k in SIDES:
                wait(_first(wo_v, wr), wo_s.at[e, k])
        wait(_first(y_vm, nb * ow * 3), y_fwd)
        for e in range(O_SLOTS):
            wait(oall_ref.at[pl.ds(0, 3 * b), pl.ds(0, qw)], o_s.at[e])
        wait(oall_ref.at[:, pl.ds(0, 3 * qw)], o_fwd)
        wait(_first(wo_v, qw), wo_d.at[0])
        for e in range(len(peers)):
            wait(_first(wo_v, 6 * wr), wo_ps.at[0, e])
        wo_end(wo_ps)

    pl.run_scoped(
        rest, loc((b, f), BF), loc((b, d), BF), loc((CHIP, hb, d), BF),
        loc((2, 2, hw, d), BF), loc((2, ow, d), BF), loc((SLOTS, ow, d), BF))


def _held(rows, d):
    return pltpu.VMEM((rows, d), BF)


def _keep(a, space):
    return pltpu.with_memory_space_constraint(a, space)


def _layer(tp, dp, zn, x, pos, inv, g1, g2, wq, wk, wv, wo, wg, wu, wd):
    t, d = x.shape
    qw = wq.shape[1]
    f = wg.shape[1]
    hl = qw // HEAD
    b = BLOCK
    nb = t // b
    hb = b // 2
    nc = tp // 2
    ow = hb // nc
    hw = ow // 2
    dh = d // 2
    assert nc == SLOTS and f <= 4 * b and nb > SLOTS and tp * qw == d and t % b == 0 and wk.shape[1] == tp * HEAD
    l1 = max(nb // 4, 1)
    l2 = min(nb * 3 // 4, nb - 2)
    hbm = pl.BlockSpec(memory_space=pl.ANY)
    bufs = [
        (tp * qw, dh), (d, f), (d, f), (f // 2, d), None, (b, d), (O_SLOTS, b, qw),
        (2, b, d), (2, hb, d), *[(SLOTS, 2, hw, d)] * 3,
    ]
    scratch = [pltpu.VMEM(a.shape, a.dtype) for a in (pos, inv, g1, g2)]
    scratch += [pltpu.VMEM((2, d), F32) if shape is None else pltpu.VMEM(shape, BF) for shape in bufs]
    two, four, ring, per = (2,), (SLOTS, 2), (2, nb), (nb,)
    sems = [(4,), (3,), (4,), (), two,
            (3,), (2, 2), (2, 2), two, two, (2, 2), (2, 2),
            (O_SLOTS,), (), ring, ring, per, two, (),
            two, two, two, (), two, (SLOTS,), four, four, two, four,
            (SLOTS,), (2, SLOTS), (2, SLOTS), (LATE,), two, ()]
    scratch += [pltpu.SemaphoreType.DMA(shape) for shape in sems]
    flops = 2 * t * (d * (qw + 2 * HEAD) + qw * t + tp * qw * dh + 3 * d * f)
    split = nb - Y_VMEM * nb // 16
    outs = [(split * b, d), None, (t, HEAD), (t, HEAD), (t, tp * qw)]
    vm = _held((nb - split) * b, d)
    return pl.pallas_call(
        functools.partial(_kernel, tp, dp, zn, split, l1, l2, nb // 4, nb // 2, nb * 3 // 4),
        name="layer",
        out_shape=tuple(jax.ShapeDtypeStruct(shape, BF) if shape else vm for shape in outs),
        in_specs=[hbm] * 12,
        out_specs=tuple(hbm if shape else pl.BlockSpec(memory_space=pltpu.VMEM) for shape in outs),
        scratch_shapes=scratch,
        compiler_params=pltpu.CompilerParams(collective_id=0, has_side_effects=True,
                                             vmem_limit_bytes=VMEM_BYTES - 2 * (nb - split) * b * d),
        cost_estimate=pl.CostEstimate(flops=flops, bytes_accessed=8 * t * d, transcendentals=t * t * hl),
    )(x, pos, inv, g1, g2, wq, wk, wv, wo, wg, wu, wd)


def _copy_kernel(src, held, k_src, v_src, dst, k_dst, v_dst, buf, kv, rd, wr, kv_sem):
    rows = buf.shape[1]
    steps = src.shape[0] // rows
    small = ((k_src, k_dst), (v_src, v_dst))
    reads, writes, late = [], [], []
    for i in range(steps):
        part = pl.ds(i * rows, rows)
        reads.append(pltpu.make_async_copy(src.at[part], buf.at[i], rd.at[i]))
        writes.append(pltpu.make_async_copy(buf.at[i], dst.at[part], rd.at[i]))
    for e, (a, z) in enumerate(small):
        reads.append(pltpu.make_async_copy(a, kv.at[e], kv_sem.at[e]))
        writes.append(pltpu.make_async_copy(kv.at[e], z, kv_sem.at[e]))
    for i in range(held.shape[0] // rows):
        to = pl.ds(src.shape[0] + i * rows, rows)
        late.append(pltpu.make_async_copy(held.at[pl.ds(i * rows, rows)], dst.at[to], wr.at[i]))
    for copy in reads:
        copy.start()
    for copy in late:
        copy.start()
    for read, write in zip(reads, writes):
        read.wait()
        write.start()
    for copy in (*late, *writes):
        copy.wait()


def _copy(y, held, k, v):
    d = y.shape[1]
    t = y.shape[0] + held.shape[0]
    rows = 256
    hbm = pl.BlockSpec(memory_space=pltpu.HBM)
    dma = pltpu.SemaphoreType.DMA
    n = y.shape[0] // rows
    shapes = ((t, d), k.shape, v.shape)
    return pl.pallas_call(
        _copy_kernel,
        name="copy_out",
        out_shape=tuple(jax.ShapeDtypeStruct(shape, BF) for shape in shapes),
        in_specs=[hbm, pl.BlockSpec(memory_space=pltpu.VMEM), hbm, hbm],
        out_specs=(hbm,) * 3,
        scratch_shapes=[pltpu.VMEM((n, rows, d), BF), pltpu.VMEM((2,) + k.shape, BF),
                        dma((n,)), dma((held.shape[0] // rows,)), dma((2,))],
        compiler_params=pltpu.CompilerParams(vmem_limit_bytes=VMEM_BYTES - 3 * held.size),
        cost_estimate=pl.CostEstimate(flops=0, bytes_accessed=4 * t * d, transcendentals=0),
    )(y, held, k, v)


def _row_length(mesh):
    at = [getattr(dev, "coords", None) for dev in mesh.devices.reshape(mesh.shape["dp"], -1)[:, 0]]
    if any(p is None for p in at):
        return None
    n = len(at)

    def apart(i, j):
        return sum(abs(p - q) for p, q in zip(at[i], at[j]))

    length = next((i for i in range(1, n) if at[i][-1] == at[0][-1]), n)
    if length % 2 or n % (2 * length):
        return None
    rows = all(apart(i, i + 1) == 1 for i in range(0, n, 2))
    across = all(apart(i, i + length) == 1 for i in range(n) if (i // length) % 2 == 0)
    return length if rows and across else None


def solution(mesh):
    tp = mesh.shape["tp"]
    dp = mesh.shape["dp"]
    zn = _row_length(mesh)

    def local(x, pos, g1, g2, wq, wk, wv, wo, wg, wu, wd):
        t = x.shape[0]
        half = ROPE_BASE ** (-2.0 * np.arange(HEAD // 2) / HEAD)
        inv = jnp.asarray(np.concatenate([half, half])[None, :].astype(np.float32))
        y, held, k, v, _ = _layer(tp, dp, zn, x, pos.reshape(t // LANES, LANES), inv, g1, g2, wq, wk, wv, wo, wg, wu, wd)
        y, k, v = (_keep(a, pltpu.HBM) for a in (y, k, v))
        y, k, v = _copy(y, _keep(held, pltpu.VMEM), k, v)
        return y, k.reshape(t, 1, HEAD), v.reshape(t, 1, HEAD)

    return jax.shard_map(
        local,
        mesh=mesh,
        in_specs=(P("dp", None), P("dp"), P(), P(), P(None, "tp"), P(), P(), P("tp", None),
                  P(None, "tp"), P(None, "tp"), P("tp", None)),
        out_specs=(P("dp", None), P("dp", "tp", None), P("dp", "tp", None)),
        check_vma=False,
    )
```

```python
import functools

import jax
import jax.numpy as jnp
import numpy as np
from jax import lax
from jax.experimental import pallas as pl
from jax.experimental.pallas import tpu as pltpu
from jax.sharding import PartitionSpec as P

HEAD = 128
LANES = 128
SUB = 16
EPS = 1e-5
ROPE_BASE = 500000.0
MESH = pl.DeviceIdType.MESH
BLOCK = 256
NR = 64
SLOTS = 4
LATE = 8
CHIP = 3
O_SLOTS = 6
SIDES = (0, 1)
BF = jnp.bfloat16
F32 = jnp.float32
VMEM_BYTES = 67040000
Y_VMEM = 15
TWO_OVER_PI = 0.6366197723675814
PI_2 = (1.5703125, 4.837512969970703125e-4, 7.54978995489188216e-8)
SIN = (-1.9515295891e-4, 8.3321608736e-3, -1.6666654611e-1)
COS = (2.443315711809948e-5, -1.388731625493765e-3, 4.166664568298827e-2)
LOG2E = 1.4426950408889634


def _sincos(ang):
    n = jnp.floor(ang * TWO_OVER_PI + 0.5)
    r = ang
    for p in PI_2:
        r = r - n * p
    z = r * r
    s = functools.reduce(lambda a, p: a * z + p, SIN[1:], SIN[0]) * z * r + r
    c = functools.reduce(lambda a, p: a * z + p, COS[1:], COS[0]) * z * z - 0.5 * z + 1.0
    m = n.astype(jnp.int32)
    odd = (m & 1) == 1
    cs = jnp.where(odd, s, c)
    sn = jnp.where(odd, c, s)
    return jnp.where(((m + 1) & 2) == 2, -cs, cs), jnp.where((m & 2) == 2, -sn, sn)


def _al(v, m):
    return pl.multiple_of(v, m)


def _first(ref, n):
    return ref.at[pl.ds(0, n)]


def _kernel(tp, dp, zn, split, l1, l2, w2, w3, w4,
            x_ref, pos_ref, inv_ref, g1_ref, g2_ref, wq_ref, wk_ref, wv_ref, wo_ref, wg_ref, wu_ref, wd_ref,
            y_ref, y_vm, k_ref, v_ref, oall_ref,
            pos_v, inv_v, g1_v, g2_v, wo_v, wg_v, wu_v, wd_v, g_scr, a_buf, o_buf,
            hbuf, rsib, rs_far, rs_near, rs_sum,
            ld_s, ld_w, ld_mlp, ld_x, kv_s,
            wo_d, wo_s, wo_r, wo_fs, wo_fr, wo_ps, wo_pr,
            o_s, o_loc, o_r, o_f, o_rs, o_rel, o_fwd,
            ld_o, h_s, h_r, r_s, r_r, part_s, far_r, near_r, sum_s, sum_r,
            y_s, y_r, y_f, y_rs, y_rel, y_fwd):
    t, d = x_ref.shape
    qw = wq_ref.shape[1]
    f = wg_ref.shape[1]
    hl = qw // HEAD
    b = BLOCK
    nb = t // b
    dh = d // 2
    hb = b // 2
    fh = f // 2
    nc = tp // 2
    ow = hb // nc
    hw = ow // 2
    kvt = 2 * b

    last_y = (nb - split) * b
    wd_late = y_vm.at[pl.ds(last_y - fh, fh)]
    x_buf = o_blk = y_vm.at[pl.ds(last_y - 4 * b, b)]
    xh = y_vm.at[pl.ds(last_y - 3 * b, b), pl.ds(0, dh)]
    wqkv = wg_v.at[:, pl.ds(0, qw + 2 * HEAD)]

    r = lax.axis_index("tp")
    c = r // 2
    s = r % 2
    c_r = (c + 1) % nc
    c_l = (c + nc - 1) % nc
    c_o = (c + 2) % nc
    dest = ({"tp": c_r * 2 + s}, {"tp": c_l * 2 + s})
    origin = (c_l, c_r)
    target = (c_r, c_l)
    sib = {"tp": c * 2 + 1 - s}
    dpi = lax.axis_index("dp")
    par = dpi % 2
    peers = [{"dp": dpi + 1 - 2 * par}] if dp % 2 == 0 else []
    if zn:
        par_y = (dpi // zn) % 2
        peers.append({"dp": dpi + zn * (1 - 2 * par_y)})

    def send(src, dst, ss, rs, dev):
        pltpu.make_async_remote_copy(
            src_ref=src, dst_ref=dst, send_sem=ss, recv_sem=rs, device_id=dev, device_id_type=MESH).start()

    def put(src, dst, sem):
        pltpu.make_async_copy(src, dst, sem).start()

    def wait(region, sem, tag=None):
        with jax.named_scope("w_" + (tag or "end")):
            pltpu.make_async_copy(region, region, sem).wait()

    def when_block(j, body):
        @pl.when((j >= 0) & (j < nb))
        def _():
            body()

    barrier = pltpu.get_barrier_semaphore()
    cross = [{"tp": target[e] * 2 + 1 - s} for e in SIDES]
    others = [*dest, *cross, sib, *peers]
    for dev in others:
        pl.semaphore_signal(barrier, inc=1, device_id=dev, device_id_type=MESH)

    small = ((pos_ref, pos_v), (inv_ref, inv_v), (g1_ref, g1_v), (g2_ref, g2_v))
    rk = _al(r * HEAD, HEAD)
    wq_dst = wqkv.at[:, pl.ds(0, qw)]
    kv_dst = [wqkv.at[:, pl.ds(qw + e * HEAD, HEAD)] for e in SIDES]
    put(_first(x_ref, b), x_buf, ld_x)
    for e, (src, dst) in enumerate(small):
        put(src, dst, ld_s.at[e])
    put(wq_ref, wq_dst, ld_w.at[2])
    for e, ref in enumerate((wk_ref, wv_ref)):
        put(ref.at[:, pl.ds(rk, HEAD)], kv_dst[e], ld_w.at[e])

    def norm_rows(src, which):
        def step(e, carry):
            for q in range(NR // SUB):
                rows = pl.ds(_al(e * NR + q * SUB, SUB), SUB)
                v32 = src[rows, :].astype(F32)
                inv = lax.rsqrt(jnp.mean(v32 * v32, axis=1, keepdims=True) + EPS)
                a_buf[rows, :] = (v32 * inv * g_scr[which:which + 1, :]).astype(BF)
            return carry

        with jax.named_scope("norm"):
            lax.fori_loop(0, b // NR, step, 0)

    for e, (src, dst) in enumerate(small):
        wait(dst, ld_s.at[e], "small")
    for e, ref in enumerate((g1_v, g2_v)):
        g_scr[e:e + 1, :] = ref[...].astype(F32).reshape(1, d)

    def x_norm(i):
        wait(x_buf, ld_x, "x")
        norm_rows(x_buf, 0)

        @pl.when(i + 1 < nb)
        def _():
            put(x_ref.at[pl.ds(_al((i + 1) * b, b), b)], x_buf, ld_x)

    x_norm(0)
    with jax.named_scope("barrier"):
        pl.semaphore_wait(barrier, len(others))

    mine = _al(s * dh, LANES)
    other = _al((1 - s) * dh, LANES)
    parts = 4 if zn else len(peers) + 1
    wr = qw // parts
    part = (2 * par_y + par) if zn else (par if peers else 0)

    def shard(dev):
        return wo_v.at[pl.ds(_al(dev * qw, LANES), qw)]

    def piece(chip, core, q=None):
        return wo_v.at[pl.ds(_al((chip * 2 + core) * qw + (part if q is None else q) * wr, 32), wr)]

    rows = pl.ds(_al(part * wr, 32), wr)
    for e in SIDES:
        for k, (cols, dev) in enumerate(((mine, dest[e]), (other, cross[e]))):
            send(wo_ref.at[rows, pl.ds(cols, dh)], piece(c, s), wo_s.at[e, k], wo_r.at[e, s], dev)
    send(wo_ref.at[:, pl.ds(other, dh)], shard(r), wo_d.at[0], wo_d.at[1], sib)
    put(wo_ref.at[:, pl.ds(mine, dh)], shard(r), wo_d.at[2])

    def wo_swap(chip):
        for e, dev in enumerate(peers):
            for core in SIDES:
                send(piece(chip, core), piece(chip, core), wo_ps.at[0, e], wo_pr.at[0, e], dev)

    def wo_stage2():
        for e in SIDES:
            for core in SIDES:
                wait(piece(origin[e], core), wo_r.at[e, core], "wo2")
            reg = piece(origin[e], e)
            send(reg, reg, wo_fs.at[e], wo_fr.at[e], dest[e])
            wo_swap(origin[e])

    def wo_stage3():
        for e in SIDES:
            wait(piece(c_o, e), wo_fr.at[e], "wo3")
        wo_swap(c_o)

    def wo_stage4():
        for e in range(len(peers)):
            wait(_first(wo_v, 6 * wr), wo_pr.at[0, e], "wo4")
        if zn:
            for chip in (*origin, c_o):
                for e, q in enumerate((2 * (1 - par_y) + par, 2 * par_y + 1 - par)):
                    reg = piece(chip, e, q)
                    send(reg, reg, wo_ps.at[1, e], wo_pr.at[1, e], peers[e])

    def wo_end(which):
        for e in SIDES if zn else ():
            wait(_first(wo_v, 3 * wr), which.at[1, e], "wo5")

    def ocol(chip, core):
        return pl.ds(_al((chip * 2 + core) * qw, LANES), qw)

    def oreg(j, chip):
        return oall_ref.at[pl.ds(_al(j * b, b), b), ocol(chip, s)]

    def ohalf(j, chip, half):
        return oall_ref.at[pl.ds(_al(j * b + half * hb, hb), hb), ocol(chip, s)]

    def orow(j):
        return pl.ds(_al(j * b, b), b)

    def o_stage2(j):
        def body():
            for e in SIDES:
                reg = oreg(j, origin[e])
                wait(reg, o_r.at[e, j], "o2")
                half = ohalf(j, origin[e], e)
                send(half, half, o_rel.at[e], o_f.at[e, j], dest[e])
                send(reg, reg, o_fwd, o_rs.at[j], sib)

        when_block(j, body)

    def o_stage3(j):
        def body():
            for e in SIDES:
                wait(ohalf(j, c_o, e), o_f.at[e, j], "o3")
            send(oreg(j, c_o), oreg(j, c_o), o_fwd, o_rs.at[j], sib)

        when_block(j, body)

    def unrolled(n, body):
        for e in range(n):
            body(e)

    def attention(q_scr, k_scr, v_scr, m_scr, l_scr, acc_scr):
        caches = ((k_scr, k_ref), (v_scr, v_ref))
        mlp = ((wu_ref, wu_v), (_first(wd_ref, fh), wd_v), (wd_ref.at[pl.ds(fh, fh)], wd_late))
        scale = HEAD ** -0.5 * LOG2E
        lane = lax.broadcasted_iota(jnp.int32, (b, HEAD), 1)

        def heads(ref, h):
            return ref.at[pl.ds(h * b, b)]

        def o_sent(slot):
            wait(oall_ref.at[pl.ds(0, 3 * b), pl.ds(0, qw)], o_s.at[slot], "osent")

        def tile(first, n, masked=False):
            keys = pl.ds(_al(first, n), n)
            kk = k_scr[keys, :]
            vv = v_scr[keys, :]
            sc = lax.dot_general(q_scr[...], kk, (((1,), (1,)), ((), ())), preferred_element_type=F32)
            if masked:
                keep = lax.broadcasted_iota(jnp.int32, (b, n), 1) <= lax.broadcasted_iota(jnp.int32, (b, n), 0)
                sc = jnp.concatenate([jnp.where(keep, sc[h * b:(h + 1) * b], -jnp.inf) for h in range(hl)], axis=0)
            m_prev = m_scr[...]
            m_new = jnp.maximum(m_prev, jnp.max(sc, axis=1, keepdims=True))
            ps = [jnp.exp2((sc[:, e * HEAD:(e + 1) * HEAD] - m_new) * scale) for e in range(n // HEAD)]
            alpha = jnp.exp2((m_prev - m_new) * scale)
            l_scr[...] = l_scr[...] * alpha + functools.reduce(lambda p, q: p + q, ps)
            pr = jnp.concatenate([p.astype(BF) for p in ps], axis=1)
            acc_scr[...] = acc_scr[...] * alpha + jnp.dot(pr, vv, preferred_element_type=F32)
            m_scr[...] = m_new

        def phase1(i, carry):
            with jax.named_scope("slot1"):
                phase1_slot(i)
            return carry

        def phase1_slot(i):
            slot = i % O_SLOTS

            @pl.when(i >= O_SLOTS)
            def _():
                o_sent(slot)

            @pl.when(i > 0)
            def _():
                wait(o_buf.at[0], o_loc, "oloc")

            @pl.when(i == 0)
            def _():
                wait(wq_dst, ld_w.at[2], "w")
                for e in SIDES:
                    wait(kv_dst[e], ld_w.at[e], "w")

            for e, (src, dst) in enumerate(mlp):
                @pl.when(i == min(w2 + e, nb - 1))
                def _(src=src, dst=dst, e=e):
                    put(src, dst, ld_mlp.at[e])

            pcol = []
            for e in range(b // LANES):
                prow = pos_v[pl.ds(i * (b // LANES) + e, 1), :].astype(F32)
                pcol.append(jnp.transpose(jnp.broadcast_to(prow, (LANES, LANES))))
            co, si = _sincos(jnp.concatenate(pcol, axis=0) * inv_v[...])
            si = jnp.where(lane < HEAD // 2, -si, si)
            qk32 = jnp.dot(a_buf[...], wg_v[:, :qw + HEAD], preferred_element_type=F32)
            v32 = jnp.dot(a_buf[...], wg_v[:, qw + HEAD:qw + 2 * HEAD], preferred_element_type=F32)
            rows = pl.ds(_al(i * b, b), b)
            for h in range(hl + 1):
                head = qk32[:, h * HEAD:(h + 1) * HEAD]
                head = (head * co + pltpu.roll(head, HEAD // 2, 1) * si).astype(BF)
                if h < hl:
                    heads(q_scr, h)[...] = head
                else:
                    k_scr[rows, :] = head
            v_scr[rows, :] = v32.astype(BF)
            for e, (src, dst) in enumerate(caches):
                @pl.when(i > 0)
                def _(src=src, e=e):
                    wait(_first(src, b), kv_s.at[e])

                put(src.at[rows], dst.at[rows], kv_s.at[e])
            m_scr[...] = jnp.full(m_scr.shape, -jnp.inf, F32)
            l_scr[...] = jnp.zeros(l_scr.shape, F32)
            acc_scr[...] = jnp.zeros(acc_scr.shape, F32)
            full = i // 2

            def inner(j, carry):
                for e in SIDES:
                    tile((2 * j + e) * kvt, kvt)
                return carry

            with jax.named_scope("tiles"):
                lax.fori_loop(0, full // 2, inner, 0)

            @pl.when(full % 2 == 1)
            def _():
                tile((full - 1) * kvt, kvt)

            @pl.when(i % 2 == 1)
            def _():
                tile((i - 1) * b, b)

            tile(i * b, b, masked=True)
            for h in range(hl):
                o_buf[slot, :, h * HEAD:(h + 1) * HEAD] = (
                    heads(acc_scr, h)[...] / jnp.sum(heads(l_scr, h)[...], axis=1, keepdims=True)).astype(BF)
            src = o_buf.at[slot]
            dst = oreg(i, c)
            for e in SIDES:
                send(src, dst, o_s.at[slot], o_r.at[e, i], dest[e])
            send(src, dst, o_s.at[slot], o_rs.at[i], sib)
            put(src, dst, o_loc)
            for when, stage in ((w2, wo_stage2), (w3, wo_stage3), (w4, wo_stage4)):
                pl.when(i == when)(stage)
            o_stage2(i - l1)
            o_stage3(i - l2)

            @pl.when(i + 1 < nb)
            def _():
                x_norm(i + 1)

        lax.fori_loop(0, nb, phase1, 0)
        for e, (src, _) in enumerate(caches):
            wait(_first(src, b), kv_s.at[e])

    loc = pltpu.VMEM
    pl.run_scoped(
        attention, loc((hl * b, HEAD), BF), loc((t, HEAD), BF),
        loc((t, HEAD), BF), *[loc((hl * b, HEAD), F32)] * 3)
    wait(o_buf.at[0], o_loc)
    wait(shard(r + 1 - 2 * s), wo_d.at[1])
    wait(shard(r), wo_d.at[2])
    wo_end(wo_pr)

    def rest(u_buf, r_buf, cp, sums, ych, hst):
        def load_o(j):
            wait(oall_ref.at[orow(j), pl.ds(0, 4 * qw)], o_rs.at[j], "os")
            put(oall_ref.at[orow(j)], o_blk, ld_o.at[0])
            put(x_ref.at[orow(j), pl.ds(mine, dh)], xh, ld_o.at[1])

        nt_h = min(512, dh)
        nt_f = min(512, f)
        nt_d = min(512, d)

        def cpart(j, chip, half):
            return cp.at[j % CHIP, pl.ds(_al(chip * ow + half * hw, hw), hw)]

        def sum_start(j):
            def body():
                two = j % 2
                q4 = j % SLOTS
                wait(rsib.at[two], r_r.at[two], "r")
                wait(rsib.at[two], r_s, "rs")

                def add(e, carry):
                    rows = pl.ds(_al(e * SUB, SUB), SUB)
                    own = r_buf[pl.ds(_al(s * hb + e * SUB, SUB), SUB), :]
                    cp[j % CHIP, rows, :] = (own.astype(F32) + rsib[two, rows, :].astype(F32)).astype(BF)
                    return carry

                with jax.named_scope("add"):
                    lax.fori_loop(0, hb // SUB, add, 0)
                for e in SIDES:
                    send(cpart(j, c_o, e), rs_far.at[q4, e], part_s.at[q4], far_r.at[q4, e], dest[e])
                for e in SIDES:
                    send(cpart(j, target[e], 1 - e), rs_near.at[q4, e], part_s.at[q4], near_r.at[q4, e], dest[e])

            when_block(j, body)

        def own_h(j):
            @pl.when(j < nb)
            def _():
                wait(o_blk, ld_o.at[0], "ldo")
                wait(xh, ld_o.at[1], "ldo")

                def col(n):
                    cols = pl.ds(n * nt_h, nt_h)
                    v32 = jnp.dot(o_blk[...], wo_v[:, cols], preferred_element_type=F32)
                    hbuf[j % 2, :, pl.ds(_al(s * dh + n * nt_h, LANES), nt_h)] = (xh[:, cols].astype(F32) + v32).astype(BF)

                with jax.named_scope("own_h"):
                    unrolled(dh // nt_h, col)

        def swap_h(j):
            @pl.when(j < nb)
            def _():
                half = hbuf.at[j % 2, :, pl.ds(mine, dh)]
                send(half, half, h_s.at[j % 2], h_r.at[j % 2], sib)

            @pl.when(j + 1 < nb)
            def _():
                load_o(j + 1)

        def mlp_norm(j):
            def body():
                two = j % 2
                wait(hbuf.at[two, :, pl.ds(other, dh)], h_r.at[two], "h")
                wait(hbuf.at[two, :, pl.ds(mine, dh)], h_s.at[two], "hs")

                @pl.when(j == 0)
                def _():
                    for e, dst in enumerate((wu_v, wd_v, wd_late, wg_v)):
                        wait(dst, ld_mlp.at[e], "mlp")

                norm_rows(hbuf.at[two], 1)
                hst[j % SLOTS] = hbuf[two, pl.ds(_al(s * hb + c * ow, SUB), ow), :]

            when_block(j, body)

        def mlp_up(j):
            def body():
                def col(n):
                    cols = pl.ds(n * nt_f, nt_f)
                    gt = jnp.dot(a_buf[...], wg_v[:, cols], preferred_element_type=F32)
                    up = jnp.dot(a_buf[...], wu_v[:, cols], preferred_element_type=F32)
                    u_buf[:, cols] = (gt * (1.0 / (1.0 + jnp.exp(-gt))) * up).astype(BF)

                with jax.named_scope("up"):
                    unrolled(f // nt_f, col)

            when_block(j, body)

        def mlp_down(j):
            def body():
                def col(n):
                    cols = pl.ds(n * nt_d, nt_d)
                    r32 = jnp.dot(u_buf[:, :fh], wd_v[:, cols], preferred_element_type=F32)
                    r32 = r32 + jnp.dot(u_buf[:, fh:], wd_late[:, cols], preferred_element_type=F32)
                    r_buf[:, cols] = r32.astype(BF)

                with jax.named_scope("down"):
                    unrolled(d // nt_d, col)
                send(r_buf.at[pl.ds(_al((1 - s) * hb, hb), hb)], rsib.at[j % 2], r_s, r_r.at[j % 2], sib)

            when_block(j, body)

        def sum_relay(j):
            def body():
                q4 = j % SLOTS
                two = j % 2

                @pl.when(j >= 2)
                def _():
                    wait(sums.at[two], sum_s.at[two], "sums")

                for e in SIDES:
                    wait(rs_far.at[q4, e], far_r.at[q4, e], "s1")
                    sums[two, e] = (rs_far[q4, e].astype(F32) + cpart(j, target[e], e)[...].astype(F32)).astype(BF)
                    send(sums.at[two, e], rs_sum.at[q4, e], sum_s.at[two], sum_r.at[q4, e], dest[e])

            when_block(j, body)

        def on_y(j, body):
            @pl.when((j >= 0) & (j < split))
            def _():
                body(y_ref, j * b, False)

            @pl.when((j >= split) & (j < nb))
            def _():
                body(y_vm, (j - split) * b, True)

        def yrow(ref, row, chip):
            return ref.at[pl.ds(_al(row + s * hb + chip * ow, ow), ow)]

        def yhalf(ref, row, chip, half):
            return ref.at[pl.ds(_al(row + s * hb + chip * ow + half * hw, hw), hw)]

        def y_sent(j, vmem):
            wait(cp.at[0, pl.ds(0, (3 if vmem else 4) * ow)], y_s.at[j % SLOTS], "ysent")

        def sum_end(j):
            @pl.when((j >= 2) & (j < split + 2))
            def _():
                y_sent(j - 2, False)

            @pl.when((j >= split + SLOTS) & (j < nb))
            def _():
                y_sent(j - SLOTS, True)

            def body(ref, row, vmem):
                q4 = j % SLOTS
                wait(cp.at[0, pl.ds(0, 4 * hw)], part_s.at[q4], "s1s")
                for e in SIDES:
                    wait(rs_near.at[q4, e], near_r.at[q4, e], "s2")
                    wait(rs_sum.at[q4, e], sum_r.at[q4, e], "s2")
                own = yrow(ref, row, c)
                src = own if vmem else ych.at[j % 2]
                for e in SIDES:
                    rows = pl.ds(e * hw, hw)
                    tot = cpart(j, c, e)[...].astype(F32) + rs_near[q4, 1 - e].astype(F32) + rs_sum[q4, e].astype(F32)
                    dst = yhalf(ref, row, c, e) if vmem else src.at[rows]
                    dst[...] = (hst[q4, rows, :].astype(F32) + tot).astype(BF)
                for e in SIDES:
                    send(src, own, y_s.at[q4], y_r.at[e, q4], dest[e])
                send(src, own, y_s.at[q4], y_rs.at[j % LATE], sib)
                if not vmem:
                    put(src, own, y_s.at[q4])

            on_y(j, body)

        def y_stage2(j):
            def body(ref, row, vmem):
                for e in SIDES:
                    reg = yrow(ref, row, origin[e])
                    wait(reg, y_r.at[e, j % SLOTS], "y2")
                    half = yhalf(ref, row, origin[e], e)
                    send(half, half, y_rel.at[e], y_f.at[e, j % SLOTS], dest[e])
                    send(reg, reg, y_fwd, y_rs.at[j % LATE], sib)

            on_y(j, body)

        def y_stage3(j):
            def body(ref, row, vmem):
                for e in SIDES:
                    wait(yhalf(ref, row, c_o, e), y_f.at[e, j % SLOTS], "y3")
                reg = yrow(ref, row, c_o)
                send(reg, reg, y_fwd, y_rs.at[j % LATE], sib)

            on_y(j, body)

        def y_seen(j):
            when_block(j, lambda: wait(cp.at[0], y_rs.at[j % LATE], "ys"))

        load_o(0)
        put(wg_ref, wg_v, ld_mlp.at[3])

        def phase2(i, carry):
            with jax.named_scope("slot2"):
                own_h(i)
                sum_start(i - 2)
                swap_h(i)
                mlp_norm(i - 1)
                sum_relay(i - 3)
                mlp_up(i - 1)
                sum_end(i - 4)
                mlp_down(i - 1)
                y_stage2(i - 5)
                y_stage3(i - 6)
                y_seen(i - LATE)
                o_stage2(nb + i - l1)
                o_stage3(nb + i - l2)
            return carry

        lax.fori_loop(0, nb + 6, phase2, 0)

        for j in range(nb + 6 - LATE, nb):
            wait(cp.at[0], y_rs.at[j % LATE])
        for j in range(max(nb - SLOTS, split), nb):
            y_sent(j, True)
        for e in SIDES:
            wait(sums.at[e], sum_s.at[e])
        for e in SIDES:
            wait(_first(y_vm, nb * hw), y_rel.at[e])
            wait(oall_ref.at[pl.ds(0, t // 2), pl.ds(0, qw)], o_rel.at[e])
            wait(_first(wo_v, wr), wo_fs.at[e])
            for k in SIDES:
                wait(_first(wo_v, wr), wo_s.at[e, k])
        wait(_first(y_vm, nb * ow * 3), y_fwd)
        for e in range(O_SLOTS):
            wait(oall_ref.at[pl.ds(0, 3 * b), pl.ds(0, qw)], o_s.at[e])
        wait(oall_ref.at[:, pl.ds(0, 3 * qw)], o_fwd)
        wait(_first(wo_v, qw), wo_d.at[0])
        for e in range(len(peers)):
            wait(_first(wo_v, 6 * wr), wo_ps.at[0, e])
        wo_end(wo_ps)

    pl.run_scoped(
        rest, loc((b, f), BF), loc((b, d), BF), loc((CHIP, hb, d), BF),
        loc((2, 2, hw, d), BF), loc((2, ow, d), BF), loc((SLOTS, ow, d), BF))


def _held(rows, d):
    return pltpu.VMEM((rows, d), BF)


def _keep(a, space):
    return pltpu.with_memory_space_constraint(a, space)


def _layer(tp, dp, zn, x, pos, inv, g1, g2, wq, wk, wv, wo, wg, wu, wd):
    t, d = x.shape
    qw = wq.shape[1]
    f = wg.shape[1]
    hl = qw // HEAD
    b = BLOCK
    nb = t // b
    hb = b // 2
    nc = tp // 2
    ow = hb // nc
    hw = ow // 2
    dh = d // 2
    assert nc == SLOTS and f <= 4 * b and nb > SLOTS and tp * qw == d and t % b == 0 and wk.shape[1] == tp * HEAD
    l1 = max(nb // 4, 1)
    l2 = min(nb * 3 // 4, nb - 2)
    hbm = pl.BlockSpec(memory_space=pl.ANY)
    bufs = [
        (tp * qw, dh), (d, f), (d, f), (f // 2, d), None, (b, d), (O_SLOTS, b, qw),
        (2, b, d), (2, hb, d), *[(SLOTS, 2, hw, d)] * 3,
    ]
    scratch = [pltpu.VMEM(a.shape, a.dtype) for a in (pos, inv, g1, g2)]
    scratch += [pltpu.VMEM((2, d), F32) if shape is None else pltpu.VMEM(shape, BF) for shape in bufs]
    two, four, ring, per = (2,), (SLOTS, 2), (2, nb), (nb,)
    sems = [(4,), (3,), (4,), (), two,
            (3,), (2, 2), (2, 2), two, two, (2, 2), (2, 2),
            (O_SLOTS,), (), ring, ring, per, two, (),
            two, two, two, (), two, (SLOTS,), four, four, two, four,
            (SLOTS,), (2, SLOTS), (2, SLOTS), (LATE,), two, ()]
    scratch += [pltpu.SemaphoreType.DMA(shape) for shape in sems]
    flops = 2 * t * (d * (qw + 2 * HEAD) + qw * t + tp * qw * dh + 3 * d * f)
    split = nb - Y_VMEM * nb // 16
    outs = [(split * b, d), None, (t, HEAD), (t, HEAD), (t, tp * qw)]
    vm = _held((nb - split) * b, d)
    return pl.pallas_call(
        functools.partial(_kernel, tp, dp, zn, split, l1, l2, nb // 4, nb // 2, nb * 3 // 4),
        name="layer",
        out_shape=tuple(jax.ShapeDtypeStruct(shape, BF) if shape else vm for shape in outs),
        in_specs=[hbm] * 12,
        out_specs=tuple(hbm if shape else pl.BlockSpec(memory_space=pltpu.VMEM) for shape in outs),
        scratch_shapes=scratch,
        compiler_params=pltpu.CompilerParams(collective_id=0, has_side_effects=True,
                                             vmem_limit_bytes=VMEM_BYTES - 2 * (nb - split) * b * d),
        cost_estimate=pl.CostEstimate(flops=flops, bytes_accessed=8 * t * d, transcendentals=t * t * hl),
    )(x, pos, inv, g1, g2, wq, wk, wv, wo, wg, wu, wd)


def _copy_kernel(src, held, k_src, v_src, dst, k_dst, v_dst, buf, kv, rd, wr, kv_sem):
    rows = buf.shape[1]
    steps = src.shape[0] // rows
    small = ((k_src, k_dst), (v_src, v_dst))
    reads, writes, late = [], [], []
    for i in range(steps):
        part = pl.ds(i * rows, rows)
        reads.append(pltpu.make_async_copy(src.at[part], buf.at[i], rd.at[i]))
        writes.append(pltpu.make_async_copy(buf.at[i], dst.at[part], rd.at[i]))
    for e, (a, z) in enumerate(small):
        reads.append(pltpu.make_async_copy(a, kv.at[e], kv_sem.at[e]))
        writes.append(pltpu.make_async_copy(kv.at[e], z, kv_sem.at[e]))
    for i in range(held.shape[0] // rows):
        to = pl.ds(src.shape[0] + i * rows, rows)
        late.append(pltpu.make_async_copy(held.at[pl.ds(i * rows, rows)], dst.at[to], wr.at[i]))
    for copy in reads:
        copy.start()
    for copy in late:
        copy.start()
    for read, write in zip(reads, writes):
        read.wait()
        write.start()
    for copy in (*late, *writes):
        copy.wait()


def _copy(y, held, k, v):
    d = y.shape[1]
    t = y.shape[0] + held.shape[0]
    rows = 256
    hbm = pl.BlockSpec(memory_space=pltpu.HBM)
    dma = pltpu.SemaphoreType.DMA
    n = y.shape[0] // rows
    shapes = ((t, d), k.shape, v.shape)
    return pl.pallas_call(
        _copy_kernel,
        name="copy_out",
        out_shape=tuple(jax.ShapeDtypeStruct(shape, BF) for shape in shapes),
        in_specs=[hbm, pl.BlockSpec(memory_space=pltpu.VMEM), hbm, hbm],
        out_specs=(hbm,) * 3,
        scratch_shapes=[pltpu.VMEM((n, rows, d), BF), pltpu.VMEM((2,) + k.shape, BF),
                        dma((n,)), dma((held.shape[0] // rows,)), dma((2,))],
        compiler_params=pltpu.CompilerParams(vmem_limit_bytes=VMEM_BYTES - 3 * held.size),
        cost_estimate=pl.CostEstimate(flops=0, bytes_accessed=4 * t * d, transcendentals=0),
    )(y, held, k, v)


def _row_length(mesh):
    at = [getattr(dev, "coords", None) for dev in mesh.devices.reshape(mesh.shape["dp"], -1)[:, 0]]
    if any(p is None for p in at):
        return None
    n = len(at)

    def apart(i, j):
        return sum(abs(p - q) for p, q in zip(at[i], at[j]))

    length = next((i for i in range(1, n) if at[i][-1] == at[0][-1]), n)
    if length % 2 or n % (2 * length):
        return None
    rows = all(apart(i, i + 1) == 1 for i in range(0, n, 2))
    across = all(apart(i, i + length) == 1 for i in range(n) if (i // length) % 2 == 0)
    return length if rows and across else None


def solution(mesh):
    tp = mesh.shape["tp"]
    dp = mesh.shape["dp"]
    zn = _row_length(mesh)

    def local(x, pos, g1, g2, wq, wk, wv, wo, wg, wu, wd):
        t = x.shape[0]
        half = ROPE_BASE ** (-2.0 * np.arange(HEAD // 2) / HEAD)
        inv = jnp.asarray(np.concatenate([half, half])[None, :].astype(np.float32))
        y, held, k, v, _ = _layer(tp, dp, zn, x, pos.reshape(t // LANES, LANES), inv, g1, g2, wq, wk, wv, wo, wg, wu, wd)
        y, k, v = (_keep(a, pltpu.HBM) for a in (y, k, v))
        y, k, v = _copy(y, _keep(held, pltpu.VMEM), k, v)
        return y, k.reshape(t, 1, HEAD), v.reshape(t, 1, HEAD)

    return jax.shard_map(
        local,
        mesh=mesh,
        in_specs=(P("dp", None), P("dp"), P(), P(), P(None, "tp"), P(), P(), P("tp", None),
                  P(None, "tp"), P(None, "tp"), P("tp", None)),
        out_specs=(P("dp", None), P("dp", "tp", None), P("dp", "tp", None)),
        check_vma=False,
    )
```

```python
import functools

import jax
import jax.numpy as jnp
import numpy as np
from jax import lax
from jax.experimental import pallas as pl
from jax.experimental.pallas import tpu as pltpu
from jax.sharding import PartitionSpec as P

HEAD = 128
LANES = 128
SUB = 16
EPS = 1e-5
ROPE_BASE = 500000.0
MESH = pl.DeviceIdType.MESH
BLOCK = 256
NR = 64
SLOTS = 4
LATE = 8
CHIP = 3
O_SLOTS = 6
SIDES = (0, 1)
BF = jnp.bfloat16
F32 = jnp.float32
VMEM_BYTES = 67040000
Y_VMEM = 15
TWO_OVER_PI = 0.6366197723675814
PI_2 = (1.5703125, 4.837512969970703125e-4, 7.54978995489188216e-8)
SIN = (-1.9515295891e-4, 8.3321608736e-3, -1.6666654611e-1)
COS = (2.443315711809948e-5, -1.388731625493765e-3, 4.166664568298827e-2)
LOG2E = 1.4426950408889634


def _sincos(ang):
    n = jnp.floor(ang * TWO_OVER_PI + 0.5)
    r = ang
    for p in PI_2:
        r = r - n * p
    z = r * r
    s = functools.reduce(lambda a, p: a * z + p, SIN[1:], SIN[0]) * z * r + r
    c = functools.reduce(lambda a, p: a * z + p, COS[1:], COS[0]) * z * z - 0.5 * z + 1.0
    m = n.astype(jnp.int32)
    odd = (m & 1) == 1
    cs = jnp.where(odd, s, c)
    sn = jnp.where(odd, c, s)
    return jnp.where(((m + 1) & 2) == 2, -cs, cs), jnp.where((m & 2) == 2, -sn, sn)


def _al(v, m):
    return pl.multiple_of(v, m)


def _first(ref, n):
    return ref.at[pl.ds(0, n)]


def _kernel(tp, dp, zn, split, l1, l2, w2, w3, w4,
            x_ref, pos_ref, inv_ref, g1_ref, g2_ref, wq_ref, wk_ref, wv_ref, wo_ref, wg_ref, wu_ref, wd_ref,
            y_ref, y_vm, k_ref, v_ref, oall_ref,
            pos_v, inv_v, g1_v, g2_v, wo_v, wg_v, wu_v, wd_v, g_scr, a_buf, o_buf,
            hbuf, rsib, rs_far, rs_near, rs_sum,
            ld_s, ld_w, ld_mlp, ld_x, kv_s,
            wo_d, wo_s, wo_r, wo_fs, wo_fr, wo_ps, wo_pr,
            o_s, o_loc, o_r, o_f, o_rs, o_rel, o_fwd,
            ld_o, h_s, h_r, r_s, r_r, part_s, far_r, near_r, sum_s, sum_r,
            y_s, y_r, y_f, y_rs, y_rel, y_fwd):
    t, d = x_ref.shape
    qw = wq_ref.shape[1]
    f = wg_ref.shape[1]
    hl = qw // HEAD
    b = BLOCK
    nb = t // b
    dh = d // 2
    hb = b // 2
    fh = f // 2
    nc = tp // 2
    ow = hb // nc
    hw = ow // 2
    kvt = 2 * b

    last_y = (nb - split) * b
    wd_late = y_vm.at[pl.ds(last_y - fh, fh)]
    x_buf = o_blk = y_vm.at[pl.ds(last_y - 4 * b, b)]
    xh = y_vm.at[pl.ds(last_y - 3 * b, b), pl.ds(0, dh)]
    wqkv = wg_v.at[:, pl.ds(0, qw + 2 * HEAD)]

    r = lax.axis_index("tp")
    c = r // 2
    s = r % 2
    c_r = (c + 1) % nc
    c_l = (c + nc - 1) % nc
    c_o = (c + 2) % nc
    dest = ({"tp": c_r * 2 + s}, {"tp": c_l * 2 + s})
    origin = (c_l, c_r)
    target = (c_r, c_l)
    sib = {"tp": c * 2 + 1 - s}
    dpi = lax.axis_index("dp")
    par = dpi % 2
    peers = [{"dp": dpi + 1 - 2 * par}] if dp % 2 == 0 else []
    if zn:
        par_y = (dpi // zn) % 2
        peers.append({"dp": dpi + zn * (1 - 2 * par_y)})

    def send(src, dst, ss, rs, dev):
        pltpu.make_async_remote_copy(
            src_ref=src, dst_ref=dst, send_sem=ss, recv_sem=rs, device_id=dev, device_id_type=MESH).start()

    def put(src, dst, sem):
        pltpu.make_async_copy(src, dst, sem).start()

    def wait(region, sem, tag=None):
        with jax.named_scope("w_" + (tag or "end")):
            pltpu.make_async_copy(region, region, sem).wait()

    def when_block(j, body):
        @pl.when((j >= 0) & (j < nb))
        def _():
            body()

    barrier = pltpu.get_barrier_semaphore()
    cross = [{"tp": target[e] * 2 + 1 - s} for e in SIDES]
    others = [*dest, *cross, sib, *peers]
    for dev in others:
        pl.semaphore_signal(barrier, inc=1, device_id=dev, device_id_type=MESH)

    small = ((pos_ref, pos_v), (inv_ref, inv_v), (g1_ref, g1_v), (g2_ref, g2_v))
    rk = _al(r * HEAD, HEAD)
    wq_dst = wqkv.at[:, pl.ds(0, qw)]
    kv_dst = [wqkv.at[:, pl.ds(qw + e * HEAD, HEAD)] for e in SIDES]
    put(_first(x_ref, b), x_buf, ld_x)
    for e, (src, dst) in enumerate(small):
        put(src, dst, ld_s.at[e])
    put(wq_ref, wq_dst, ld_w.at[2])
    for e, ref in enumerate((wk_ref, wv_ref)):
        put(ref.at[:, pl.ds(rk, HEAD)], kv_dst[e], ld_w.at[e])

    def norm_rows(src, which):
        def step(e, carry):
            for q in range(NR // SUB):
                rows = pl.ds(_al(e * NR + q * SUB, SUB), SUB)
                v32 = src[rows, :].astype(F32)
                inv = lax.rsqrt(jnp.mean(v32 * v32, axis=1, keepdims=True) + EPS)
                a_buf[rows, :] = (v32 * inv * g_scr[which:which + 1, :]).astype(BF)
            return carry

        with jax.named_scope("norm"):
            lax.fori_loop(0, b // NR, step, 0)

    for e, (src, dst) in enumerate(small):
        wait(dst, ld_s.at[e], "small")
    for e, ref in enumerate((g1_v, g2_v)):
        g_scr[e:e + 1, :] = ref[...].astype(F32).reshape(1, d)

    def x_norm(i):
        wait(x_buf, ld_x, "x")
        norm_rows(x_buf, 0)

        @pl.when(i + 1 < nb)
        def _():
            put(x_ref.at[pl.ds(_al((i + 1) * b, b), b)], x_buf, ld_x)

    x_norm(0)
    with jax.named_scope("barrier"):
        pl.semaphore_wait(barrier, len(others))

    mine = _al(s * dh, LANES)
    other = _al((1 - s) * dh, LANES)
    parts = 4 if zn else len(peers) + 1
    wr = qw // parts
    part = (2 * par_y + par) if zn else (par if peers else 0)

    def shard(dev):
        return wo_v.at[pl.ds(_al(dev * qw, LANES), qw)]

    def piece(chip, core, q=None):
        return wo_v.at[pl.ds(_al((chip * 2 + core) * qw + (part if q is None else q) * wr, 32), wr)]

    rows = pl.ds(_al(part * wr, 32), wr)
    for e in SIDES:
        for k, (cols, dev) in enumerate(((mine, dest[e]), (other, cross[e]))):
            send(wo_ref.at[rows, pl.ds(cols, dh)], piece(c, s), wo_s.at[e, k], wo_r.at[e, s], dev)
    send(wo_ref.at[:, pl.ds(other, dh)], shard(r), wo_d.at[0], wo_d.at[1], sib)
    put(wo_ref.at[:, pl.ds(mine, dh)], shard(r), wo_d.at[2])

    def wo_swap(chip):
        for e, dev in enumerate(peers):
            for core in SIDES:
                send(piece(chip, core), piece(chip, core), wo_ps.at[0, e], wo_pr.at[0, e], dev)

    def wo_stage2():
        for e in SIDES:
            for core in SIDES:
                wait(piece(origin[e], core), wo_r.at[e, core], "wo2")
            reg = piece(origin[e], e)
            send(reg, reg, wo_fs.at[e], wo_fr.at[e], dest[e])
            wo_swap(origin[e])

    def wo_stage3():
        for e in SIDES:
            wait(piece(c_o, e), wo_fr.at[e], "wo3")
        wo_swap(c_o)

    def wo_stage4():
        for e in range(len(peers)):
            wait(_first(wo_v, 6 * wr), wo_pr.at[0, e], "wo4")
        if zn:
            for chip in (*origin, c_o):
                for e, q in enumerate((2 * (1 - par_y) + par, 2 * par_y + 1 - par)):
                    reg = piece(chip, e, q)
                    send(reg, reg, wo_ps.at[1, e], wo_pr.at[1, e], peers[e])

    def wo_end(which):
        for e in SIDES if zn else ():
            wait(_first(wo_v, 3 * wr), which.at[1, e], "wo5")

    def ocol(chip, core):
        return pl.ds(_al((chip * 2 + core) * qw, LANES), qw)

    def oreg(j, chip):
        return oall_ref.at[pl.ds(_al(j * b, b), b), ocol(chip, s)]

    def ohalf(j, chip, half):
        return oall_ref.at[pl.ds(_al(j * b + half * hb, hb), hb), ocol(chip, s)]

    def orow(j):
        return pl.ds(_al(j * b, b), b)

    def o_stage2(j):
        def body():
            for e in SIDES:
                reg = oreg(j, origin[e])
                wait(reg, o_r.at[e, j], "o2")
                half = ohalf(j, origin[e], e)
                send(half, half, o_rel.at[e], o_f.at[e, j], dest[e])
                send(reg, reg, o_fwd, o_rs.at[j], sib)

        when_block(j, body)

    def o_stage3(j):
        def body():
            for e in SIDES:
                wait(ohalf(j, c_o, e), o_f.at[e, j], "o3")
            send(oreg(j, c_o), oreg(j, c_o), o_fwd, o_rs.at[j], sib)

        when_block(j, body)

    def unrolled(n, body):
        for e in range(n):
            body(e)

    def load_o(j):
        wait(oall_ref.at[orow(j), pl.ds(0, 4 * qw)], o_rs.at[j], "os")
        put(oall_ref.at[orow(j)], o_blk, ld_o.at[0])
        put(x_ref.at[orow(j), pl.ds(mine, dh)], xh, ld_o.at[1])

    def attention(q_scr, k_scr, v_scr, m_scr, l_scr, acc_scr):
        caches = ((k_scr, k_ref), (v_scr, v_ref))
        mlp = ((wu_ref, wu_v), (_first(wd_ref, fh), wd_v), (wd_ref.at[pl.ds(fh, fh)], wd_late))
        scale = HEAD ** -0.5 * LOG2E
        lane = lax.broadcasted_iota(jnp.int32, (b, HEAD), 1)

        def heads(ref, h):
            return ref.at[pl.ds(h * b, b)]

        def o_sent(slot):
            wait(oall_ref.at[pl.ds(0, 3 * b), pl.ds(0, qw)], o_s.at[slot], "osent")

        def tile(first, n, masked=False):
            keys = pl.ds(_al(first, n), n)
            kk = k_scr[keys, :]
            vv = v_scr[keys, :]
            sc = lax.dot_general(q_scr[...], kk, (((1,), (1,)), ((), ())), preferred_element_type=F32)
            if masked:
                keep = lax.broadcasted_iota(jnp.int32, (b, n), 1) <= lax.broadcasted_iota(jnp.int32, (b, n), 0)
                sc = jnp.concatenate([jnp.where(keep, sc[h * b:(h + 1) * b], -jnp.inf) for h in range(hl)], axis=0)
            m_prev = m_scr[...]
            m_new = jnp.maximum(m_prev, jnp.max(sc, axis=1, keepdims=True))
            ps = [jnp.exp2((sc[:, e * HEAD:(e + 1) * HEAD] - m_new) * scale) for e in range(n // HEAD)]
            alpha = jnp.exp2((m_prev - m_new) * scale)
            l_scr[...] = l_scr[...] * alpha + functools.reduce(lambda p, q: p + q, ps)
            pr = jnp.concatenate([p.astype(BF) for p in ps], axis=1)
            acc_scr[...] = acc_scr[...] * alpha + jnp.dot(pr, vv, preferred_element_type=F32)
            m_scr[...] = m_new

        def phase1(i, carry):
            with jax.named_scope("slot1"):
                phase1_slot(i)
            return carry

        def phase1_slot(i):
            slot = i % O_SLOTS

            @pl.when(i >= O_SLOTS)
            def _():
                o_sent(slot)

            @pl.when(i > 0)
            def _():
                wait(o_buf.at[0], o_loc, "oloc")

            @pl.when(i == nb - 1)
            def _():
                load_o(0)

            @pl.when(i == 0)
            def _():
                wait(wq_dst, ld_w.at[2], "w")
                for e in SIDES:
                    wait(kv_dst[e], ld_w.at[e], "w")

            for e, (src, dst) in enumerate(mlp):
                @pl.when(i == min(w2 + e, nb - 1))
                def _(src=src, dst=dst, e=e):
                    put(src, dst, ld_mlp.at[e])

            pcol = []
            for e in range(b // LANES):
                prow = pos_v[pl.ds(i * (b // LANES) + e, 1), :].astype(F32)
                pcol.append(jnp.transpose(jnp.broadcast_to(prow, (LANES, LANES))))
            co, si = _sincos(jnp.concatenate(pcol, axis=0) * inv_v[...])
            si = jnp.where(lane < HEAD // 2, -si, si)
            qk32 = jnp.dot(a_buf[...], wg_v[:, :qw + HEAD], preferred_element_type=F32)
            v32 = jnp.dot(a_buf[...], wg_v[:, qw + HEAD:qw + 2 * HEAD], preferred_element_type=F32)
            rows = pl.ds(_al(i * b, b), b)
            for h in range(hl + 1):
                head = qk32[:, h * HEAD:(h + 1) * HEAD]
                head = (head * co + pltpu.roll(head, HEAD // 2, 1) * si).astype(BF)
                if h < hl:
                    heads(q_scr, h)[...] = head
                else:
                    k_scr[rows, :] = head
            v_scr[rows, :] = v32.astype(BF)
            for e, (src, dst) in enumerate(caches):
                @pl.when(i > 0)
                def _(src=src, e=e):
                    wait(_first(src, b), kv_s.at[e])

                put(src.at[rows], dst.at[rows], kv_s.at[e])
            m_scr[...] = jnp.full(m_scr.shape, -jnp.inf, F32)
            l_scr[...] = jnp.zeros(l_scr.shape, F32)
            acc_scr[...] = jnp.zeros(acc_scr.shape, F32)
            full = i // 2

            def inner(j, carry):
                for e in SIDES:
                    tile((2 * j + e) * kvt, kvt)
                return carry

            with jax.named_scope("tiles"):
                lax.fori_loop(0, full // 2, inner, 0)

            @pl.when(full % 2 == 1)
            def _():
                tile((full - 1) * kvt, kvt)

            @pl.when(i % 2 == 1)
            def _():
                tile((i - 1) * b, b)

            tile(i * b, b, masked=True)
            for h in range(hl):
                o_buf[slot, :, h * HEAD:(h + 1) * HEAD] = (
                    heads(acc_scr, h)[...] / jnp.sum(heads(l_scr, h)[...], axis=1, keepdims=True)).astype(BF)
            src = o_buf.at[slot]
            dst = oreg(i, c)
            for e in SIDES:
                send(src, dst, o_s.at[slot], o_r.at[e, i], dest[e])
            send(src, dst, o_s.at[slot], o_rs.at[i], sib)
            put(src, dst, o_loc)
            for when, stage in ((w2, wo_stage2), (w3, wo_stage3), (w4, wo_stage4)):
                pl.when(i == when)(stage)
            o_stage2(i - l1)
            o_stage3(i - l2)

            @pl.when(i + 1 < nb)
            def _():
                x_norm(i + 1)

        lax.fori_loop(0, nb, phase1, 0)
        for e, (src, _) in enumerate(caches):
            wait(_first(src, b), kv_s.at[e])

    loc = pltpu.VMEM
    pl.run_scoped(
        attention, loc((hl * b, HEAD), BF), loc((t, HEAD), BF),
        loc((t, HEAD), BF), *[loc((hl * b, HEAD), F32)] * 3)
    wait(o_buf.at[0], o_loc)
    wait(shard(r + 1 - 2 * s), wo_d.at[1])
    wait(shard(r), wo_d.at[2])
    wo_end(wo_pr)

    def rest(u_buf, r_buf, cp, sums, ych, hst):
        nt_h = min(512, dh)
        nt_f = min(512, f)
        nt_d = min(512, d)

        def cpart(j, chip, half):
            return cp.at[j % CHIP, pl.ds(_al(chip * ow + half * hw, hw), hw)]

        def sum_start(j):
            def body():
                two = j % 2
                q4 = j % SLOTS
                wait(rsib.at[two], r_r.at[two], "r")
                wait(rsib.at[two], r_s, "rs")

                def add(e, carry):
                    rows = pl.ds(_al(e * SUB, SUB), SUB)
                    own = r_buf[pl.ds(_al(s * hb + e * SUB, SUB), SUB), :]
                    cp[j % CHIP, rows, :] = (own.astype(F32) + rsib[two, rows, :].astype(F32)).astype(BF)
                    return carry

                with jax.named_scope("add"):
                    lax.fori_loop(0, hb // SUB, add, 0)
                for e in SIDES:
                    send(cpart(j, c_o, e), rs_far.at[q4, e], part_s.at[q4], far_r.at[q4, e], dest[e])
                for e in SIDES:
                    send(cpart(j, target[e], 1 - e), rs_near.at[q4, e], part_s.at[q4], near_r.at[q4, e], dest[e])

            when_block(j, body)

        def own_h(j):
            @pl.when(j < nb)
            def _():
                wait(o_blk, ld_o.at[0], "ldo")
                wait(xh, ld_o.at[1], "ldo")

                def col(n):
                    cols = pl.ds(n * nt_h, nt_h)
                    v32 = jnp.dot(o_blk[...], wo_v[:, cols], preferred_element_type=F32)
                    hbuf[j % 2, :, pl.ds(_al(s * dh + n * nt_h, LANES), nt_h)] = (xh[:, cols].astype(F32) + v32).astype(BF)

                with jax.named_scope("own_h"):
                    unrolled(dh // nt_h, col)

        def swap_h(j):
            @pl.when(j < nb)
            def _():
                half = hbuf.at[j % 2, :, pl.ds(mine, dh)]
                send(half, half, h_s.at[j % 2], h_r.at[j % 2], sib)

            @pl.when(j + 1 < nb)
            def _():
                load_o(j + 1)

        def mlp_norm(j):
            def body():
                two = j % 2
                wait(hbuf.at[two, :, pl.ds(other, dh)], h_r.at[two], "h")
                wait(hbuf.at[two, :, pl.ds(mine, dh)], h_s.at[two], "hs")

                @pl.when(j == 0)
                def _():
                    for e, dst in enumerate((wu_v, wd_v, wd_late, wg_v)):
                        wait(dst, ld_mlp.at[e], "mlp")

                norm_rows(hbuf.at[two], 1)
                hst[j % SLOTS] = hbuf[two, pl.ds(_al(s * hb + c * ow, SUB), ow), :]

            when_block(j, body)

        def mlp_up(j):
            def body():
                def col(n):
                    cols = pl.ds(n * nt_f, nt_f)
                    gt = jnp.dot(a_buf[...], wg_v[:, cols], preferred_element_type=F32)
                    up = jnp.dot(a_buf[...], wu_v[:, cols], preferred_element_type=F32)
                    u_buf[:, cols] = (gt * (1.0 / (1.0 + jnp.exp(-gt))) * up).astype(BF)

                with jax.named_scope("up"):
                    unrolled(f // nt_f, col)

            when_block(j, body)

        def mlp_down(j):
            def body():
                def col(n):
                    cols = pl.ds(n * nt_d, nt_d)
                    r32 = jnp.dot(u_buf[:, :fh], wd_v[:, cols], preferred_element_type=F32)
                    r32 = r32 + jnp.dot(u_buf[:, fh:], wd_late[:, cols], preferred_element_type=F32)
                    r_buf[:, cols] = r32.astype(BF)

                with jax.named_scope("down"):
                    unrolled(d // nt_d, col)
                send(r_buf.at[pl.ds(_al((1 - s) * hb, hb), hb)], rsib.at[j % 2], r_s, r_r.at[j % 2], sib)

            when_block(j, body)

        def sum_relay(j):
            def body():
                q4 = j % SLOTS
                two = j % 2

                @pl.when(j >= 2)
                def _():
                    wait(sums.at[two], sum_s.at[two], "sums")

                for e in SIDES:
                    wait(rs_far.at[q4, e], far_r.at[q4, e], "s1")
                    sums[two, e] = (rs_far[q4, e].astype(F32) + cpart(j, target[e], e)[...].astype(F32)).astype(BF)
                    send(sums.at[two, e], rs_sum.at[q4, e], sum_s.at[two], sum_r.at[q4, e], dest[e])

            when_block(j, body)

        def on_y(j, body):
            @pl.when((j >= 0) & (j < split))
            def _():
                body(y_ref, j * b, False)

            @pl.when((j >= split) & (j < nb))
            def _():
                body(y_vm, (j - split) * b, True)

        def yrow(ref, row, chip):
            return ref.at[pl.ds(_al(row + s * hb + chip * ow, ow), ow)]

        def yhalf(ref, row, chip, half):
            return ref.at[pl.ds(_al(row + s * hb + chip * ow + half * hw, hw), hw)]

        def y_sent(j, vmem):
            wait(cp.at[0, pl.ds(0, (3 if vmem else 4) * ow)], y_s.at[j % SLOTS], "ysent")

        def sum_end(j):
            @pl.when((j >= 2) & (j < split + 2))
            def _():
                y_sent(j - 2, False)

            @pl.when((j >= split + SLOTS) & (j < nb))
            def _():
                y_sent(j - SLOTS, True)

            def body(ref, row, vmem):
                q4 = j % SLOTS
                wait(cp.at[0, pl.ds(0, 4 * hw)], part_s.at[q4], "s1s")
                for e in SIDES:
                    wait(rs_near.at[q4, e], near_r.at[q4, e], "s2")
                    wait(rs_sum.at[q4, e], sum_r.at[q4, e], "s2")
                own = yrow(ref, row, c)
                src = own if vmem else ych.at[j % 2]
                for e in SIDES:
                    rows = pl.ds(e * hw, hw)
                    tot = cpart(j, c, e)[...].astype(F32) + rs_near[q4, 1 - e].astype(F32) + rs_sum[q4, e].astype(F32)
                    dst = yhalf(ref, row, c, e) if vmem else src.at[rows]
                    dst[...] = (hst[q4, rows, :].astype(F32) + tot).astype(BF)
                for e in SIDES:
                    send(src, own, y_s.at[q4], y_r.at[e, q4], dest[e])
                send(src, own, y_s.at[q4], y_rs.at[j % LATE], sib)
                if not vmem:
                    put(src, own, y_s.at[q4])

            on_y(j, body)

        def y_stage2(j):
            def body(ref, row, vmem):
                for e in SIDES:
                    reg = yrow(ref, row, origin[e])
                    wait(reg, y_r.at[e, j % SLOTS], "y2")
                    half = yhalf(ref, row, origin[e], e)
                    send(half, half, y_rel.at[e], y_f.at[e, j % SLOTS], dest[e])
                    send(reg, reg, y_fwd, y_rs.at[j % LATE], sib)

            on_y(j, body)

        def y_stage3(j):
            def body(ref, row, vmem):
                for e in SIDES:
                    wait(yhalf(ref, row, c_o, e), y_f.at[e, j % SLOTS], "y3")
                reg = yrow(ref, row, c_o)
                send(reg, reg, y_fwd, y_rs.at[j % LATE], sib)

            on_y(j, body)

        def y_seen(j):
            when_block(j, lambda: wait(cp.at[0], y_rs.at[j % LATE], "ys"))

        put(wg_ref, wg_v, ld_mlp.at[3])

        def phase2(i, carry):
            with jax.named_scope("slot2"):
                own_h(i)
                sum_start(i - 2)
                swap_h(i)
                mlp_norm(i - 1)
                sum_relay(i - 3)
                mlp_up(i - 1)
                sum_end(i - 4)
                mlp_down(i - 1)
                y_stage2(i - 5)
                y_stage3(i - 6)
                y_seen(i - LATE)
                o_stage2(nb + i - l1)
                o_stage3(nb + i - l2)
            return carry

        lax.fori_loop(0, nb + 6, phase2, 0)

        for j in range(nb + 6 - LATE, nb):
            wait(cp.at[0], y_rs.at[j % LATE])
        for j in range(max(nb - SLOTS, split), nb):
            y_sent(j, True)
        for e in SIDES:
            wait(sums.at[e], sum_s.at[e])
        for e in SIDES:
            wait(_first(y_vm, nb * hw), y_rel.at[e])
            wait(oall_ref.at[pl.ds(0, t // 2), pl.ds(0, qw)], o_rel.at[e])
            wait(_first(wo_v, wr), wo_fs.at[e])
            for k in SIDES:
                wait(_first(wo_v, wr), wo_s.at[e, k])
        wait(_first(y_vm, nb * ow * 3), y_fwd)
        for e in range(O_SLOTS):
            wait(oall_ref.at[pl.ds(0, 3 * b), pl.ds(0, qw)], o_s.at[e])
        wait(oall_ref.at[:, pl.ds(0, 3 * qw)], o_fwd)
        wait(_first(wo_v, qw), wo_d.at[0])
        for e in range(len(peers)):
            wait(_first(wo_v, 6 * wr), wo_ps.at[0, e])
        wo_end(wo_ps)

    pl.run_scoped(
        rest, loc((b, f), BF), loc((b, d), BF), loc((CHIP, hb, d), BF),
        loc((2, 2, hw, d), BF), loc((2, ow, d), BF), loc((SLOTS, ow, d), BF))


def _held(rows, d):
    return pltpu.VMEM((rows, d), BF)


def _keep(a, space):
    return pltpu.with_memory_space_constraint(a, space)


def _layer(tp, dp, zn, x, pos, inv, g1, g2, wq, wk, wv, wo, wg, wu, wd):
    t, d = x.shape
    qw = wq.shape[1]
    f = wg.shape[1]
    hl = qw // HEAD
    b = BLOCK
    nb = t // b
    hb = b // 2
    nc = tp // 2
    ow = hb // nc
    hw = ow // 2
    dh = d // 2
    assert nc == SLOTS and f <= 4 * b and nb > SLOTS and tp * qw == d and t % b == 0 and wk.shape[1] == tp * HEAD
    l1 = max(nb // 4, 1)
    l2 = min(nb * 3 // 4, nb - 2)
    hbm = pl.BlockSpec(memory_space=pl.ANY)
    bufs = [
        (tp * qw, dh), (d, f), (d, f), (f // 2, d), None, (b, d), (O_SLOTS, b, qw),
        (2, b, d), (2, hb, d), *[(SLOTS, 2, hw, d)] * 3,
    ]
    scratch = [pltpu.VMEM(a.shape, a.dtype) for a in (pos, inv, g1, g2)]
    scratch += [pltpu.VMEM((2, d), F32) if shape is None else pltpu.VMEM(shape, BF) for shape in bufs]
    two, four, ring, per = (2,), (SLOTS, 2), (2, nb), (nb,)
    sems = [(4,), (3,), (4,), (), two,
            (3,), (2, 2), (2, 2), two, two, (2, 2), (2, 2),
            (O_SLOTS,), (), ring, ring, per, two, (),
            two, two, two, (), two, (SLOTS,), four, four, two, four,
            (SLOTS,), (2, SLOTS), (2, SLOTS), (LATE,), two, ()]
    scratch += [pltpu.SemaphoreType.DMA(shape) for shape in sems]
    flops = 2 * t * (d * (qw + 2 * HEAD) + qw * t + tp * qw * dh + 3 * d * f)
    split = nb - Y_VMEM * nb // 16
    outs = [(split * b, d), None, (t, HEAD), (t, HEAD), (t, tp * qw)]
    vm = _held((nb - split) * b, d)
    return pl.pallas_call(
        functools.partial(_kernel, tp, dp, zn, split, l1, l2, nb // 4, nb // 2, nb * 3 // 4),
        name="layer",
        out_shape=tuple(jax.ShapeDtypeStruct(shape, BF) if shape else vm for shape in outs),
        in_specs=[hbm] * 12,
        out_specs=tuple(hbm if shape else pl.BlockSpec(memory_space=pltpu.VMEM) for shape in outs),
        scratch_shapes=scratch,
        compiler_params=pltpu.CompilerParams(collective_id=0, has_side_effects=True,
                                             vmem_limit_bytes=VMEM_BYTES - 2 * (nb - split) * b * d),
        cost_estimate=pl.CostEstimate(flops=flops, bytes_accessed=8 * t * d, transcendentals=t * t * hl),
    )(x, pos, inv, g1, g2, wq, wk, wv, wo, wg, wu, wd)


def _copy_kernel(src, held, k_src, v_src, dst, k_dst, v_dst, buf, kv, rd, wr, kv_sem):
    rows = buf.shape[1]
    steps = src.shape[0] // rows
    small = ((k_src, k_dst), (v_src, v_dst))
    reads, writes, late = [], [], []
    for i in range(steps):
        part = pl.ds(i * rows, rows)
        reads.append(pltpu.make_async_copy(src.at[part], buf.at[i], rd.at[i]))
        writes.append(pltpu.make_async_copy(buf.at[i], dst.at[part], rd.at[i]))
    for e, (a, z) in enumerate(small):
        reads.append(pltpu.make_async_copy(a, kv.at[e], kv_sem.at[e]))
        writes.append(pltpu.make_async_copy(kv.at[e], z, kv_sem.at[e]))
    for i in range(held.shape[0] // rows):
        to = pl.ds(src.shape[0] + i * rows, rows)
        late.append(pltpu.make_async_copy(held.at[pl.ds(i * rows, rows)], dst.at[to], wr.at[i]))
    for copy in reads:
        copy.start()
    for copy in late:
        copy.start()
    for read, write in zip(reads, writes):
        read.wait()
        write.start()
    for copy in (*late, *writes):
        copy.wait()


def _copy(y, held, k, v):
    d = y.shape[1]
    t = y.shape[0] + held.shape[0]
    rows = 256
    hbm = pl.BlockSpec(memory_space=pltpu.HBM)
    dma = pltpu.SemaphoreType.DMA
    n = y.shape[0] // rows
    shapes = ((t, d), k.shape, v.shape)
    return pl.pallas_call(
        _copy_kernel,
        name="copy_out",
        out_shape=tuple(jax.ShapeDtypeStruct(shape, BF) for shape in shapes),
        in_specs=[hbm, pl.BlockSpec(memory_space=pltpu.VMEM), hbm, hbm],
        out_specs=(hbm,) * 3,
        scratch_shapes=[pltpu.VMEM((n, rows, d), BF), pltpu.VMEM((2,) + k.shape, BF),
                        dma((n,)), dma((held.shape[0] // rows,)), dma((2,))],
        compiler_params=pltpu.CompilerParams(vmem_limit_bytes=VMEM_BYTES - 3 * held.size),
        cost_estimate=pl.CostEstimate(flops=0, bytes_accessed=4 * t * d, transcendentals=0),
    )(y, held, k, v)


def _row_length(mesh):
    at = [getattr(dev, "coords", None) for dev in mesh.devices.reshape(mesh.shape["dp"], -1)[:, 0]]
    if any(p is None for p in at):
        return None
    n = len(at)

    def apart(i, j):
        return sum(abs(p - q) for p, q in zip(at[i], at[j]))

    length = next((i for i in range(1, n) if at[i][-1] == at[0][-1]), n)
    if length % 2 or n % (2 * length):
        return None
    rows = all(apart(i, i + 1) == 1 for i in range(0, n, 2))
    across = all(apart(i, i + length) == 1 for i in range(n) if (i // length) % 2 == 0)
    return length if rows and across else None


def solution(mesh):
    tp = mesh.shape["tp"]
    dp = mesh.shape["dp"]
    zn = _row_length(mesh)

    def local(x, pos, g1, g2, wq, wk, wv, wo, wg, wu, wd):
        t = x.shape[0]
        half = ROPE_BASE ** (-2.0 * np.arange(HEAD // 2) / HEAD)
        inv = jnp.asarray(np.concatenate([half, half])[None, :].astype(np.float32))
        y, held, k, v, _ = _layer(tp, dp, zn, x, pos.reshape(t // LANES, LANES), inv, g1, g2, wq, wk, wv, wo, wg, wu, wd)
        y, k, v = (_keep(a, pltpu.HBM) for a in (y, k, v))
        y, k, v = _copy(y, _keep(held, pltpu.VMEM), k, v)
        return y, k.reshape(t, 1, HEAD), v.reshape(t, 1, HEAD)

    return jax.shard_map(
        local,
        mesh=mesh,
        in_specs=(P("dp", None), P("dp"), P(), P(), P(None, "tp"), P(), P(), P("tp", None),
                  P(None, "tp"), P(None, "tp"), P("tp", None)),
        out_specs=(P("dp", None), P("dp", "tp", None), P("dp", "tp", None)),
        check_vma=False,
    )
```

```python
import functools

import jax
import jax.numpy as jnp
import numpy as np
from jax import lax
from jax.experimental import pallas as pl
from jax.experimental.pallas import tpu as pltpu
from jax.sharding import PartitionSpec as P

HEAD = 128
LANES = 128
SUB = 16
EPS = 1e-5
ROPE_BASE = 500000.0
MESH = pl.DeviceIdType.MESH
BLOCK = 256
NR = 64
SLOTS = 4
LATE = 8
CHIP = 3
O_SLOTS = 6
SIDES = (0, 1)
BF = jnp.bfloat16
F32 = jnp.float32
VMEM_BYTES = 67040000
Y_VMEM = 15
TWO_OVER_PI = 0.6366197723675814
PI_2 = (1.5703125, 4.837512969970703125e-4, 7.54978995489188216e-8)
SIN = (-1.9515295891e-4, 8.3321608736e-3, -1.6666654611e-1)
COS = (2.443315711809948e-5, -1.388731625493765e-3, 4.166664568298827e-2)
LOG2E = 1.4426950408889634


def _sincos(ang):
    n = jnp.floor(ang * TWO_OVER_PI + 0.5)
    r = ang
    for p in PI_2:
        r = r - n * p
    z = r * r
    s = functools.reduce(lambda a, p: a * z + p, SIN[1:], SIN[0]) * z * r + r
    c = functools.reduce(lambda a, p: a * z + p, COS[1:], COS[0]) * z * z - 0.5 * z + 1.0
    m = n.astype(jnp.int32)
    odd = (m & 1) == 1
    cs = jnp.where(odd, s, c)
    sn = jnp.where(odd, c, s)
    return jnp.where(((m + 1) & 2) == 2, -cs, cs), jnp.where((m & 2) == 2, -sn, sn)


def _al(v, m):
    return pl.multiple_of(v, m)


def _first(ref, n):
    return ref.at[pl.ds(0, n)]


def _kernel(tp, dp, zn, split, l1, l2, w2, w3, w4,
            x_ref, pos_ref, inv_ref, g1_ref, g2_ref, wq_ref, wk_ref, wv_ref, wo_ref, wg_ref, wu_ref, wd_ref,
            y_ref, y_vm, k_ref, v_ref, oall_ref,
            pos_v, inv_v, g1_v, g2_v, wo_v, wg_v, wu_v, wd_v, g_scr, a_buf, o_buf,
            hbuf, rsib, rs_far, rs_near, rs_sum,
            ld_s, ld_w, ld_mlp, ld_x, kv_s,
            wo_d, wo_s, wo_r, wo_fs, wo_fr, wo_ps, wo_pr,
            o_s, o_loc, o_r, o_f, o_rs, o_rel, o_fwd,
            ld_o, h_s, h_r, r_s, r_r, part_s, far_r, near_r, sum_s, sum_r,
            y_s, y_r, y_f, y_rs, y_rel, y_fwd):
    t, d = x_ref.shape
    qw = wq_ref.shape[1]
    f = wg_ref.shape[1]
    hl = qw // HEAD
    b = BLOCK
    nb = t // b
    dh = d // 2
    hb = b // 2
    fh = f // 2
    nc = tp // 2
    ow = hb // nc
    hw = ow // 2
    kvt = 2 * b

    last_y = (nb - split) * b
    wd_late = y_vm.at[pl.ds(last_y - fh, fh)]
    x_buf = o_blk = y_vm.at[pl.ds(last_y - 4 * b, b)]
    xh = y_vm.at[pl.ds(last_y - 3 * b, b), pl.ds(0, dh)]
    wqkv = wg_v.at[:, pl.ds(0, qw + 2 * HEAD)]

    r = lax.axis_index("tp")
    c = r // 2
    s = r % 2
    c_r = (c + 1) % nc
    c_l = (c + nc - 1) % nc
    c_o = (c + 2) % nc
    dest = ({"tp": c_r * 2 + s}, {"tp": c_l * 2 + s})
    origin = (c_l, c_r)
    target = (c_r, c_l)
    sib = {"tp": c * 2 + 1 - s}
    dpi = lax.axis_index("dp")
    par = dpi % 2
    peers = [{"dp": dpi + 1 - 2 * par}] if dp % 2 == 0 else []
    if zn:
        par_y = (dpi // zn) % 2
        peers.append({"dp": dpi + zn * (1 - 2 * par_y)})

    def send(src, dst, ss, rs, dev):
        pltpu.make_async_remote_copy(
            src_ref=src, dst_ref=dst, send_sem=ss, recv_sem=rs, device_id=dev, device_id_type=MESH).start()

    def put(src, dst, sem):
        pltpu.make_async_copy(src, dst, sem).start()

    def wait(region, sem, tag=None):
        with jax.named_scope("w_" + (tag or "end")):
            pltpu.make_async_copy(region, region, sem).wait()

    def when_block(j, body):
        @pl.when((j >= 0) & (j < nb))
        def _():
            body()

    barrier = pltpu.get_barrier_semaphore()
    cross = [{"tp": target[e] * 2 + 1 - s} for e in SIDES]
    others = [*dest, *cross, sib, *peers]
    for dev in others:
        pl.semaphore_signal(barrier, inc=1, device_id=dev, device_id_type=MESH)

    small = ((pos_ref, pos_v), (inv_ref, inv_v), (g1_ref, g1_v), (g2_ref, g2_v))
    rk = _al(r * HEAD, HEAD)
    wq_dst = wqkv.at[:, pl.ds(0, qw)]
    kv_dst = [wqkv.at[:, pl.ds(qw + e * HEAD, HEAD)] for e in SIDES]
    put(_first(x_ref, b), x_buf, ld_x)
    for e, (src, dst) in enumerate(small):
        put(src, dst, ld_s.at[e])
    put(wq_ref, wq_dst, ld_w.at[2])
    for e, ref in enumerate((wk_ref, wv_ref)):
        put(ref.at[:, pl.ds(rk, HEAD)], kv_dst[e], ld_w.at[e])

    def norm_rows(src, which):
        def step(e, carry):
            for q in range(NR // SUB):
                rows = pl.ds(_al(e * NR + q * SUB, SUB), SUB)
                v32 = src[rows, :].astype(F32)
                inv = lax.rsqrt(jnp.mean(v32 * v32, axis=1, keepdims=True) + EPS)
                a_buf[rows, :] = (v32 * inv * g_scr[which:which + 1, :]).astype(BF)
            return carry

        with jax.named_scope("norm"):
            lax.fori_loop(0, b // NR, step, 0)

    for e, (src, dst) in enumerate(small):
        wait(dst, ld_s.at[e], "small")
    for e, ref in enumerate((g1_v, g2_v)):
        g_scr[e:e + 1, :] = ref[...].astype(F32).reshape(1, d)

    def x_norm(i):
        wait(x_buf, ld_x, "x")
        norm_rows(x_buf, 0)

        @pl.when(i + 1 < nb)
        def _():
            put(x_ref.at[pl.ds(_al((i + 1) * b, b), b)], x_buf, ld_x)

    with jax.named_scope("barrier"):
        pl.semaphore_wait(barrier, len(others))

    mine = _al(s * dh, LANES)
    other = _al((1 - s) * dh, LANES)
    parts = 4 if zn else len(peers) + 1
    wr = qw // parts
    part = (2 * par_y + par) if zn else (par if peers else 0)

    def shard(dev):
        return wo_v.at[pl.ds(_al(dev * qw, LANES), qw)]

    def piece(chip, core, q=None):
        return wo_v.at[pl.ds(_al((chip * 2 + core) * qw + (part if q is None else q) * wr, 32), wr)]

    rows = pl.ds(_al(part * wr, 32), wr)
    for e in SIDES:
        for k, (cols, dev) in enumerate(((mine, dest[e]), (other, cross[e]))):
            send(wo_ref.at[rows, pl.ds(cols, dh)], piece(c, s), wo_s.at[e, k], wo_r.at[e, s], dev)
    send(wo_ref.at[:, pl.ds(other, dh)], shard(r), wo_d.at[0], wo_d.at[1], sib)
    put(wo_ref.at[:, pl.ds(mine, dh)], shard(r), wo_d.at[2])
    x_norm(0)

    def wo_swap(chip):
        for e, dev in enumerate(peers):
            for core in SIDES:
                send(piece(chip, core), piece(chip, core), wo_ps.at[0, e], wo_pr.at[0, e], dev)

    def wo_stage2():
        for e in SIDES:
            for core in SIDES:
                wait(piece(origin[e], core), wo_r.at[e, core], "wo2")
            reg = piece(origin[e], e)
            send(reg, reg, wo_fs.at[e], wo_fr.at[e], dest[e])
            wo_swap(origin[e])

    def wo_stage3():
        for e in SIDES:
            wait(piece(c_o, e), wo_fr.at[e], "wo3")
        wo_swap(c_o)

    def wo_stage4():
        for e in range(len(peers)):
            wait(_first(wo_v, 6 * wr), wo_pr.at[0, e], "wo4")
        if zn:
            for chip in (*origin, c_o):
                for e, q in enumerate((2 * (1 - par_y) + par, 2 * par_y + 1 - par)):
                    reg = piece(chip, e, q)
                    send(reg, reg, wo_ps.at[1, e], wo_pr.at[1, e], peers[e])

    def wo_end(which):
        for e in SIDES if zn else ():
            wait(_first(wo_v, 3 * wr), which.at[1, e], "wo5")

    def ocol(chip, core):
        return pl.ds(_al((chip * 2 + core) * qw, LANES), qw)

    def oreg(j, chip):
        return oall_ref.at[pl.ds(_al(j * b, b), b), ocol(chip, s)]

    def ohalf(j, chip, half):
        return oall_ref.at[pl.ds(_al(j * b + half * hb, hb), hb), ocol(chip, s)]

    def orow(j):
        return pl.ds(_al(j * b, b), b)

    def o_stage2(j):
        def body():
            for e in SIDES:
                reg = oreg(j, origin[e])
                wait(reg, o_r.at[e, j], "o2")
                half = ohalf(j, origin[e], e)
                send(half, half, o_rel.at[e], o_f.at[e, j], dest[e])
                send(reg, reg, o_fwd, o_rs.at[j], sib)

        when_block(j, body)

    def o_stage3(j):
        def body():
            for e in SIDES:
                wait(ohalf(j, c_o, e), o_f.at[e, j], "o3")
            send(oreg(j, c_o), oreg(j, c_o), o_fwd, o_rs.at[j], sib)

        when_block(j, body)

    def unrolled(n, body):
        for e in range(n):
            body(e)

    def load_o(j):
        wait(oall_ref.at[orow(j), pl.ds(0, 4 * qw)], o_rs.at[j], "os")
        put(oall_ref.at[orow(j)], o_blk, ld_o.at[0])
        put(x_ref.at[orow(j), pl.ds(mine, dh)], xh, ld_o.at[1])

    def attention(q_scr, k_scr, v_scr, m_scr, l_scr, acc_scr):
        caches = ((k_scr, k_ref), (v_scr, v_ref))
        mlp = ((wu_ref, wu_v), (_first(wd_ref, fh), wd_v), (wd_ref.at[pl.ds(fh, fh)], wd_late))
        scale = HEAD ** -0.5 * LOG2E
        lane = lax.broadcasted_iota(jnp.int32, (b, HEAD), 1)

        def heads(ref, h):
            return ref.at[pl.ds(h * b, b)]

        def o_sent(slot):
            wait(oall_ref.at[pl.ds(0, 3 * b), pl.ds(0, qw)], o_s.at[slot], "osent")

        def tile(first, n, masked=False):
            keys = pl.ds(_al(first, n), n)
            kk = k_scr[keys, :]
            vv = v_scr[keys, :]
            sc = lax.dot_general(q_scr[...], kk, (((1,), (1,)), ((), ())), preferred_element_type=F32)
            if masked:
                keep = lax.broadcasted_iota(jnp.int32, (b, n), 1) <= lax.broadcasted_iota(jnp.int32, (b, n), 0)
                sc = jnp.concatenate([jnp.where(keep, sc[h * b:(h + 1) * b], -jnp.inf) for h in range(hl)], axis=0)
            m_prev = m_scr[...]
            m_new = jnp.maximum(m_prev, jnp.max(sc, axis=1, keepdims=True))
            ps = [jnp.exp2((sc[:, e * HEAD:(e + 1) * HEAD] - m_new) * scale) for e in range(n // HEAD)]
            alpha = jnp.exp2((m_prev - m_new) * scale)
            l_scr[...] = l_scr[...] * alpha + functools.reduce(lambda p, q: p + q, ps)
            pr = jnp.concatenate([p.astype(BF) for p in ps], axis=1)
            acc_scr[...] = acc_scr[...] * alpha + jnp.dot(pr, vv, preferred_element_type=F32)
            m_scr[...] = m_new

        def phase1(i, carry):
            with jax.named_scope("slot1"):
                phase1_slot(i)
            return carry

        def phase1_slot(i):
            slot = i % O_SLOTS

            @pl.when(i >= O_SLOTS)
            def _():
                o_sent(slot)

            @pl.when(i > 0)
            def _():
                wait(o_buf.at[0], o_loc, "oloc")

            @pl.when(i == nb - 1)
            def _():
                load_o(0)

            @pl.when(i == 0)
            def _():
                wait(wq_dst, ld_w.at[2], "w")
                for e in SIDES:
                    wait(kv_dst[e], ld_w.at[e], "w")

            for e, (src, dst) in enumerate(mlp):
                @pl.when(i == min(w2 + e, nb - 1))
                def _(src=src, dst=dst, e=e):
                    put(src, dst, ld_mlp.at[e])

            pcol = []
            for e in range(b // LANES):
                prow = pos_v[pl.ds(i * (b // LANES) + e, 1), :].astype(F32)
                pcol.append(jnp.transpose(jnp.broadcast_to(prow, (LANES, LANES))))
            co, si = _sincos(jnp.concatenate(pcol, axis=0) * inv_v[...])
            si = jnp.where(lane < HEAD // 2, -si, si)
            qk32 = jnp.dot(a_buf[...], wg_v[:, :qw + HEAD], preferred_element_type=F32)
            v32 = jnp.dot(a_buf[...], wg_v[:, qw + HEAD:qw + 2 * HEAD], preferred_element_type=F32)
            rows = pl.ds(_al(i * b, b), b)
            for h in range(hl + 1):
                head = qk32[:, h * HEAD:(h + 1) * HEAD]
                head = (head * co + pltpu.roll(head, HEAD // 2, 1) * si).astype(BF)
                if h < hl:
                    heads(q_scr, h)[...] = head
                else:
                    k_scr[rows, :] = head
            v_scr[rows, :] = v32.astype(BF)
            for e, (src, dst) in enumerate(caches):
                @pl.when(i > 0)
                def _(src=src, e=e):
                    wait(_first(src, b), kv_s.at[e])

                put(src.at[rows], dst.at[rows], kv_s.at[e])
            m_scr[...] = jnp.full(m_scr.shape, -jnp.inf, F32)
            l_scr[...] = jnp.zeros(l_scr.shape, F32)
            acc_scr[...] = jnp.zeros(acc_scr.shape, F32)
            full = i // 2

            def inner(j, carry):
                for e in SIDES:
                    tile((2 * j + e) * kvt, kvt)
                return carry

            with jax.named_scope("tiles"):
                lax.fori_loop(0, full // 2, inner, 0)

            @pl.when(full % 2 == 1)
            def _():
                tile((full - 1) * kvt, kvt)

            @pl.when(i % 2 == 1)
            def _():
                tile((i - 1) * b, b)

            tile(i * b, b, masked=True)
            for h in range(hl):
                o_buf[slot, :, h * HEAD:(h + 1) * HEAD] = (
                    heads(acc_scr, h)[...] / jnp.sum(heads(l_scr, h)[...], axis=1, keepdims=True)).astype(BF)
            src = o_buf.at[slot]
            dst = oreg(i, c)
            for e in SIDES:
                send(src, dst, o_s.at[slot], o_r.at[e, i], dest[e])
            send(src, dst, o_s.at[slot], o_rs.at[i], sib)
            put(src, dst, o_loc)
            for when, stage in ((w2, wo_stage2), (w3, wo_stage3), (w4, wo_stage4)):
                pl.when(i == when)(stage)
            o_stage2(i - l1)
            o_stage3(i - l2)

            @pl.when(i + 1 < nb)
            def _():
                x_norm(i + 1)

        lax.fori_loop(0, nb, phase1, 0)
        for e, (src, _) in enumerate(caches):
            wait(_first(src, b), kv_s.at[e])

    loc = pltpu.VMEM
    pl.run_scoped(
        attention, loc((hl * b, HEAD), BF), loc((t, HEAD), BF),
        loc((t, HEAD), BF), *[loc((hl * b, HEAD), F32)] * 3)
    wait(o_buf.at[0], o_loc)
    wait(shard(r + 1 - 2 * s), wo_d.at[1])
    wait(shard(r), wo_d.at[2])
    wo_end(wo_pr)

    def rest(u_buf, r_buf, cp, sums, ych, hst):
        nt_h = min(512, dh)
        nt_f = min(512, f)
        nt_d = min(512, d)

        def cpart(j, chip, half):
            return cp.at[j % CHIP, pl.ds(_al(chip * ow + half * hw, hw), hw)]

        def sum_start(j):
            def body():
                two = j % 2
                q4 = j % SLOTS
                wait(rsib.at[two], r_r.at[two], "r")
                wait(rsib.at[two], r_s, "rs")

                def add(e, carry):
                    rows = pl.ds(_al(e * SUB, SUB), SUB)
                    own = r_buf[pl.ds(_al(s * hb + e * SUB, SUB), SUB), :]
                    cp[j % CHIP, rows, :] = (own.astype(F32) + rsib[two, rows, :].astype(F32)).astype(BF)
                    return carry

                with jax.named_scope("add"):
                    lax.fori_loop(0, hb // SUB, add, 0)
                for e in SIDES:
                    send(cpart(j, c_o, e), rs_far.at[q4, e], part_s.at[q4], far_r.at[q4, e], dest[e])
                for e in SIDES:
                    send(cpart(j, target[e], 1 - e), rs_near.at[q4, e], part_s.at[q4], near_r.at[q4, e], dest[e])

            when_block(j, body)

        def own_h(j):
            @pl.when(j < nb)
            def _():
                wait(o_blk, ld_o.at[0], "ldo")
                wait(xh, ld_o.at[1], "ldo")

                def col(n):
                    cols = pl.ds(n * nt_h, nt_h)
                    v32 = jnp.dot(o_blk[...], wo_v[:, cols], preferred_element_type=F32)
                    hbuf[j % 2, :, pl.ds(_al(s * dh + n * nt_h, LANES), nt_h)] = (xh[:, cols].astype(F32) + v32).astype(BF)

                with jax.named_scope("own_h"):
                    unrolled(dh // nt_h, col)

        def swap_h(j):
            @pl.when(j < nb)
            def _():
                half = hbuf.at[j % 2, :, pl.ds(mine, dh)]
                send(half, half, h_s.at[j % 2], h_r.at[j % 2], sib)

            @pl.when(j + 1 < nb)
            def _():
                load_o(j + 1)

        def mlp_norm(j):
            def body():
                two = j % 2
                wait(hbuf.at[two, :, pl.ds(other, dh)], h_r.at[two], "h")
                wait(hbuf.at[two, :, pl.ds(mine, dh)], h_s.at[two], "hs")

                @pl.when(j == 0)
                def _():
                    for e, dst in enumerate((wu_v, wd_v, wd_late, wg_v)):
                        wait(dst, ld_mlp.at[e], "mlp")

                norm_rows(hbuf.at[two], 1)
                hst[j % SLOTS] = hbuf[two, pl.ds(_al(s * hb + c * ow, SUB), ow), :]

            when_block(j, body)

        def mlp_up(j):
            def body():
                def col(n):
                    cols = pl.ds(n * nt_f, nt_f)
                    gt = jnp.dot(a_buf[...], wg_v[:, cols], preferred_element_type=F32)
                    up = jnp.dot(a_buf[...], wu_v[:, cols], preferred_element_type=F32)
                    u_buf[:, cols] = (gt * (1.0 / (1.0 + jnp.exp(-gt))) * up).astype(BF)

                with jax.named_scope("up"):
                    unrolled(f // nt_f, col)

            when_block(j, body)

        def mlp_down(j):
            def body():
                def col(n):
                    cols = pl.ds(n * nt_d, nt_d)
                    r32 = jnp.dot(u_buf[:, :fh], wd_v[:, cols], preferred_element_type=F32)
                    r32 = r32 + jnp.dot(u_buf[:, fh:], wd_late[:, cols], preferred_element_type=F32)
                    r_buf[:, cols] = r32.astype(BF)

                with jax.named_scope("down"):
                    unrolled(d // nt_d, col)
                send(r_buf.at[pl.ds(_al((1 - s) * hb, hb), hb)], rsib.at[j % 2], r_s, r_r.at[j % 2], sib)

            when_block(j, body)

        def sum_relay(j):
            def body():
                q4 = j % SLOTS
                two = j % 2

                @pl.when(j >= 2)
                def _():
                    wait(sums.at[two], sum_s.at[two], "sums")

                for e in SIDES:
                    wait(rs_far.at[q4, e], far_r.at[q4, e], "s1")
                    sums[two, e] = (rs_far[q4, e].astype(F32) + cpart(j, target[e], e)[...].astype(F32)).astype(BF)
                    send(sums.at[two, e], rs_sum.at[q4, e], sum_s.at[two], sum_r.at[q4, e], dest[e])

            when_block(j, body)

        def on_y(j, body):
            @pl.when((j >= 0) & (j < split))
            def _():
                body(y_ref, j * b, False)

            @pl.when((j >= split) & (j < nb))
            def _():
                body(y_vm, (j - split) * b, True)

        def yrow(ref, row, chip):
            return ref.at[pl.ds(_al(row + s * hb + chip * ow, ow), ow)]

        def yhalf(ref, row, chip, half):
            return ref.at[pl.ds(_al(row + s * hb + chip * ow + half * hw, hw), hw)]

        def y_sent(j, vmem):
            wait(cp.at[0, pl.ds(0, (3 if vmem else 4) * ow)], y_s.at[j % SLOTS], "ysent")

        def sum_end(j):
            @pl.when((j >= 2) & (j < split + 2))
            def _():
                y_sent(j - 2, False)

            @pl.when((j >= split + SLOTS) & (j < nb))
            def _():
                y_sent(j - SLOTS, True)

            def body(ref, row, vmem):
                q4 = j % SLOTS
                wait(cp.at[0, pl.ds(0, 4 * hw)], part_s.at[q4], "s1s")
                for e in SIDES:
                    wait(rs_near.at[q4, e], near_r.at[q4, e], "s2")
                    wait(rs_sum.at[q4, e], sum_r.at[q4, e], "s2")
                own = yrow(ref, row, c)
                src = own if vmem else ych.at[j % 2]
                for e in SIDES:
                    rows = pl.ds(e * hw, hw)
                    tot = cpart(j, c, e)[...].astype(F32) + rs_near[q4, 1 - e].astype(F32) + rs_sum[q4, e].astype(F32)
                    dst = yhalf(ref, row, c, e) if vmem else src.at[rows]
                    dst[...] = (hst[q4, rows, :].astype(F32) + tot).astype(BF)
                for e in SIDES:
                    send(src, own, y_s.at[q4], y_r.at[e, q4], dest[e])
                send(src, own, y_s.at[q4], y_rs.at[j % LATE], sib)
                if not vmem:
                    put(src, own, y_s.at[q4])

            on_y(j, body)

        def y_stage2(j):
            def body(ref, row, vmem):
                for e in SIDES:
                    reg = yrow(ref, row, origin[e])
                    wait(reg, y_r.at[e, j % SLOTS], "y2")
                    half = yhalf(ref, row, origin[e], e)
                    send(half, half, y_rel.at[e], y_f.at[e, j % SLOTS], dest[e])
                    send(reg, reg, y_fwd, y_rs.at[j % LATE], sib)

            on_y(j, body)

        def y_stage3(j):
            def body(ref, row, vmem):
                for e in SIDES:
                    wait(yhalf(ref, row, c_o, e), y_f.at[e, j % SLOTS], "y3")
                reg = yrow(ref, row, c_o)
                send(reg, reg, y_fwd, y_rs.at[j % LATE], sib)

            on_y(j, body)

        def y_seen(j):
            when_block(j, lambda: wait(cp.at[0], y_rs.at[j % LATE], "ys"))

        put(wg_ref, wg_v, ld_mlp.at[3])

        def phase2(i, carry):
            with jax.named_scope("slot2"):
                own_h(i)
                sum_start(i - 2)
                swap_h(i)
                mlp_norm(i - 1)
                sum_relay(i - 3)
                mlp_up(i - 1)
                sum_end(i - 4)
                mlp_down(i - 1)
                y_stage2(i - 5)
                y_stage3(i - 6)
                y_seen(i - LATE)
                o_stage2(nb + i - l1)
                o_stage3(nb + i - l2)
            return carry

        lax.fori_loop(0, nb + 6, phase2, 0)

        for j in range(nb + 6 - LATE, nb):
            wait(cp.at[0], y_rs.at[j % LATE])
        for j in range(max(nb - SLOTS, split), nb):
            y_sent(j, True)
        for e in SIDES:
            wait(sums.at[e], sum_s.at[e])
        for e in SIDES:
            wait(_first(y_vm, nb * hw), y_rel.at[e])
            wait(oall_ref.at[pl.ds(0, t // 2), pl.ds(0, qw)], o_rel.at[e])
            wait(_first(wo_v, wr), wo_fs.at[e])
            for k in SIDES:
                wait(_first(wo_v, wr), wo_s.at[e, k])
        wait(_first(y_vm, nb * ow * 3), y_fwd)
        for e in range(O_SLOTS):
            wait(oall_ref.at[pl.ds(0, 3 * b), pl.ds(0, qw)], o_s.at[e])
        wait(oall_ref.at[:, pl.ds(0, 3 * qw)], o_fwd)
        wait(_first(wo_v, qw), wo_d.at[0])
        for e in range(len(peers)):
            wait(_first(wo_v, 6 * wr), wo_ps.at[0, e])
        wo_end(wo_ps)

    pl.run_scoped(
        rest, loc((b, f), BF), loc((b, d), BF), loc((CHIP, hb, d), BF),
        loc((2, 2, hw, d), BF), loc((2, ow, d), BF), loc((SLOTS, ow, d), BF))


def _held(rows, d):
    return pltpu.VMEM((rows, d), BF)


def _keep(a, space):
    return pltpu.with_memory_space_constraint(a, space)


def _layer(tp, dp, zn, x, pos, inv, g1, g2, wq, wk, wv, wo, wg, wu, wd):
    t, d = x.shape
    qw = wq.shape[1]
    f = wg.shape[1]
    hl = qw // HEAD
    b = BLOCK
    nb = t // b
    hb = b // 2
    nc = tp // 2
    ow = hb // nc
    hw = ow // 2
    dh = d // 2
    assert nc == SLOTS and f <= 4 * b and nb > SLOTS and tp * qw == d and t % b == 0 and wk.shape[1] == tp * HEAD
    l1 = max(nb // 4, 1)
    l2 = min(nb * 3 // 4, nb - 2)
    hbm = pl.BlockSpec(memory_space=pl.ANY)
    bufs = [
        (tp * qw, dh), (d, f), (d, f), (f // 2, d), None, (b, d), (O_SLOTS, b, qw),
        (2, b, d), (2, hb, d), *[(SLOTS, 2, hw, d)] * 3,
    ]
    scratch = [pltpu.VMEM(a.shape, a.dtype) for a in (pos, inv, g1, g2)]
    scratch += [pltpu.VMEM((2, d), F32) if shape is None else pltpu.VMEM(shape, BF) for shape in bufs]
    two, four, ring, per = (2,), (SLOTS, 2), (2, nb), (nb,)
    sems = [(4,), (3,), (4,), (), two,
            (3,), (2, 2), (2, 2), two, two, (2, 2), (2, 2),
            (O_SLOTS,), (), ring, ring, per, two, (),
            two, two, two, (), two, (SLOTS,), four, four, two, four,
            (SLOTS,), (2, SLOTS), (2, SLOTS), (LATE,), two, ()]
    scratch += [pltpu.SemaphoreType.DMA(shape) for shape in sems]
    flops = 2 * t * (d * (qw + 2 * HEAD) + qw * t + tp * qw * dh + 3 * d * f)
    split = nb - Y_VMEM * nb // 16
    outs = [(split * b, d), None, (t, HEAD), (t, HEAD), (t, tp * qw)]
    vm = _held((nb - split) * b, d)
    return pl.pallas_call(
        functools.partial(_kernel, tp, dp, zn, split, l1, l2, nb // 4, nb // 2, nb * 3 // 4),
        name="layer",
        out_shape=tuple(jax.ShapeDtypeStruct(shape, BF) if shape else vm for shape in outs),
        in_specs=[hbm] * 12,
        out_specs=tuple(hbm if shape else pl.BlockSpec(memory_space=pltpu.VMEM) for shape in outs),
        scratch_shapes=scratch,
        compiler_params=pltpu.CompilerParams(collective_id=0, has_side_effects=True,
                                             vmem_limit_bytes=VMEM_BYTES - 2 * (nb - split) * b * d),
        cost_estimate=pl.CostEstimate(flops=flops, bytes_accessed=8 * t * d, transcendentals=t * t * hl),
    )(x, pos, inv, g1, g2, wq, wk, wv, wo, wg, wu, wd)


def _copy_kernel(src, held, k_src, v_src, dst, k_dst, v_dst, buf, kv, rd, wr, kv_sem):
    rows = buf.shape[1]
    steps = src.shape[0] // rows
    small = ((k_src, k_dst), (v_src, v_dst))
    reads, writes, late = [], [], []
    for i in range(steps):
        part = pl.ds(i * rows, rows)
        reads.append(pltpu.make_async_copy(src.at[part], buf.at[i], rd.at[i]))
        writes.append(pltpu.make_async_copy(buf.at[i], dst.at[part], rd.at[i]))
    for e, (a, z) in enumerate(small):
        reads.append(pltpu.make_async_copy(a, kv.at[e], kv_sem.at[e]))
        writes.append(pltpu.make_async_copy(kv.at[e], z, kv_sem.at[e]))
    for i in range(held.shape[0] // rows):
        to = pl.ds(src.shape[0] + i * rows, rows)
        late.append(pltpu.make_async_copy(held.at[pl.ds(i * rows, rows)], dst.at[to], wr.at[i]))
    for copy in reads:
        copy.start()
    for copy in late:
        copy.start()
    for read, write in zip(reads, writes):
        read.wait()
        write.start()
    for copy in (*late, *writes):
        copy.wait()


def _copy(y, held, k, v):
    d = y.shape[1]
    t = y.shape[0] + held.shape[0]
    rows = 256
    hbm = pl.BlockSpec(memory_space=pltpu.HBM)
    dma = pltpu.SemaphoreType.DMA
    n = y.shape[0] // rows
    shapes = ((t, d), k.shape, v.shape)
    return pl.pallas_call(
        _copy_kernel,
        name="copy_out",
        out_shape=tuple(jax.ShapeDtypeStruct(shape, BF) for shape in shapes),
        in_specs=[hbm, pl.BlockSpec(memory_space=pltpu.VMEM), hbm, hbm],
        out_specs=(hbm,) * 3,
        scratch_shapes=[pltpu.VMEM((n, rows, d), BF), pltpu.VMEM((2,) + k.shape, BF),
                        dma((n,)), dma((held.shape[0] // rows,)), dma((2,))],
        compiler_params=pltpu.CompilerParams(vmem_limit_bytes=VMEM_BYTES - 3 * held.size),
        cost_estimate=pl.CostEstimate(flops=0, bytes_accessed=4 * t * d, transcendentals=0),
    )(y, held, k, v)


def _row_length(mesh):
    at = [getattr(dev, "coords", None) for dev in mesh.devices.reshape(mesh.shape["dp"], -1)[:, 0]]
    if any(p is None for p in at):
        return None
    n = len(at)

    def apart(i, j):
        return sum(abs(p - q) for p, q in zip(at[i], at[j]))

    length = next((i for i in range(1, n) if at[i][-1] == at[0][-1]), n)
    if length % 2 or n % (2 * length):
        return None
    rows = all(apart(i, i + 1) == 1 for i in range(0, n, 2))
    across = all(apart(i, i + length) == 1 for i in range(n) if (i // length) % 2 == 0)
    return length if rows and across else None


def solution(mesh):
    tp = mesh.shape["tp"]
    dp = mesh.shape["dp"]
    zn = _row_length(mesh)

    def local(x, pos, g1, g2, wq, wk, wv, wo, wg, wu, wd):
        t = x.shape[0]
        half = ROPE_BASE ** (-2.0 * np.arange(HEAD // 2) / HEAD)
        inv = jnp.asarray(np.concatenate([half, half])[None, :].astype(np.float32))
        y, held, k, v, _ = _layer(tp, dp, zn, x, pos.reshape(t // LANES, LANES), inv, g1, g2, wq, wk, wv, wo, wg, wu, wd)
        y, k, v = (_keep(a, pltpu.HBM) for a in (y, k, v))
        y, k, v = _copy(y, _keep(held, pltpu.VMEM), k, v)
        return y, k.reshape(t, 1, HEAD), v.reshape(t, 1, HEAD)

    return jax.shard_map(
        local,
        mesh=mesh,
        in_specs=(P("dp", None), P("dp"), P(), P(), P(None, "tp"), P(), P(), P("tp", None),
                  P(None, "tp"), P(None, "tp"), P("tp", None)),
        out_specs=(P("dp", None), P("dp", "tp", None), P("dp", "tp", None)),
        check_vma=False,
    )
```
